32 devices in a mesh: dp: 1 (over z), sx: 4 (over y), sy: 8 (over x, core).
Axes of the slice: x: 4, y: 4, z: 1, core: 2. Of those that a mesh axis runs over, the one named last changes fastest.
The devices are a block of a 4x4x8 slice.
Arguments:
- act_in: bfloat16 [4, 512, 64, 256], P('dp', 'sy', 'sx')
- norm_first: bfloat16 [2, 256], replicated
- w_first: bfloat16 [3, 3, 256, 128], replicated
- w_short: bfloat16 [256, 128], replicated
- norm_rest: bfloat16 [6, 2, 128], replicated
- w_rest: bfloat16 [5, 3, 3, 128, 128], replicated
- bias_rest: bfloat16 [7, 128], replicated
- w_out: bfloat16 [3, 3, 128, 3], replicated
- bias_out: bfloat16 [3], replicated
Outputs:
- output: float32 [4, 512, 64, 3], P('dp', 'sy', 'sx')
All inputs are finite; a program needn't handle non-finite values.
Results may differ from the reference program's by a relative error of at most 0.0121751.
Values are sent between devices in bfloat16 or wider.
A program may use at most 768 MiB of HBM per device.

```python
import math
import jax
import jax.numpy as jnp
from jax import lax

SAMPLES = 4
IMG_H = 512
IMG_W = 64
IN_CH = 256
MID_CH = 128
OUT_CH = 3
GROUPS = 32
GN_EPS = 1e-6


def normal_weight(key, shape, fan_in):
    return (jax.random.normal(key, shape, jnp.float32) * fan_in ** -0.5).astype(jnp.bfloat16)


def norm_params(key, layer_count, chan_count):
    gain_key, shift_key = jax.random.split(key)
    gains = 1.0 + 0.25 * jax.random.normal(gain_key, (layer_count, chan_count), jnp.float32)
    shifts = 0.25 * jax.random.normal(shift_key, (layer_count, chan_count), jnp.float32)
    return jnp.stack([gains, shifts], axis=1).astype(jnp.bfloat16)


def setup_inputs(seed: int = 0, part: int = 0) -> dict:
    base_key = jax.random.key(seed)
    act_keys = jax.random.split(jax.random.fold_in(base_key, part), 6)
    weight_keys = jax.random.split(base_key, 8)
    wave_count = 3
    base_noise = jax.random.normal(act_keys[0], (SAMPLES, IMG_H, IMG_W, IN_CH), jnp.float32)
    wave_amp = jax.random.normal(act_keys[1], (SAMPLES, wave_count, 1, IN_CH), jnp.float32)
    row_freq = jax.random.uniform(act_keys[2], (SAMPLES, wave_count, 1, 1), jnp.float32, 0.5, 2.5)
    col_freq = jax.random.uniform(act_keys[3], (SAMPLES, wave_count, 1, 1), jnp.float32, 0.5, 2.5)
    row_phase = jax.random.uniform(act_keys[4], (SAMPLES, wave_count, 1, IN_CH), jnp.float32, 0.0, 2.0 * math.pi)
    col_phase = jax.random.uniform(act_keys[5], (SAMPLES, wave_count, 1, IN_CH), jnp.float32, 0.0, 2.0 * math.pi)
    row_pos = (jnp.arange(IMG_H, dtype=jnp.float32) / IMG_H)[:, None]
    col_pos = (jnp.arange(IMG_W, dtype=jnp.float32) / IMG_W)[:, None]
    row_wave = wave_amp * jnp.cos(2.0 * math.pi * row_freq * row_pos + row_phase)
    col_wave = jnp.cos(2.0 * math.pi * col_freq * col_pos + col_phase)
    smooth_field = jnp.einsum("skhc,skwc->shwc", row_wave, col_wave)
    act_in = (0.7 * base_noise + smooth_field).astype(jnp.bfloat16)
    return {
        "act_in": act_in,
        "norm_first": norm_params(weight_keys[0], 1, IN_CH)[0],
        "w_first": normal_weight(weight_keys[1], (3, 3, IN_CH, MID_CH), 9 * IN_CH),
        "w_short": normal_weight(weight_keys[2], (IN_CH, MID_CH), IN_CH),
        "norm_rest": norm_params(weight_keys[3], 6, MID_CH),
        "w_rest": normal_weight(weight_keys[4], (5, 3, 3, MID_CH, MID_CH), 9 * MID_CH),
        "bias_rest": (0.3 * jax.random.normal(weight_keys[5], (7, MID_CH), jnp.float32)).astype(jnp.bfloat16),
        "w_out": normal_weight(weight_keys[6], (3, 3, MID_CH, OUT_CH), 9 * MID_CH),
        "bias_out": (0.3 * jax.random.normal(weight_keys[7], (OUT_CH,), jnp.float32)).astype(jnp.bfloat16),
    }


def group_norm_act(act_map, norm_pair):
    num_rows, num_cols, channels = act_map.shape
    per_group = channels // GROUPS
    group_count = num_rows * num_cols * per_group
    sum_one = jnp.sum(act_map, axis=(0, 1), dtype=jnp.float32).reshape(GROUPS, per_group).sum(axis=1)
    sum_two = jnp.sum(jnp.square(act_map.astype(jnp.float32)), axis=(0, 1)).reshape(GROUPS, per_group).sum(axis=1)
    group_mean = sum_one / group_count
    inv_std = lax.rsqrt(sum_two / group_count - group_mean * group_mean + GN_EPS)
    chan_scale = jnp.repeat(inv_std, per_group) * norm_pair[0].astype(jnp.float32)
    chan_shift = norm_pair[1].astype(jnp.float32) - jnp.repeat(group_mean, per_group) * chan_scale
    return jax.nn.silu(act_map.astype(jnp.float32) * chan_scale + chan_shift).astype(jnp.bfloat16)


def conv_three(act_map, kernel):
    num_rows, num_cols, in_chans = act_map.shape
    padded = jnp.pad(act_map, ((1, 1), (1, 1), (0, 0)))
    accum_sum = jnp.zeros((num_rows * num_cols, kernel.shape[3]), jnp.float32)
    for row_off in range(3):
        for col_off in range(3):
            window = padded[row_off:row_off + num_rows, col_off:col_off + num_cols].reshape(num_rows * num_cols, in_chans)
            accum_sum = accum_sum + jnp.dot(window, kernel[row_off, col_off], preferred_element_type=jnp.float32)
    return accum_sum.reshape(num_rows, num_cols, kernel.shape[3])


def reference(act_in, norm_first, w_first, w_short, norm_rest, w_rest, bias_rest, w_out, bias_out):
    bias_rows = bias_rest.astype(jnp.float32)

    def decode_sample(sample):
        num_rows, num_cols, in_chans = sample.shape
        mid_act = (conv_three(group_norm_act(sample, norm_first), w_first) + bias_rows[0]).astype(jnp.bfloat16)
        skip_path = jnp.dot(sample.reshape(num_rows * num_cols, in_chans), w_short, preferred_element_type=jnp.float32).reshape(num_rows, num_cols, -1) + bias_rows[6]
        hidden = (conv_three(group_norm_act(mid_act, norm_rest[0]), w_rest[0]) + bias_rows[1] + skip_path).astype(jnp.bfloat16)
        for res_index in range(1, 3):
            first_at = 2 * res_index - 1
            mid_act = (conv_three(group_norm_act(hidden, norm_rest[first_at]), w_rest[first_at]) + bias_rows[first_at + 1]).astype(jnp.bfloat16)
            hidden = (conv_three(group_norm_act(mid_act, norm_rest[first_at + 1]), w_rest[first_at + 1]) + bias_rows[first_at + 2] + hidden.astype(jnp.float32)).astype(jnp.bfloat16)
        return conv_three(group_norm_act(hidden, norm_rest[5]), w_out) + bias_out.astype(jnp.float32)

    return lax.map(decode_sample, act_in)
```

```python
import functools

import jax
import jax.numpy as jnp
from jax import lax
from jax.experimental import pallas as pl
from jax.experimental.pallas import tpu as pltpu
from jax.sharding import PartitionSpec as P

GROUPS = 32
GN_EPS = 1e-6
MESH = pl.DeviceIdType.MESH
LANES = 128
ROW_BLOCK = 8
LAYERS = 7


def group_total(vec, per_group):
    lane = lax.broadcasted_iota(jnp.int32, vec.shape, 1)
    step = 1
    while step < per_group:
        low = pltpu.roll(vec, LANES - step, 1)
        high = pltpu.roll(vec, step, 1)
        vec = vec + jnp.where((lane & step) == 0, low, high)
        step *= 2
    return vec


def decode_kernel(rows_n, cols_n, act_hbm, norm_first, wf_hbm, ws_hbm, norm_rest, wr_hbm, bias_rest, wo_ref, bias_out, y_ref,
                  act, wf, ws, wr, wo, mid, hid, skip, pad_first, pad_rest, slab, edge_l, edge_r, turn,
                  st_first, st_rest, row_first, row_rest, col_first, col_rest,
                  cs_first, cs_rest, rs_rest,
                  load_sem, st_recv, row_recv, col_recv, st_send, row_send, col_send):
    samples, rows, cols, _ = act.shape
    pairs = rows // 2
    peers_n = rows_n * cols_n
    sx, sy = lax.axis_index("sx"), lax.axis_index("sy")
    at_x = [sx] + [lax.rem(sx + off, cols_n) for off in range(1, cols_n)]
    at_y = [sy] + [lax.rem(sy + off, rows_n) for off in range(1, rows_n)]
    peers = [{"sx": at_x[off // rows_n], "sy": at_y[off % rows_n]} for off in range(1, peers_n)]
    left, right, above, below = at_x[cols_n - 1], at_x[1], at_y[rows_n - 1], at_y[1]
    has_l, has_r, has_t, has_b = sx > 0, sx < cols_n - 1, sy > 0, sy < rows_n - 1

    loads = [pltpu.make_async_copy(act_hbm.at[s], act.at[s], load_sem.at[s]) for s in range(samples)]
    loads.append(pltpu.make_async_copy(ws_hbm, ws, load_sem.at[samples]))
    loads.append(pltpu.make_async_copy(wf_hbm, wf, load_sem.at[samples + 1]))
    loads.append(pltpu.make_async_copy(wr_hbm, wr, load_sem.at[samples + 2]))
    for load in loads:
        load.start()
    barrier = pltpu.get_barrier_semaphore()
    for peer in peers:
        pl.semaphore_signal(barrier, inc=1, device_id=peer, device_id_type=MESH)

    def stat_ref(layer):
        return st_first if layer == 0 else st_rest.at[layer - 1]

    def row_ref(layer):
        return row_first if layer == 0 else row_rest.at[layer - 1]

    def col_ref(layer):
        return col_first if layer == 0 else col_rest.at[layer - 1]

    def remote(src, dst, send, recv, peer):
        pltpu.make_async_remote_copy(src_ref=src, dst_ref=dst, send_sem=send, recv_sem=recv, device_id=peer, device_id_type=MESH).start()

    def send_all(layer, s, sums):
        stats = stat_ref(layer)
        for at, part in enumerate(sums):
            stats[s, 0, :, at * LANES:(at + 1) * LANES] = part
        for slot, peer in enumerate(peers):
            remote(stats.at[s, 0], stats.at[s, slot + 1], st_send.at[layer], st_recv.at[layer, s], peer)
        top = act.at[s, 0] if layer == 0 else rs_rest.at[layer - 1, s, 0]
        bottom = act.at[s, rows - 1] if layer == 0 else rs_rest.at[layer - 1, s, 1]
        col_src = cs_first.at[s] if layer == 0 else cs_rest.at[layer - 1, s]
        halo_rows, halo_cols = row_ref(layer), col_ref(layer)
        for src, y_to, base in ((top, above, 3), (bottom, below, 0)):
            for x_to, at in ((sx, 1), (left, 2), (right, 0)):
                remote(src, halo_rows.at[s, base + at], row_send.at[layer], row_recv.at[layer, s], {"sx": x_to, "sy": y_to})
        remote(col_src.at[0], halo_cols.at[s, 1], col_send.at[layer], col_recv.at[layer, s], {"sx": left, "sy": sy})
        remote(col_src.at[1], halo_cols.at[s, 0], col_send.at[layer], col_recv.at[layer, s], {"sx": right, "sy": sy})

    def wait_for(ref, sem):
        pltpu.make_async_copy(ref, ref, sem).wait()

    sub = lax.broadcasted_iota(jnp.int32, (8, LANES), 0)
    first_sub, last_sub = sub == 0, sub == 7

    def affine(layer, s):
        stats = stat_ref(layer)
        norm = norm_first if layer == 0 else norm_rest.at[layer - 1]
        channels = stats.shape[-1]
        per_group = channels // GROUPS
        count = rows * rows_n * cols * cols_n * per_group
        total = jnp.sum(stats[s], axis=0)
        pair = norm[...].astype(jnp.float32)
        out = []
        for at in range(channels // LANES):
            lanes = slice(at * LANES, (at + 1) * LANES)
            mean = group_total(jnp.broadcast_to(total[0:1, lanes], (8, LANES)), per_group) / count
            square = group_total(jnp.broadcast_to(total[1:2, lanes], (8, LANES)), per_group) / count
            scale = lax.rsqrt(square - mean * mean + GN_EPS) * jnp.broadcast_to(pair[0:1, lanes], (8, LANES))
            shift = jnp.broadcast_to(pair[1:2, lanes], (8, LANES)) - mean * scale
            out.append((0.5 * scale, 0.5 * shift))
        return out

    def silu(x, half_scale, half_shift):
        u = x * half_scale + half_shift
        return u + u * jnp.tanh(u)

    def activate(layer, s, pad, row_source, place):
        wait_for(stat_ref(layer).at[s, pl.ds(1, peers_n - 1)], st_recv.at[layer, s])
        scales = affine(layer, s)
        wait_for(row_ref(layer).at[s], row_recv.at[layer, s])
        wait_for(col_ref(layer).at[s], col_recv.at[layer, s])
        halo_rows, halo_cols = row_ref(layer), col_ref(layer)

        def store(v0, v1, from_left, from_right, tile, pair_at, half):
            r0, r1 = pltpu.roll(v0, 1, 0), pltpu.roll(v1, 1, 0)
            q0, q1 = pltpu.roll(v0, 7, 0), pltpu.roll(v1, 7, 0)
            shifted = (
                (jnp.where(first_sub, from_left, r0), jnp.where(first_sub, r0, r1)),
                (v0, v1),
                (jnp.where(last_sub, q1, q0), jnp.where(last_sub, from_right, q1)),
            )
            for off in range(3):
                place(pad, off, tile, pair_at, half, jnp.concatenate(shifted[off], axis=0).astype(jnp.bfloat16))

        for tile, (hs, ht) in enumerate(scales):
            lanes = slice(tile * LANES, (tile + 1) * LANES)
            edge_l[...] = jnp.where(has_l, silu(halo_cols[s, 0, :, lanes].astype(jnp.float32), hs[0:1], ht[0:1]), 0.0)
            edge_r[...] = jnp.where(has_r, silu(halo_cols[s, 1, :, lanes].astype(jnp.float32), hs[0:1], ht[0:1]), 0.0)
            for base, has, pair_at, half in ((0, has_t, 0, 0), (3, has_b, pairs, 1)):
                def halo(at):
                    row = halo_rows[s, base + at, :, lanes].astype(jnp.float32)
                    return silu(row[0:8], hs, ht), silu(row[8:16], hs, ht)

                corner_l = jnp.where(jnp.logical_and(has, has_l), pltpu.roll(halo(0)[1], 1, 0), 0.0)
                corner_r = jnp.where(jnp.logical_and(has, has_r), pltpu.roll(halo(2)[0], 7, 0), 0.0)
                v0, v1 = halo(1)
                store(jnp.where(has, v0, 0.0), jnp.where(has, v1, 0.0), corner_l, corner_r, tile, pair_at, half)

            def body(step, carry):
                r0 = step * ROW_BLOCK
                for at in range(ROW_BLOCK):
                    r = r0 + at
                    v0, v1 = row_source(s, r, tile)
                    v0, v1 = silu(v0, hs, ht), silu(v1, hs, ht)
                    from_left = jnp.broadcast_to(edge_l[pl.ds(r, 1), :], (8, LANES))
                    from_right = jnp.broadcast_to(edge_r[pl.ds(r, 1), :], (8, LANES))
                    store(v0, v1, from_left, from_right, tile, step * (ROW_BLOCK // 2) + (at + 1) // 2, (at + 1) % 2)
                return carry

            lax.fori_loop(0, rows // ROW_BLOCK, body, 0)

    def place_rest(pad, off, tile, pair_at, half, value):
        pad[off, pair_at, :, half * LANES:(half + 1) * LANES] = value

    def place_first(pad, off, tile, pair_at, half, value):
        pad[off, pair_at, half, :, tile * LANES:(tile + 1) * LANES] = value

    def act_rows(s, r, tile):
        row = act[s, r, :, tile * LANES:(tile + 1) * LANES].astype(jnp.float32)
        return row[0:8], row[8:16]

    def rows_of(ref):
        def source(s, r, tile):
            base = pl.multiple_of(r * cols, cols)
            return ref[s, pl.ds(base, 8), :], ref[s, pl.ds(base + 8, 8), :]
        return source

    zero = jnp.zeros((LANES, LANES), jnp.bfloat16)

    def square_of(a, b, c, d):
        return jnp.concatenate([jnp.concatenate([a, b], axis=1), jnp.concatenate([c, d], axis=1)], axis=0)

    def conv_rest(weight):
        total = None
        for off in range(3):
            w0, w1, w2 = (weight(row_off, off) for row_off in range(3))
            for shift, tap in ((0, square_of(w0, zero, w1, w0)), (1, square_of(w2, w1, zero, w2))):
                lhs = pad_rest[off, shift:shift + pairs].reshape(pairs * cols, 2 * LANES)
                part = jnp.dot(lhs, tap, preferred_element_type=jnp.float32)
                total = part if total is None else total + part
        return total

    def conv_first():
        wide = jnp.zeros((2 * LANES, LANES), jnp.bfloat16)
        total = None
        for off in range(3):
            w0, w1, w2 = (wf[row_off, off] for row_off in range(3))
            for at, (a, b) in enumerate(((w0, wide), (w1, w0), (w2, w1), (wide, w2))):
                lhs = pad_first[off, at // 2:at // 2 + pairs, at % 2].reshape(pairs * cols, 2 * LANES)
                part = jnp.dot(lhs, jnp.concatenate([a, b], axis=1), preferred_element_type=jnp.float32)
                total = part if total is None else total + part
        return total

    def finish(layer, s, total, bias, target, extra):
        next_layer = layer + 1
        acc = [[None, None], [None, None]]
        edges = {}
        for pair_at in range(pairs):
            for half in range(2):
                value = total[pair_at * cols:(pair_at + 1) * cols, half * LANES:(half + 1) * LANES] + bias
                base = (2 * pair_at + half) * cols
                if extra is not None:
                    value = value + extra[s, base:base + cols, :]
                packed = value.astype(jnp.bfloat16)
                value = packed.astype(jnp.float32)
                target[s, base:base + cols, :] = value
                if pair_at == 0 and half == 0:
                    rs_rest[layer, s, 0] = packed
                if pair_at == pairs - 1 and half == 1:
                    rs_rest[layer, s, 1] = packed
                one = value[0:8] + value[8:16]
                two = value[0:8] * value[0:8] + value[8:16] * value[8:16]
                for at, part in enumerate((one, two)):
                    acc[at][half] = part if acc[at][half] is None else acc[at][half] + part
        for side in range(2):
            column = target[s, pl.ds(side * (cols - 1), rows, stride=cols), :]
            cs_rest[layer, s, side] = column.astype(jnp.bfloat16)
        sums = [jnp.sum(acc[at][0] + acc[at][1], axis=0, keepdims=True) for at in range(2)]
        send_all(next_layer, s, [jnp.concatenate(sums, axis=0)])

    def first_sums(s, carry):
        wait_for(act.at[s], load_sem.at[s])

        def body(step, sums):
            sums = list(sums)
            for at in range(ROW_BLOCK):
                r = step * ROW_BLOCK + at
                for tile in range(2):
                    v0, v1 = act_rows(s, r, tile)
                    slab[0, tile, pl.ds(pl.multiple_of(r * 8, 8), 8), :] = v0
                    slab[1, tile, pl.ds(pl.multiple_of(r * 8, 8), 8), :] = v1
                    sums[2 * tile] = sums[2 * tile] + (v0 + v1)
                    sums[2 * tile + 1] = sums[2 * tile + 1] + (v0 * v0 + v1 * v1)
            return tuple(sums)

        sums = lax.fori_loop(0, rows // ROW_BLOCK, body, (jnp.zeros((8, LANES), jnp.float32),) * 4)
        for side in range(2):
            for tile in range(2):
                column = slab[side, tile, pl.ds(7 * side, rows, stride=8), :]
                cs_first[s, side, :, tile * LANES:(tile + 1) * LANES] = column.astype(jnp.bfloat16)
        sums = [jnp.sum(part, axis=0, keepdims=True) for part in sums]
        if carry == "first":
            pl.semaphore_wait(barrier, peers_n - 1)
        send_all(0, s, [jnp.concatenate(sums[0:2], axis=0), jnp.concatenate(sums[2:4], axis=0)])
        return carry

    first_sums(0, "first")
    lax.fori_loop(1, samples, first_sums, 0)

    bias = bias_rest[...].astype(jnp.float32)
    loads[samples].wait()

    def shortcut(s, carry):
        flat = act[s].reshape(rows * cols, 2 * LANES)
        skip[s] = jnp.dot(flat, ws[...], preferred_element_type=jnp.float32) + bias[6:7]
        return carry

    lax.fori_loop(0, samples, shortcut, 0)
    for tap in range(9):
        three = wo_ref[tap // 3, tap % 3].astype(jnp.float32)
        eight = jnp.concatenate([three, jnp.zeros((8 - three.shape[0], LANES), jnp.float32)], axis=0)
        wo[tap] = jnp.concatenate([eight] * 16, axis=0).T.astype(jnp.bfloat16)
    loads[samples + 1].wait()
    loads[samples + 2].wait()

    def layer_first(s, carry):
        activate(0, s, pad_first, act_rows, place_first)
        finish(0, s, conv_first(), bias[0:1], mid, None)
        return carry

    lax.fori_loop(0, samples, layer_first, 0)
    for layer in range(1, LAYERS - 1):
        source, target = (mid, hid) if layer % 2 else (hid, mid)
        extra = None if layer % 2 == 0 else (skip if layer == 1 else hid)

        def layer_rest(s, carry):
            activate(layer, s, pad_rest, rows_of(source), place_rest)
            total = conv_rest(lambda row_off, off: wr[layer - 1, row_off, off])
            finish(layer, s, total, bias[layer:layer + 1], target, extra)
            return carry

        lax.fori_loop(0, samples, layer_rest, 0)

    lane = lax.broadcasted_iota(jnp.int32, (rows, LANES), 1)
    out_bias = bias_out[...].astype(jnp.float32)

    def layer_last(s, carry):
        activate(LAYERS - 1, s, pad_rest, rows_of(hid), place_rest)
        total = conv_rest(lambda row_off, off: wo[3 * row_off + off])
        for pair_at in range(pairs):
            for half in range(2):
                base = (2 * pair_at + half) * cols
                mid[s, base:base + cols, :] = total[pair_at * cols:(pair_at + 1) * cols, half * LANES:(half + 1) * LANES]
        merged = mid[s, pl.ds(0, rows, stride=cols), :]
        for col in range(1, cols):
            merged = jnp.where(lane // 8 == col, mid[s, pl.ds(col, rows, stride=cols), :], merged)
        turn[...] = jnp.concatenate([merged] * (LANES // rows), axis=0).T
        for chan in range(y_ref.shape[1]):
            plane = turn[pl.ds(chan, cols, stride=8), :]
            y_ref[s, chan] = plane[:, 0:rows] + out_bias[0:1, chan:chan + 1]
        return carry

    lax.fori_loop(0, samples, layer_last, 0)

    for layer in range(LAYERS):
        wait_for(stat_ref(layer).at[:, pl.ds(1, peers_n - 1)], st_send.at[layer])
        wait_for(row_ref(layer), row_send.at[layer])
        wait_for(col_ref(layer), col_send.at[layer])


def solution(mesh):
    rows_n, cols_n = mesh.shape["sy"], mesh.shape["sx"]
    peers_n = rows_n * cols_n
    tile_spec = P("dp", "sy", "sx", None)
    replicated = P()

    def local_decode(act_in, norm_first, w_first, w_short, norm_rest, w_rest, bias_rest, w_out, bias_out):
        samples, rows, cols, wide = act_in.shape
        chans = w_short.shape[1]
        out_chans = w_out.shape[3]
        f32, bf16 = jnp.float32, jnp.bfloat16
        rest = LAYERS - 1
        whole = pl.BlockSpec(memory_space=pltpu.VMEM)
        there = pl.BlockSpec(memory_space=pl.ANY)
        image = pl.pallas_call(
            functools.partial(decode_kernel, rows_n, cols_n),
            name="decode",
            out_shape=jax.ShapeDtypeStruct((samples, out_chans, cols, rows), f32),
            in_specs=[there, whole, there, there, whole, there, whole, whole, whole],
            out_specs=whole,
            scratch_shapes=[
                pltpu.VMEM(act_in.shape, bf16),
                pltpu.VMEM(w_first.shape, bf16),
                pltpu.VMEM(w_short.shape, bf16),
                pltpu.VMEM(w_rest.shape, bf16),
                pltpu.VMEM((9, chans, LANES), bf16),
                pltpu.VMEM((samples, rows * cols, chans), f32),
                pltpu.VMEM((samples, rows * cols, chans), f32),
                pltpu.VMEM((samples, rows * cols, chans), f32),
                pltpu.VMEM((3, rows // 2 + 1, 2, cols, wide), bf16),
                pltpu.VMEM((3, rows // 2 + 1, cols, 2 * chans), bf16),
                pltpu.VMEM((2, 2, rows * 8, LANES), f32),
                pltpu.VMEM((rows, LANES), f32),
                pltpu.VMEM((rows, LANES), f32),
                pltpu.VMEM((LANES, LANES), f32),
                pltpu.VMEM((samples, peers_n, 2, wide), f32),
                pltpu.VMEM((rest, samples, peers_n, 2, chans), f32),
                pltpu.VMEM((samples, 6, cols, wide), bf16),
                pltpu.VMEM((rest, samples, 6, cols, chans), bf16),
                pltpu.VMEM((samples, 2, rows, wide), bf16),
                pltpu.VMEM((rest, samples, 2, rows, chans), bf16),
                pltpu.VMEM((samples, 2, rows, wide), bf16),
                pltpu.VMEM((rest, samples, 2, rows, chans), bf16),
                pltpu.VMEM((rest, samples, 2, cols, chans), bf16),
                pltpu.SemaphoreType.DMA((samples + 3,)),
                pltpu.SemaphoreType.DMA((LAYERS, samples)),
                pltpu.SemaphoreType.DMA((LAYERS, samples)),
                pltpu.SemaphoreType.DMA((LAYERS, samples)),
                pltpu.SemaphoreType.DMA((LAYERS,)),
                pltpu.SemaphoreType.DMA((LAYERS,)),
                pltpu.SemaphoreType.DMA((LAYERS,)),
            ],
            compiler_params=pltpu.CompilerParams(collective_id=0, has_side_effects=True, vmem_limit_bytes=60 * 1024 * 1024),
        )(act_in, norm_first, w_first, w_short, norm_rest, w_rest, bias_rest, jnp.transpose(w_out, (0, 1, 3, 2)), bias_out.reshape(1, out_chans))
        return jnp.transpose(image, (0, 3, 2, 1))

    return jax.shard_map(local_decode, mesh=mesh, in_specs=(tile_spec,) + (replicated,) * 8, out_specs=tile_spec, check_vma=False)
```

```python
import functools

import jax
import jax.numpy as jnp
from jax import lax
from jax.experimental import pallas as pl
from jax.experimental.pallas import tpu as pltpu
from jax.sharding import PartitionSpec as P

GROUPS = 32
GN_EPS = 1e-6
MESH = pl.DeviceIdType.MESH
LANES = 128
ROW_BLOCK = 8
LAYERS = 7
CHUNKS = 4


def group_total(vec, per_group):
    lane = lax.broadcasted_iota(jnp.int32, vec.shape, 1) & (per_group - 1)
    parts = [vec]
    for dist in range(1, per_group):
        parts.append(jnp.where(lane >= dist, pltpu.roll(vec, dist, 1), pltpu.roll(vec, LANES - per_group + dist, 1)))
    while len(parts) > 1:
        parts = [parts[at] + parts[at + 1] if at + 1 < len(parts) else parts[at] for at in range(0, len(parts), 2)]
    return parts[0]


def far_first(rows_n, cols_n):
    every = [(a, b) for a in range(cols_n) for b in range(rows_n) if a or b]
    return sorted(every, key=lambda off: -(min(off[0], cols_n - off[0]) + min(off[1], rows_n - off[1]) / 2))


def decode_kernel(rows_n, cols_n, act_hbm, norm_first, wf_hbm, ws_hbm, norm_rest, wr_hbm, bias_rest, wo_ref, bias_out, y_ref,
                  act, wf, ws, wr, wo, mid, hid, bias_rows, pad_first, pad_rest, slab, edge_l, edge_r, turn,
                  st_first, row_first, col_first, cs_first,
                  st_rest, corner_in, row_in, col_in, corner_out, row_out, col_out, whole_inbox,
                  load_sem, first_recv, col_recv, first_send, recv, send):
    samples, rows, cols, _ = act.shape
    pairs = rows // 2
    peers_n = rows_n * cols_n
    sx, sy = lax.axis_index("sx"), lax.axis_index("sy")
    at_x = [sx] + [lax.rem(sx + off, cols_n) for off in range(1, cols_n)]
    at_y = [sy] + [lax.rem(sy + off, rows_n) for off in range(1, rows_n)]
    order = far_first(rows_n, cols_n)
    has_l, has_r, has_t, has_b = sx > 0, sx < cols_n - 1, sy > 0, sy < rows_n - 1

    def device(off):
        return {"sx": at_x[off[0] % cols_n], "sy": at_y[off[1] % rows_n]}

    def wrap(off):
        return (off[0] % cols_n, off[1] % rows_n)

    corner_to = {wrap(off): at for at, off in enumerate(((-1, -1), (1, -1), (-1, 1), (1, 1)))}
    row_to = {wrap(off): at for at, off in enumerate(((0, -1), (0, 1)))}
    col_to = {wrap(off): at for at, off in enumerate(((-1, 0), (1, 0)))}
    plain = [off for off in order if off not in corner_to and off not in row_to and off not in col_to]

    loads = [pltpu.make_async_copy(act_hbm.at[s], act.at[s], load_sem.at[s]) for s in range(samples)]
    loads.append(pltpu.make_async_copy(ws_hbm, ws, load_sem.at[samples]))
    loads.append(pltpu.make_async_copy(wf_hbm, wf, load_sem.at[samples + 1]))
    loads.append(pltpu.make_async_copy(wr_hbm, wr, load_sem.at[samples + 2]))
    for load in loads:
        load.start()
    barrier = pltpu.get_barrier_semaphore()
    for off in order:
        pl.semaphore_signal(barrier, inc=1, device_id=device(off), device_id_type=MESH)

    def remote(src, dst, send_to, recv_at, off):
        pltpu.make_async_remote_copy(src_ref=src, dst_ref=dst, send_sem=send_to, recv_sem=recv_at, device_id=device(off), device_id_type=MESH).start()

    def wait_for(ref, sem):
        pltpu.make_async_copy(ref, ref, sem).wait()

    def send_rest(at, s):
        sem = recv.at[at, s]
        for off in order:
            if off in corner_to:
                box = corner_to[off]
                remote(corner_out.at[at, s, box], corner_in.at[at, s, 3 - box], send.at[1], sem, off)
            elif off in row_to:
                box = row_to[off]
                remote(row_out.at[at, s, box], row_in.at[at, s, 1 - box], send.at[2], sem, off)
            elif off in col_to:
                box = col_to[off]
                remote(col_out.at[at, s, box], col_in.at[at, s, 1 - box], send.at[3], sem, off)
            else:
                remote(st_rest.at[at, s, 0], st_rest.at[at, s, 1 + plain.index(off)], send.at[0], sem, off)

    sub = lax.broadcasted_iota(jnp.int32, (1, 8, LANES), 1)
    first_sub, last_sub = sub == 0, sub == 7

    def affine(total, norm, per_group):
        count = rows * rows_n * cols * cols_n * per_group
        mean = group_total(jnp.broadcast_to(total[0:1], (8, LANES)), per_group) / count
        square = group_total(jnp.broadcast_to(total[1:2], (8, LANES)), per_group) / count
        scale = lax.rsqrt(square - mean * mean + GN_EPS) * jnp.broadcast_to(norm[0:1], (8, LANES))
        shift = jnp.broadcast_to(norm[1:2], (8, LANES)) - mean * scale
        return 0.5 * scale, 0.5 * shift

    def silu(x, scales):
        u = x * scales[0] + scales[1]
        return u + u * jnp.tanh(u)

    def spread(rows_of_cols, from_left, from_right):
        v0, v1 = rows_of_cols[:, 0], rows_of_cols[:, 1]
        r0, r1 = pltpu.roll(v0, 1, 1), pltpu.roll(v1, 1, 1)
        q0, q1 = pltpu.roll(v0, 7, 1), pltpu.roll(v1, 7, 1)
        shifted = (
            (jnp.where(first_sub, from_left, r0), jnp.where(first_sub, r0, r1)),
            (v0, v1),
            (jnp.where(last_sub, q1, q0), jnp.where(last_sub, from_right, q1)),
        )
        return [jnp.concatenate(pair, axis=1).astype(jnp.bfloat16) for pair in shifted]

    def edges(tile, scales, halo_cols):
        one_row = (scales[0][0:1], scales[1][0:1])
        edge_l[tile] = jnp.where(has_l, silu(halo_cols[0], one_row), 0.0)
        edge_r[tile] = jnp.where(has_r, silu(halo_cols[1], one_row), 0.0)

    def activate(block, tile, scales, halo_rows, corners, row_source, place):
        begin, end = max(0, 8 * block + 1), min(rows, 8 * block + 9)
        value = row_source(begin, end)
        lefts = [jnp.broadcast_to(edge_l[tile, r:r + 1, :], (8, LANES)) for r in range(begin, end)]
        rights = [jnp.broadcast_to(edge_r[tile, r:r + 1, :], (8, LANES)) for r in range(begin, end)]
        value = silu(value, scales)
        for at, has in enumerate((has_t, has_b)):
            if block == (-1, rows // 8 - 1)[at]:
                halo = jnp.where(has, silu(halo_rows[at].reshape(1, 2, 8, LANES), scales), 0.0)
                corner_l = jnp.where(jnp.logical_and(has, has_l), silu(corners[2 * at], scales), 0.0)
                corner_r = jnp.where(jnp.logical_and(has, has_r), silu(corners[2 * at + 1], scales), 0.0)
                where_at = 0 if at == 0 else len(lefts)
                value = jnp.concatenate([halo, value] if at == 0 else [value, halo], axis=0)
                lefts.insert(where_at, corner_l)
                rights.insert(where_at, corner_r)
        for off, part in enumerate(spread(value, jnp.stack(lefts), jnp.stack(rights))):
            place(off, tile, 4 * block + 1 if block >= 0 else 0, part.reshape(part.shape[0] // 2, 2, cols, LANES))

    def prepare_rest(at, s, source):
        wait_for(whole_inbox, recv.at[at, s])
        total = jnp.sum(st_rest[at, s], axis=0)
        for box in range(4):
            total = total + corner_in[at, s, box, 0:2]
        for box in range(2):
            total = total + (row_in[at, s, box, 0:2] + col_in[at, s, box, 0:2])
        scales = affine(total, norm_rest[at].astype(jnp.float32), LANES // GROUPS)

        def row_source(begin, end):
            return source[s, begin * cols:end * cols, :].reshape(end - begin, 2, 8, LANES)

        def place(off, tile, pair_at, value):
            for half in range(2):
                pad_rest[off, pair_at:pair_at + value.shape[0], :, half * LANES:(half + 1) * LANES] = value[:, half]

        edges(0, scales, [col_in[at, s, box, 8:8 + rows, :] for box in range(2)])
        halo_rows = [row_in[at, s, box, 8:8 + cols, :] for box in range(2)]
        corners = [jnp.broadcast_to(corner_in[at, s, box, 2:3, :], (8, LANES)) for box in range(4)]
        return lambda block: activate(block, 0, scales, halo_rows, corners, row_source, place)

    def prepare_first(s):
        wait_for(col_first.at[s], col_recv.at[s])
        total = jnp.sum(st_first[:, s], axis=0)
        norm = norm_first[...].astype(jnp.float32)

        def one_tile(tile):
            lanes = slice(tile * LANES, (tile + 1) * LANES)
            scales = affine(total[:, lanes], norm[:, lanes], 2 * LANES // GROUPS)

            def row_source(begin, end):
                return act[s, begin:end, :, lanes].astype(jnp.float32).reshape(end - begin, 2, 8, LANES)

            def place(off, tile, pair_at, value):
                pad_first[off, pair_at:pair_at + value.shape[0], :, :, lanes] = value

            edges(tile, scales, [col_first[s, box, :, lanes].astype(jnp.float32) for box in range(2)])
            halo_rows = [row_first[box, s, :, lanes].astype(jnp.float32) for box in (1, 4)]
            corners = []
            for box in (0, 2, 3, 5):
                row = row_first[box, s, :, lanes].astype(jnp.float32)
                corners.append(pltpu.roll(row[8:16], 1, 0) if box % 3 == 0 else pltpu.roll(row[0:8], 7, 0))
            return lambda block: activate(block, tile, scales, halo_rows, corners, row_source, place)

        tiles = [one_tile(tile) for tile in range(2)]
        return lambda block: [tile(block) for tile in tiles]

    zero = jnp.zeros((LANES, LANES), jnp.bfloat16)
    wide_zero = jnp.zeros((2 * LANES, LANES), jnp.bfloat16)

    def square_of(a, b, c, d):
        return jnp.concatenate([jnp.concatenate([a, b], axis=1), jnp.concatenate([c, d], axis=1)], axis=0)

    def conv_rest(weight, pair_from, pair_n):
        total = None
        for off in range(3):
            w0, w1, w2 = (weight(row_off, off) for row_off in range(3))
            for shift, tap in ((0, square_of(w0, zero, w1, w0)), (1, square_of(w2, w1, zero, w2))):
                lhs = pad_rest[off, pair_from + shift:pair_from + shift + pair_n].reshape(pair_n * cols, 2 * LANES)
                part = jnp.dot(lhs, tap, preferred_element_type=jnp.float32)
                total = part if total is None else total + part
        return total

    def conv_first(pair_from, pair_n):
        total = None
        for off in range(3):
            w0, w1, w2 = (wf[row_off, off] for row_off in range(3))
            for at, (a, b) in enumerate(((w0, wide_zero), (w1, w0), (w2, w1), (wide_zero, w2))):
                begin = pair_from + at // 2
                lhs = pad_first[off, begin:begin + pair_n, at % 2].reshape(pair_n * cols, 2 * LANES)
                part = jnp.dot(lhs, jnp.concatenate([a, b], axis=1), preferred_element_type=jnp.float32)
                total = part if total is None else total + part
        return total

    def in_chunks(block, conv, use):
        block(-1)
        done, per_chunk = 0, pairs // CHUNKS
        for chunk in range(CHUNKS):
            while 4 * done < (chunk + 1) * per_chunk:
                block(done)
                done += 1
            total = conv(chunk * per_chunk, per_chunk)
            halves = [total[:, half * LANES:(half + 1) * LANES].reshape(per_chunk, 1, cols, LANES) for half in range(2)]
            use(2 * chunk * per_chunk, jnp.concatenate(halves, axis=1).reshape(2 * per_chunk * cols, LANES))

    def finish(at, s, block, conv, bias, target, residual):
        acc = []

        def use(row, value):
            rows_in = value.shape[0] // cols
            value = value + bias
            if residual is not None:
                value = value + residual[s, row * cols:row * cols + value.shape[0], :]
            value = value.astype(jnp.bfloat16).astype(jnp.float32)
            target[s, row * cols:row * cols + value.shape[0], :] = value
            for edge, edge_row in enumerate((0, rows - 1)):
                if row <= edge_row < row + rows_in:
                    line = value[(edge_row - row) * cols:(edge_row - row + 1) * cols]
                    row_out[at, s, edge, 8:8 + cols, :] = line
                    corner_out[at, s, 2 * edge, 2:3, :] = line[0:1]
                    corner_out[at, s, 2 * edge + 1, 2:3, :] = line[cols - 1:cols]
            split = value.reshape(value.shape[0] // 16, 2, 8, LANES)
            acc.append([jnp.sum(split, axis=0), jnp.sum(split * split, axis=0)])

        in_chunks(block, conv, use)
        sums = []
        for which in range(2):
            part = acc[0][which]
            for more in acc[1:]:
                part = part + more[which]
            sums.append(jnp.sum(part[0] + part[1], axis=0, keepdims=True))
        sums = jnp.concatenate(sums, axis=0)
        st_rest[at, s, 0] = sums
        for box in range(4):
            corner_out[at, s, box, 0:2, :] = sums
        for box in range(2):
            col_out[at, s, box, 8:8 + rows, :] = target[s, pl.ds(box * (cols - 1), rows, stride=cols), :]
            row_out[at, s, box, 0:2, :] = sums
            col_out[at, s, box, 0:2, :] = sums
        send_rest(at, s)

    def first_sums(s, carry):
        wait_for(act.at[s], load_sem.at[s])

        def body(step, sums):
            sums = list(sums)
            for at in range(ROW_BLOCK):
                r = step * ROW_BLOCK + at
                for tile in range(2):
                    row = act[s, r, :, tile * LANES:(tile + 1) * LANES].astype(jnp.float32)
                    v0, v1 = row[0:8], row[8:16]
                    slab[0, tile, pl.ds(pl.multiple_of(r * 8, 8), 8), :] = v0
                    slab[1, tile, pl.ds(pl.multiple_of(r * 8, 8), 8), :] = v1
                    sums[2 * tile] = sums[2 * tile] + (v0 + v1)
                    sums[2 * tile + 1] = sums[2 * tile + 1] + (v0 * v0 + v1 * v1)
            return tuple(sums)

        sums = lax.fori_loop(0, rows // ROW_BLOCK, body, (jnp.zeros((8, LANES), jnp.float32),) * 4)
        for side in range(2):
            for tile in range(2):
                column = slab[side, tile, pl.ds(7 * side, rows, stride=8), :]
                cs_first[s, side, :, tile * LANES:(tile + 1) * LANES] = column.astype(jnp.bfloat16)
        for tile in range(2):
            two = [jnp.sum(part, axis=0, keepdims=True) for part in sums[2 * tile:2 * tile + 2]]
            st_first[0, s, :, tile * LANES:(tile + 1) * LANES] = jnp.concatenate(two, axis=0)
        return carry

    lax.fori_loop(0, samples, first_sums, 0)
    pl.semaphore_wait(barrier, peers_n - 1)

    def first_columns(s, carry):
        for off, box in col_to.items():
            remote(cs_first.at[s, box], col_first.at[s, 1 - box], first_send.at[2], col_recv.at[s], off)
        return carry

    lax.fori_loop(0, samples, first_columns, 0)
    for slot, off in enumerate(order):
        remote(st_first.at[0], st_first.at[slot + 1], first_send.at[0], first_recv.at[0], off)
    for row, y_off, base in ((0, -1, 3), (rows - 1, 1, 0)):
        for x_off, at in ((-1, 2), (0, 1), (1, 0)):
            remote(act.at[:, row], row_first.at[base + at], first_send.at[1], first_recv.at[1], (x_off, y_off))

    bias = bias_rest[...].astype(jnp.float32)
    loads[samples].wait()

    def shortcut(s, carry):
        flat = act[s].reshape(rows * cols, 2 * LANES)
        hid[s] = jnp.dot(flat, ws[...], preferred_element_type=jnp.float32) + bias[6:7]
        return carry

    lax.fori_loop(0, samples, shortcut, 0)
    for tap in range(9):
        three = wo_ref[tap // 3, tap % 3].astype(jnp.float32)
        eight = jnp.concatenate([three, jnp.zeros((8 - three.shape[0], LANES), jnp.float32)], axis=0)
        wo[tap] = jnp.concatenate([eight] * 16, axis=0).T.astype(jnp.bfloat16)
    loads[samples + 1].wait()
    loads[samples + 2].wait()
    wait_for(st_first.at[pl.ds(1, peers_n - 1)], first_recv.at[0])
    wait_for(row_first, first_recv.at[1])

    def layer_first(s, carry):
        finish(0, s, prepare_first(s), conv_first, bias[0:1], mid, None)
        return carry

    lax.fori_loop(0, samples, layer_first, 0)

    def layer_rest(layer, source, target, residual):
        def one_sample(s, carry):
            block = prepare_rest(layer - 1, s, source)
            conv = functools.partial(conv_rest, lambda row_off, off: wr[layer - 1, row_off, off])
            finish(layer, s, block, conv, bias_rows[pl.ds(layer, 1), :], target, residual)
            return carry

        lax.fori_loop(0, samples, one_sample, 0)

    def layer_pair(step, carry):
        layer_rest(2 * step + 1, mid, hid, hid)
        layer_rest(2 * step + 2, hid, mid, None)
        return carry

    bias_rows[0:bias.shape[0], :] = bias
    lax.fori_loop(0, (LAYERS - 2) // 2, layer_pair, 0)
    layer_rest(LAYERS - 2, mid, hid, hid)

    lane = lax.broadcasted_iota(jnp.int32, (rows, LANES), 1)
    out_bias = bias_out[...].astype(jnp.float32)

    def layer_last(s, carry):
        def use(row, value):
            mid[s, row * cols:row * cols + value.shape[0], :] = value

        in_chunks(prepare_rest(LAYERS - 2, s, hid), functools.partial(conv_rest, lambda row_off, off: wo[3 * row_off + off]), use)
        merged = mid[s, pl.ds(0, rows, stride=cols), :]
        for col in range(1, cols):
            merged = jnp.where(lane // 8 == col, mid[s, pl.ds(col, rows, stride=cols), :], merged)
        turn[...] = jnp.concatenate([merged] * (LANES // rows), axis=0).T
        for chan in range(y_ref.shape[1]):
            plane = turn[pl.ds(chan, cols, stride=8), :]
            y_ref[s, chan] = plane[:, 0:rows] + out_bias[0:1, chan:chan + 1]
        return carry

    lax.fori_loop(0, samples, layer_last, 0)

    wait_for(st_first.at[pl.ds(1, peers_n - 1)], first_send.at[0])
    wait_for(row_first, first_send.at[1])
    wait_for(cs_first, first_send.at[2])
    wait_for(st_rest.at[:, :, pl.ds(1, len(plain))], send.at[0])
    wait_for(corner_out, send.at[1])
    wait_for(row_out, send.at[2])
    wait_for(col_out, send.at[3])


def solution(mesh):
    rows_n, cols_n = mesh.shape["sy"], mesh.shape["sx"]
    peers_n = rows_n * cols_n
    tile_spec = P("dp", "sy", "sx", None)
    replicated = P()

    def local_decode(act_in, norm_first, w_first, w_short, norm_rest, w_rest, bias_rest, w_out, bias_out):
        samples, rows, cols, wide = act_in.shape
        chans = w_short.shape[1]
        out_chans = w_out.shape[3]
        f32, bf16 = jnp.float32, jnp.bfloat16
        rest, plain_n = LAYERS - 1, peers_n - 9
        whole = pl.BlockSpec(memory_space=pltpu.VMEM)
        there = pl.BlockSpec(memory_space=pl.ANY)
        image = pl.pallas_call(
            functools.partial(decode_kernel, rows_n, cols_n),
            name="decode",
            out_shape=jax.ShapeDtypeStruct((samples, out_chans, cols, rows), f32),
            in_specs=[there, whole, there, there, whole, there, whole, whole, whole],
            out_specs=whole,
            scratch_shapes=[
                pltpu.VMEM(act_in.shape, bf16),
                pltpu.VMEM(w_first.shape, bf16),
                pltpu.VMEM(w_short.shape, bf16),
                pltpu.VMEM(w_rest.shape, bf16),
                pltpu.VMEM((9, chans, LANES), bf16),
                pltpu.VMEM((samples, rows * cols, chans), f32),
                pltpu.VMEM((samples, rows * cols, chans), f32),
                pltpu.VMEM((8, chans), f32),
                pltpu.VMEM((3, rows // 2 + 1, 2, cols, wide), bf16),
                pltpu.VMEM((3, rows // 2 + 1, cols, 2 * chans), bf16),
                pltpu.VMEM((2, 2, rows * 8, LANES), f32),
                pltpu.VMEM((2, rows, LANES), f32),
                pltpu.VMEM((2, rows, LANES), f32),
                pltpu.VMEM((LANES, LANES), f32),
                pltpu.VMEM((peers_n, samples, 2, wide), f32),
                pltpu.VMEM((6, samples, cols, wide), bf16),
                pltpu.VMEM((samples, 2, rows, wide), bf16),
                pltpu.VMEM((samples, 2, rows, wide), bf16),
                pltpu.VMEM((rest, samples, plain_n + 1, 2, chans), f32),
                pltpu.VMEM((rest, samples, 4, 4, chans), f32),
                pltpu.VMEM((rest, samples, 2, 8 + cols, chans), f32),
                pltpu.VMEM((rest, samples, 2, 8 + rows, chans), f32),
                pltpu.VMEM((rest, samples, 4, 4, chans), f32),
                pltpu.VMEM((rest, samples, 2, 8 + cols, chans), f32),
                pltpu.VMEM((rest, samples, 2, 8 + rows, chans), f32),
                pltpu.VMEM((plain_n + 8 + 16 + cols + rows, 2, chans), f32),
                pltpu.SemaphoreType.DMA((samples + 3,)),
                pltpu.SemaphoreType.DMA((2,)),
                pltpu.SemaphoreType.DMA((samples,)),
                pltpu.SemaphoreType.DMA((3,)),
                pltpu.SemaphoreType.DMA((rest, samples)),
                pltpu.SemaphoreType.DMA((4,)),
            ],
            compiler_params=pltpu.CompilerParams(collective_id=0, has_side_effects=True, vmem_limit_bytes=60 * 1024 * 1024),
        )(act_in, norm_first, w_first, w_short, norm_rest, w_rest, bias_rest, jnp.transpose(w_out, (0, 1, 3, 2)), bias_out.reshape(1, out_chans))
        return jnp.transpose(image, (0, 3, 2, 1))

    return jax.shard_map(local_decode, mesh=mesh, in_specs=(tile_spec,) + (replicated,) * 8, out_specs=tile_spec, check_vma=False)
```

```python
import functools

import jax
import jax.numpy as jnp
from jax import lax
from jax.experimental import pallas as pl
from jax.experimental.pallas import tpu as pltpu
from jax.sharding import PartitionSpec as P

GROUPS = 32
GN_EPS = 1e-6
MESH = pl.DeviceIdType.MESH
LANES = 128
ROW_BLOCK = 8
LAYERS = 7
CHUNKS = 4


def group_total(vec, per_group):
    lane = lax.broadcasted_iota(jnp.int32, vec.shape, 1) & (per_group - 1)
    parts = [vec]
    for dist in range(1, per_group):
        parts.append(jnp.where(lane >= dist, pltpu.roll(vec, dist, 1), pltpu.roll(vec, LANES - per_group + dist, 1)))
    while len(parts) > 1:
        parts = [parts[at] + parts[at + 1] if at + 1 < len(parts) else parts[at] for at in range(0, len(parts), 2)]
    return parts[0]


def far_first(rows_n, cols_n):
    every = [(a, b) for a in range(cols_n) for b in range(rows_n) if a or b]
    return sorted(every, key=lambda off: -(min(off[0], cols_n - off[0]) + min(off[1], rows_n - off[1]) / 2))


def decode_kernel(rows_n, cols_n, act_hbm, nf_hbm, wf_hbm, ws_hbm, nr_hbm, wr_hbm, br_hbm, wo_hbm, bo_hbm, y_ref,
                  act, norm_first, wf, ws, norm_rest, wr, bias_rest, wo_ref, bias_out, sums_first, total_first, wo, mid, hid, bias_rows, pad_first, pad_rest, slab, edge_l, edge_r, turn,
                  st_first, row_first, col_first, cs_first,
                  st_rest, corner_in, row_in, col_in, corner_out, row_out, col_out, whole_inbox,
                  load_sem, first_recv, col_recv, first_send, recv, send):
    samples, rows, cols, _ = act.shape
    pairs = rows // 2
    peers_n = rows_n * cols_n
    sx, sy = lax.axis_index("sx"), lax.axis_index("sy")
    at_x = [sx] + [lax.rem(sx + off, cols_n) for off in range(1, cols_n)]
    at_y = [sy] + [lax.rem(sy + off, rows_n) for off in range(1, rows_n)]
    order = far_first(rows_n, cols_n)
    has_l, has_r, has_t, has_b = sx > 0, sx < cols_n - 1, sy > 0, sy < rows_n - 1

    def device(off):
        return {"sx": at_x[off[0] % cols_n], "sy": at_y[off[1] % rows_n]}

    def wrap(off):
        return (off[0] % cols_n, off[1] % rows_n)

    corner_to = {wrap(off): at for at, off in enumerate(((-1, -1), (1, -1), (-1, 1), (1, 1)))}
    row_to = {wrap(off): at for at, off in enumerate(((0, -1), (0, 1)))}
    col_to = {wrap(off): at for at, off in enumerate(((-1, 0), (1, 0)))}
    plain = [off for off in order if off not in corner_to and off not in row_to and off not in col_to]

    loads = [pltpu.make_async_copy(act_hbm.at[s], act.at[s], load_sem.at[s]) for s in range(samples)]
    others = ((ws_hbm, ws), (br_hbm, bias_rest), (wo_hbm, wo_ref), (nf_hbm, norm_first), (wf_hbm, wf), (wr_hbm, wr), (nr_hbm, norm_rest), (bo_hbm, bias_out))
    for at, (src, dst) in enumerate(others):
        loads.append(pltpu.make_async_copy(src, dst, load_sem.at[samples + at]))
    for load in loads:
        load.start()
    barrier = pltpu.get_barrier_semaphore()
    for off in order:
        pl.semaphore_signal(barrier, inc=1, device_id=device(off), device_id_type=MESH)

    def remote(src, dst, send_to, recv_at, off):
        pltpu.make_async_remote_copy(src_ref=src, dst_ref=dst, send_sem=send_to, recv_sem=recv_at, device_id=device(off), device_id_type=MESH).start()

    def wait_for(ref, sem):
        pltpu.make_async_copy(ref, ref, sem).wait()

    def send_rest(at, s):
        sem = recv.at[at, s]
        for off in order:
            if off in corner_to:
                box = corner_to[off]
                remote(corner_out.at[at, s, box], corner_in.at[at, s, 3 - box], send.at[1], sem, off)
            elif off in row_to:
                box = row_to[off]
                remote(row_out.at[at, s, box], row_in.at[at, s, 1 - box], send.at[2], sem, off)
            elif off in col_to:
                box = col_to[off]
                remote(col_out.at[at, s, box], col_in.at[at, s, 1 - box], send.at[3], sem, off)
            else:
                remote(st_rest.at[at, s, 0], st_rest.at[at, s, 1 + plain.index(off)], send.at[0], sem, off)

    sub = lax.broadcasted_iota(jnp.int32, (1, 8, LANES), 1)
    first_sub, last_sub = sub == 0, sub == 7

    def affine(one, two, norm, per_group):
        count = rows * rows_n * cols * cols_n * per_group
        mean = group_total(one, per_group) / count
        square = group_total(two, per_group) / count
        scale = lax.rsqrt(square - mean * mean + GN_EPS) * jnp.broadcast_to(norm[0:1], (8, LANES))
        shift = jnp.broadcast_to(norm[1:2], (8, LANES)) - mean * scale
        return 0.5 * scale, 0.5 * shift

    first_group = 2 * LANES // GROUPS
    lane_in_group = lax.broadcasted_iota(jnp.int32, (8, LANES), 1) & (first_group - 1)

    def silu(x, scales):
        u = x * scales[0] + scales[1]
        return u + u * jnp.tanh(u)

    def spread(rows_of_cols, from_left, from_right):
        v0, v1 = rows_of_cols[:, 0], rows_of_cols[:, 1]
        r0, r1 = pltpu.roll(v0, 1, 1), pltpu.roll(v1, 1, 1)
        q0, q1 = pltpu.roll(v0, 7, 1), pltpu.roll(v1, 7, 1)
        shifted = (
            (jnp.where(first_sub, from_left, r0), jnp.where(first_sub, r0, r1)),
            (v0, v1),
            (jnp.where(last_sub, q1, q0), jnp.where(last_sub, from_right, q1)),
        )
        return [jnp.concatenate(pair, axis=1).astype(jnp.bfloat16) for pair in shifted]

    def edges(tile, scales, halo_cols):
        one_row = (scales[0][0:1], scales[1][0:1])
        edge_l[tile] = jnp.where(has_l, silu(halo_cols[0], one_row), 0.0)
        edge_r[tile] = jnp.where(has_r, silu(halo_cols[1], one_row), 0.0)

    def activate(block, tile, scales, halo_rows, corners, row_source, place):
        begin, end = max(0, 8 * block + 1), min(rows, 8 * block + 9)
        value = row_source(begin, end)
        lefts = [jnp.broadcast_to(edge_l[tile, r:r + 1, :], (8, LANES)) for r in range(begin, end)]
        rights = [jnp.broadcast_to(edge_r[tile, r:r + 1, :], (8, LANES)) for r in range(begin, end)]
        value = silu(value, scales)
        for at, has in enumerate((has_t, has_b)):
            if block == (-1, rows // 8 - 1)[at]:
                halo = jnp.where(has, silu(halo_rows[at].reshape(1, 2, 8, LANES), scales), 0.0)
                corner_l = jnp.where(jnp.logical_and(has, has_l), silu(corners[2 * at], scales), 0.0)
                corner_r = jnp.where(jnp.logical_and(has, has_r), silu(corners[2 * at + 1], scales), 0.0)
                where_at = 0 if at == 0 else len(lefts)
                value = jnp.concatenate([halo, value] if at == 0 else [value, halo], axis=0)
                lefts.insert(where_at, corner_l)
                rights.insert(where_at, corner_r)
        for off, part in enumerate(spread(value, jnp.stack(lefts), jnp.stack(rights))):
            place(off, tile, 4 * block + 1 if block >= 0 else 0, part.reshape(part.shape[0] // 2, 2, cols, LANES))

    def prepare_rest(at, s, source):
        wait_for(whole_inbox, recv.at[at, s])
        total = jnp.sum(st_rest[at, s], axis=0)
        for box in range(4):
            total = total + corner_in[at, s, box, 0:2]
        for box in range(2):
            total = total + (row_in[at, s, box, 0:2] + col_in[at, s, box, 0:2])
        one, two = (jnp.broadcast_to(total[which:which + 1], (8, LANES)) for which in range(2))
        scales = affine(one, two, norm_rest[at].astype(jnp.float32), LANES // GROUPS)

        def row_source(begin, end):
            return source[s, begin * cols:end * cols, :].reshape(end - begin, 2, 8, LANES)

        def place(off, tile, pair_at, value):
            for half in range(2):
                pad_rest[off, pair_at:pair_at + value.shape[0], :, half * LANES:(half + 1) * LANES] = value[:, half]

        edges(0, scales, [col_in[at, s, box, 8:8 + rows, :] for box in range(2)])
        halo_rows = [row_in[at, s, box, 8:8 + cols, :] for box in range(2)]
        corners = [jnp.broadcast_to(corner_in[at, s, box, 2:3, :], (8, LANES)) for box in range(4)]
        return lambda block: activate(block, 0, scales, halo_rows, corners, row_source, place)

    def prepare_first(s):
        wait_for(col_first.at[s], col_recv.at[s])
        norm = norm_first[...].astype(jnp.float32)

        def one_tile(tile):
            lanes = slice(tile * LANES, (tile + 1) * LANES)
            packed = jnp.broadcast_to(total_first[tile:tile + 1], (8, LANES))
            one, two = (jnp.where(lane_in_group == which * samples + s, packed, 0.0) for which in range(2))
            scales = affine(one, two, norm[:, lanes], first_group)

            def row_source(begin, end):
                return act[s, begin:end, :, lanes].astype(jnp.float32).reshape(end - begin, 2, 8, LANES)

            def place(off, tile, pair_at, value):
                pad_first[off, pair_at:pair_at + value.shape[0], :, :, lanes] = value

            edges(tile, scales, [col_first[s, box, :, lanes].astype(jnp.float32) for box in range(2)])
            halo_rows = [row_first[box, s, :, lanes].astype(jnp.float32) for box in (1, 4)]
            corners = []
            for box in (0, 2, 3, 5):
                row = row_first[box, s, :, lanes].astype(jnp.float32)
                corners.append(pltpu.roll(row[8:16], 1, 0) if box % 3 == 0 else pltpu.roll(row[0:8], 7, 0))
            return lambda block: activate(block, tile, scales, halo_rows, corners, row_source, place)

        tiles = [one_tile(tile) for tile in range(2)]
        return lambda block: [tile(block) for tile in tiles]

    zero = jnp.zeros((LANES, LANES), jnp.bfloat16)
    wide_zero = jnp.zeros((2 * LANES, LANES), jnp.bfloat16)

    def square_of(a, b, c, d):
        return jnp.concatenate([jnp.concatenate([a, b], axis=1), jnp.concatenate([c, d], axis=1)], axis=0)

    def conv_rest(weight, pair_from, pair_n):
        total = None
        for off in range(3):
            w0, w1, w2 = (weight(row_off, off) for row_off in range(3))
            for shift, tap in ((0, square_of(w0, zero, w1, w0)), (1, square_of(w2, w1, zero, w2))):
                lhs = pad_rest[off, pair_from + shift:pair_from + shift + pair_n].reshape(pair_n * cols, 2 * LANES)
                part = jnp.dot(lhs, tap, preferred_element_type=jnp.float32)
                total = part if total is None else total + part
        return total

    def conv_first(pair_from, pair_n):
        total = None
        for off in range(3):
            w0, w1, w2 = (wf[row_off, off] for row_off in range(3))
            for at, (a, b) in enumerate(((w0, wide_zero), (w1, w0), (w2, w1), (wide_zero, w2))):
                begin = pair_from + at // 2
                lhs = pad_first[off, begin:begin + pair_n, at % 2].reshape(pair_n * cols, 2 * LANES)
                part = jnp.dot(lhs, jnp.concatenate([a, b], axis=1), preferred_element_type=jnp.float32)
                total = part if total is None else total + part
        return total

    def in_chunks(block, conv, use):
        block(-1)
        done, per_chunk = 0, pairs // CHUNKS
        for chunk in range(CHUNKS):
            while 4 * done < (chunk + 1) * per_chunk:
                block(done)
                done += 1
            total = conv(chunk * per_chunk, per_chunk)
            halves = [total[:, half * LANES:(half + 1) * LANES].reshape(per_chunk, 1, cols, LANES) for half in range(2)]
            use(2 * chunk * per_chunk, jnp.concatenate(halves, axis=1).reshape(2 * per_chunk * cols, LANES))

    def finish(at, s, block, conv, bias, target, residual):
        acc = []

        def use(row, value):
            rows_in = value.shape[0] // cols
            value = value + bias
            if residual is not None:
                value = value + residual[s, row * cols:row * cols + value.shape[0], :]
            value = value.astype(jnp.bfloat16).astype(jnp.float32)
            target[s, row * cols:row * cols + value.shape[0], :] = value
            for edge, edge_row in enumerate((0, rows - 1)):
                if row <= edge_row < row + rows_in:
                    line = value[(edge_row - row) * cols:(edge_row - row + 1) * cols]
                    row_out[at, s, edge, 8:8 + cols, :] = line
                    corner_out[at, s, 2 * edge, 2:3, :] = line[0:1]
                    corner_out[at, s, 2 * edge + 1, 2:3, :] = line[cols - 1:cols]
            split = value.reshape(value.shape[0] // 16, 2, 8, LANES)
            acc.append([jnp.sum(split, axis=0), jnp.sum(split * split, axis=0)])

        in_chunks(block, conv, use)
        sums = []
        for which in range(2):
            part = acc[0][which]
            for more in acc[1:]:
                part = part + more[which]
            sums.append(jnp.sum(part[0] + part[1], axis=0, keepdims=True))
        sums = jnp.concatenate(sums, axis=0)
        st_rest[at, s, 0] = sums
        for box in range(4):
            corner_out[at, s, box, 0:2, :] = sums
        for box in range(2):
            col_out[at, s, box, 8:8 + rows, :] = target[s, pl.ds(box * (cols - 1), rows, stride=cols), :]
            row_out[at, s, box, 0:2, :] = sums
            col_out[at, s, box, 0:2, :] = sums
        send_rest(at, s)

    def first_sums(s, carry):
        wait_for(act.at[s], load_sem.at[s])

        def body(step, sums):
            sums = list(sums)
            for at in range(ROW_BLOCK):
                r = step * ROW_BLOCK + at
                for tile in range(2):
                    row = act[s, r, :, tile * LANES:(tile + 1) * LANES].astype(jnp.float32)
                    v0, v1 = row[0:8], row[8:16]
                    slab[0, tile, pl.ds(pl.multiple_of(r * 8, 8), 8), :] = v0
                    slab[1, tile, pl.ds(pl.multiple_of(r * 8, 8), 8), :] = v1
                    sums[2 * tile] = sums[2 * tile] + (v0 + v1)
                    sums[2 * tile + 1] = sums[2 * tile + 1] + (v0 * v0 + v1 * v1)
            return tuple(sums)

        sums = lax.fori_loop(0, rows // ROW_BLOCK, body, (jnp.zeros((8, LANES), jnp.float32),) * 4)
        for side in range(2):
            for tile in range(2):
                column = slab[side, tile, pl.ds(7 * side, rows, stride=8), :]
                cs_first[s, side, :, tile * LANES:(tile + 1) * LANES] = column.astype(jnp.bfloat16)
        for tile in range(2):
            for which in range(2):
                sums_first[tile, pl.ds(which * samples + s, 1), :] = jnp.sum(sums[2 * tile + which], axis=0, keepdims=True)
        return carry

    lax.fori_loop(0, samples, first_sums, 0)
    row_at = lax.broadcasted_iota(jnp.int32, (8, LANES), 0)
    for tile in range(2):
        grouped = jnp.where(row_at == lane_in_group, group_total(sums_first[tile], first_group), 0.0)
        st_first[0, tile:tile + 1, :] = jnp.sum(grouped, axis=0, keepdims=True)
    pl.semaphore_wait(barrier, peers_n - 1)
    for slot, off in enumerate(order):
        remote(st_first.at[0], st_first.at[slot + 1], first_send.at[0], first_recv.at[0], off)
    for row, y_off, base in ((0, -1, 3), (rows - 1, 1, 0)):
        for x_off, at in ((-1, 2), (0, 1), (1, 0)):
            remote(act.at[:, row], row_first.at[base + at], first_send.at[1], first_recv.at[1], (x_off, y_off))

    def first_columns(s, carry):
        for off, box in col_to.items():
            remote(cs_first.at[s, box], col_first.at[s, 1 - box], first_send.at[2], col_recv.at[s], off)
        return carry

    lax.fori_loop(0, samples, first_columns, 0)

    for load in loads[samples:samples + 3]:
        load.wait()
    bias = bias_rest[...].astype(jnp.float32)

    def shortcut(s, carry):
        flat = act[s].reshape(rows * cols, 2 * LANES)
        hid[s] = jnp.dot(flat, ws[...], preferred_element_type=jnp.float32) + bias[6:7]
        return carry

    lax.fori_loop(0, samples, shortcut, 0)
    for tap in range(9):
        three = wo_ref[tap // 3, tap % 3].astype(jnp.float32)
        eight = jnp.concatenate([three, jnp.zeros((8 - three.shape[0], LANES), jnp.float32)], axis=0)
        wo[tap] = jnp.concatenate([eight] * 16, axis=0).T.astype(jnp.bfloat16)
    for load in loads[samples + 3:]:
        load.wait()
    wait_for(st_first.at[pl.ds(1, peers_n - 1)], first_recv.at[0])
    total_first[0:2, :] = jnp.sum(st_first[...], axis=0)
    wait_for(row_first, first_recv.at[1])

    def layer_first(s, carry):
        finish(0, s, prepare_first(s), conv_first, bias[0:1], mid, None)
        return carry

    lax.fori_loop(0, samples, layer_first, 0)

    def layer_rest(layer, source, target, residual):
        def one_sample(s, carry):
            block = prepare_rest(layer - 1, s, source)
            conv = functools.partial(conv_rest, lambda row_off, off: wr[layer - 1, row_off, off])
            finish(layer, s, block, conv, bias_rows[pl.ds(layer, 1), :], target, residual)
            return carry

        lax.fori_loop(0, samples, one_sample, 0)

    def layer_pair(step, carry):
        layer_rest(2 * step + 1, mid, hid, hid)
        layer_rest(2 * step + 2, hid, mid, None)
        return carry

    bias_rows[0:bias.shape[0], :] = bias
    lax.fori_loop(0, (LAYERS - 2) // 2, layer_pair, 0)
    layer_rest(LAYERS - 2, mid, hid, hid)

    lane = lax.broadcasted_iota(jnp.int32, (rows, LANES), 1)
    out_bias = bias_out[...].astype(jnp.float32)

    def layer_last(s, carry):
        def use(row, value):
            mid[s, row * cols:row * cols + value.shape[0], :] = value

        in_chunks(prepare_rest(LAYERS - 2, s, hid), functools.partial(conv_rest, lambda row_off, off: wo[3 * row_off + off]), use)
        merged = mid[s, pl.ds(0, rows, stride=cols), :]
        for col in range(1, cols):
            merged = jnp.where(lane // 8 == col, mid[s, pl.ds(col, rows, stride=cols), :], merged)
        turn[...] = jnp.concatenate([merged] * (LANES // rows), axis=0).T
        for chan in range(y_ref.shape[1]):
            plane = turn[pl.ds(chan, cols, stride=8), :]
            y_ref[s, chan] = plane[:, 0:rows] + out_bias[0:1, chan:chan + 1]
        return carry

    lax.fori_loop(0, samples, layer_last, 0)

    wait_for(st_first.at[pl.ds(1, peers_n - 1)], first_send.at[0])
    wait_for(row_first, first_send.at[1])
    wait_for(cs_first, first_send.at[2])
    wait_for(st_rest.at[:, :, pl.ds(1, len(plain))], send.at[0])
    wait_for(corner_out, send.at[1])
    wait_for(row_out, send.at[2])
    wait_for(col_out, send.at[3])


def solution(mesh):
    rows_n, cols_n = mesh.shape["sy"], mesh.shape["sx"]
    peers_n = rows_n * cols_n
    tile_spec = P("dp", "sy", "sx", None)
    replicated = P()

    def local_decode(act_in, norm_first, w_first, w_short, norm_rest, w_rest, bias_rest, w_out, bias_out):
        samples, rows, cols, wide = act_in.shape
        chans = w_short.shape[1]
        out_chans = w_out.shape[3]
        f32, bf16 = jnp.float32, jnp.bfloat16
        rest, plain_n = LAYERS - 1, peers_n - 9
        whole = pl.BlockSpec(memory_space=pltpu.VMEM)
        there = pl.BlockSpec(memory_space=pltpu.HBM)
        image = pl.pallas_call(
            functools.partial(decode_kernel, rows_n, cols_n),
            name="decode",
            out_shape=jax.ShapeDtypeStruct((samples, out_chans, cols, rows), f32),
            in_specs=[there] * 9,
            out_specs=whole,
            scratch_shapes=[
                pltpu.VMEM(act_in.shape, bf16),
                pltpu.VMEM(norm_first.shape, bf16),
                pltpu.VMEM(w_first.shape, bf16),
                pltpu.VMEM(w_short.shape, bf16),
                pltpu.VMEM(norm_rest.shape, bf16),
                pltpu.VMEM(w_rest.shape, bf16),
                pltpu.VMEM(bias_rest.shape, bf16),
                pltpu.VMEM((3, 3, out_chans, chans), bf16),
                pltpu.VMEM((1, out_chans), bf16),
                pltpu.VMEM((2, 8, LANES), f32),
                pltpu.VMEM((8, LANES), f32),
                pltpu.VMEM((9, chans, LANES), bf16),
                pltpu.VMEM((samples, rows * cols, chans), f32),
                pltpu.VMEM((samples, rows * cols, chans), f32),
                pltpu.VMEM((8, chans), f32),
                pltpu.VMEM((3, rows // 2 + 1, 2, cols, wide), bf16),
                pltpu.VMEM((3, rows // 2 + 1, cols, 2 * chans), bf16),
                pltpu.VMEM((2, 2, rows * 8, LANES), f32),
                pltpu.VMEM((2, rows, LANES), f32),
                pltpu.VMEM((2, rows, LANES), f32),
                pltpu.VMEM((LANES, LANES), f32),
                pltpu.VMEM((peers_n, 2, LANES), f32),
                pltpu.VMEM((6, samples, cols, wide), bf16),
                pltpu.VMEM((samples, 2, rows, wide), bf16),
                pltpu.VMEM((samples, 2, rows, wide), bf16),
                pltpu.VMEM((rest, samples, plain_n + 1, 2, chans), f32),
                pltpu.VMEM((rest, samples, 4, 4, chans), f32),
                pltpu.VMEM((rest, samples, 2, 8 + cols, chans), f32),
                pltpu.VMEM((rest, samples, 2, 8 + rows, chans), f32),
                pltpu.VMEM((rest, samples, 4, 4, chans), f32),
                pltpu.VMEM((rest, samples, 2, 8 + cols, chans), f32),
                pltpu.VMEM((rest, samples, 2, 8 + rows, chans), f32),
                pltpu.VMEM((plain_n + 8 + 16 + cols + rows, 2, chans), f32),
                pltpu.SemaphoreType.DMA((samples + 8,)),
                pltpu.SemaphoreType.DMA((2,)),
                pltpu.SemaphoreType.DMA((samples,)),
                pltpu.SemaphoreType.DMA((3,)),
                pltpu.SemaphoreType.DMA((rest, samples)),
                pltpu.SemaphoreType.DMA((4,)),
            ],
            compiler_params=pltpu.CompilerParams(collective_id=0, has_side_effects=True, vmem_limit_bytes=60 * 1024 * 1024),
        )(act_in, norm_first, w_first, w_short, norm_rest, w_rest, bias_rest, jnp.transpose(w_out, (0, 1, 3, 2)), bias_out.reshape(1, out_chans))
        return jnp.transpose(image, (0, 3, 2, 1))

    return jax.shard_map(local_decode, mesh=mesh, in_specs=(tile_spec,) + (replicated,) * 8, out_specs=tile_spec, check_vma=False)
```

```python
import functools

import jax
import jax.numpy as jnp
from jax import lax
from jax.experimental import pallas as pl
from jax.experimental.pallas import tpu as pltpu
from jax.sharding import PartitionSpec as P

GROUPS = 32
GN_EPS = 1e-6
MESH = pl.DeviceIdType.MESH
LANES = 128
ROW_BLOCK = 8
LAYERS = 7
CHUNKS = 4


def group_total(vec, per_group):
    lane = lax.broadcasted_iota(jnp.int32, vec.shape, 1) & (per_group - 1)
    parts = [vec]
    for dist in range(1, per_group):
        parts.append(jnp.where(lane >= dist, pltpu.roll(vec, dist, 1), pltpu.roll(vec, LANES - per_group + dist, 1)))
    while len(parts) > 1:
        parts = [parts[at] + parts[at + 1] if at + 1 < len(parts) else parts[at] for at in range(0, len(parts), 2)]
    return parts[0]


def far_first(rows_n, cols_n):
    every = [(a, b) for a in range(cols_n) for b in range(rows_n) if a or b]
    return sorted(every, key=lambda off: -(min(off[0], cols_n - off[0]) + min(off[1], rows_n - off[1]) / 2))


def decode_kernel(rows_n, cols_n, act_hbm, nf_hbm, wf_hbm, ws_hbm, nr_hbm, wr_hbm, br_hbm, wo_hbm, bo_hbm, y_ref,
                  act, norm_first, wf, ws, norm_rest, wr, bias_rest, wo_ref, bias_out, sums_first, total_first, wo, mid, hid, bias_rows, pad_first, pad_rest, slab, edge_l, edge_r, turn,
                  st_first, row_first, col_first, cs_first,
                  st_rest, corner_in, row_in, col_in, corner_out, row_out, col_out, whole_inbox,
                  load_sem, first_recv, col_recv, first_send, recv, send):
    samples, rows, cols, _ = act.shape
    pairs = rows // 2
    peers_n = rows_n * cols_n
    sx, sy = lax.axis_index("sx"), lax.axis_index("sy")
    at_x = [sx] + [lax.rem(sx + off, cols_n) for off in range(1, cols_n)]
    at_y = [sy] + [lax.rem(sy + off, rows_n) for off in range(1, rows_n)]
    order = far_first(rows_n, cols_n)
    has_l, has_r, has_t, has_b = sx > 0, sx < cols_n - 1, sy > 0, sy < rows_n - 1

    def device(off):
        return {"sx": at_x[off[0] % cols_n], "sy": at_y[off[1] % rows_n]}

    def wrap(off):
        return (off[0] % cols_n, off[1] % rows_n)

    corner_to = {wrap(off): at for at, off in enumerate(((-1, -1), (1, -1), (-1, 1), (1, 1)))}
    row_to = {wrap(off): at for at, off in enumerate(((0, -1), (0, 1)))}
    col_to = {wrap(off): at for at, off in enumerate(((-1, 0), (1, 0)))}
    plain = [off for off in order if off not in corner_to and off not in row_to and off not in col_to]

    loads = [pltpu.make_async_copy(act_hbm.at[s], act.at[s], load_sem.at[s]) for s in range(samples)]
    others = ((ws_hbm, ws), (br_hbm, bias_rest), (wo_hbm, wo_ref), (nf_hbm, norm_first), (wf_hbm, wf), (wr_hbm, wr), (nr_hbm, norm_rest), (bo_hbm, bias_out))
    for at, (src, dst) in enumerate(others):
        loads.append(pltpu.make_async_copy(src, dst, load_sem.at[samples + at]))
    for load in loads[:samples]:
        load.start()
    barrier = pltpu.get_barrier_semaphore()
    for off in order:
        pl.semaphore_signal(barrier, inc=1, device_id=device(off), device_id_type=MESH)

    def remote(src, dst, send_to, recv_at, off):
        pltpu.make_async_remote_copy(src_ref=src, dst_ref=dst, send_sem=send_to, recv_sem=recv_at, device_id=device(off), device_id_type=MESH).start()

    def wait_for(ref, sem):
        pltpu.make_async_copy(ref, ref, sem).wait()

    def send_rest(at, s):
        sem = recv.at[at, s]
        for off in order:
            if off in corner_to:
                box = corner_to[off]
                remote(corner_out.at[at, s, box], corner_in.at[at, s, 3 - box], send.at[1], sem, off)
            elif off in row_to:
                box = row_to[off]
                remote(row_out.at[at, s, box], row_in.at[at, s, 1 - box], send.at[2], sem, off)
            elif off in col_to:
                box = col_to[off]
                remote(col_out.at[at, s, box], col_in.at[at, s, 1 - box], send.at[3], sem, off)
            else:
                remote(st_rest.at[at, s, 0], st_rest.at[at, s, 1 + plain.index(off)], send.at[0], sem, off)

    sub = lax.broadcasted_iota(jnp.int32, (1, 8, LANES), 1)
    first_sub, last_sub = sub == 0, sub == 7

    def tree_sum(stack):
        while stack.shape[0] > 1:
            half = stack.shape[0] // 2
            folded = stack[:half] + stack[half:2 * half]
            stack = folded if stack.shape[0] == 2 * half else jnp.concatenate([folded[:1] + stack[2 * half:], folded[1:]], axis=0) if half > 1 else folded + stack[2 * half:]
        return stack[0]

    def affine(one, two, norm, per_group):
        count = rows * rows_n * cols * cols_n * per_group
        mean = group_total(one, per_group) / count
        square = group_total(two, per_group) / count
        scale = lax.rsqrt(square - mean * mean + GN_EPS) * jnp.broadcast_to(norm[0:1], (8, LANES))
        shift = jnp.broadcast_to(norm[1:2], (8, LANES)) - mean * scale
        return 0.5 * scale, 0.5 * shift

    first_group = 2 * LANES // GROUPS
    lane_in_group = lax.broadcasted_iota(jnp.int32, (8, LANES), 1) & (first_group - 1)

    def silu(x, scales):
        u = x * scales[0] + scales[1]
        return u + u * jnp.tanh(u)

    def spread(rows_of_cols, from_left, from_right):
        v0, v1 = rows_of_cols[:, 0], rows_of_cols[:, 1]
        r0, r1 = pltpu.roll(v0, 1, 1), pltpu.roll(v1, 1, 1)
        q0, q1 = pltpu.roll(v0, 7, 1), pltpu.roll(v1, 7, 1)
        shifted = (
            (jnp.where(first_sub, from_left, r0), jnp.where(first_sub, r0, r1)),
            (v0, v1),
            (jnp.where(last_sub, q1, q0), jnp.where(last_sub, from_right, q1)),
        )
        return [jnp.concatenate(pair, axis=1).astype(jnp.bfloat16) for pair in shifted]

    def edges(tile, scales, halo_cols):
        one_row = (scales[0][0:1], scales[1][0:1])
        edge_l[tile] = jnp.where(has_l, silu(halo_cols[0], one_row), 0.0)
        edge_r[tile] = jnp.where(has_r, silu(halo_cols[1], one_row), 0.0)

    def activate(block, tile, scales, halo_rows, corners, row_source, place):
        begin, end = max(0, 8 * block + 1), min(rows, 8 * block + 9)
        value = row_source(begin, end)
        lefts = [jnp.broadcast_to(edge_l[tile, r:r + 1, :], (8, LANES)) for r in range(begin, end)]
        rights = [jnp.broadcast_to(edge_r[tile, r:r + 1, :], (8, LANES)) for r in range(begin, end)]
        value = silu(value, scales)
        for at, has in enumerate((has_t, has_b)):
            if block == (-1, rows // 8 - 1)[at]:
                halo = jnp.where(has, silu(halo_rows[at].reshape(1, 2, 8, LANES), scales), 0.0)
                corner_l = jnp.where(jnp.logical_and(has, has_l), silu(corners[2 * at], scales), 0.0)
                corner_r = jnp.where(jnp.logical_and(has, has_r), silu(corners[2 * at + 1], scales), 0.0)
                where_at = 0 if at == 0 else len(lefts)
                value = jnp.concatenate([halo, value] if at == 0 else [value, halo], axis=0)
                lefts.insert(where_at, corner_l)
                rights.insert(where_at, corner_r)
        for off, part in enumerate(spread(value, jnp.stack(lefts), jnp.stack(rights))):
            place(off, tile, 4 * block + 1 if block >= 0 else 0, part.reshape(part.shape[0] // 2, 2, cols, LANES))

    def prepare_rest(at, s, source):
        wait_for(whole_inbox, recv.at[at, s])
        slots = [st_rest[at, s], corner_in[at, s, :, 0:2], row_in[at, s, :, 0:2], col_in[at, s, :, 0:2]]
        total = tree_sum(jnp.concatenate(slots, axis=0))
        one, two = (jnp.broadcast_to(total[which:which + 1], (8, LANES)) for which in range(2))
        scales = affine(one, two, norm_rest[at].astype(jnp.float32), LANES // GROUPS)

        def row_source(begin, end):
            return source[s, begin * cols:end * cols, :].reshape(end - begin, 2, 8, LANES)

        def place(off, tile, pair_at, value):
            for half in range(2):
                pad_rest[off, pair_at:pair_at + value.shape[0], :, half * LANES:(half + 1) * LANES] = value[:, half]

        edges(0, scales, [col_in[at, s, box, 8:8 + rows, :] for box in range(2)])
        halo_rows = [row_in[at, s, box, 8:8 + cols, :] for box in range(2)]
        corners = [jnp.broadcast_to(corner_in[at, s, box, 2:3, :], (8, LANES)) for box in range(4)]
        return lambda block: activate(block, 0, scales, halo_rows, corners, row_source, place)

    def prepare_first(s):
        wait_for(col_first.at[s], col_recv.at[s])
        norm = norm_first[...].astype(jnp.float32)

        def one_tile(tile):
            lanes = slice(tile * LANES, (tile + 1) * LANES)
            packed = jnp.broadcast_to(total_first[tile:tile + 1], (8, LANES))
            one, two = (jnp.where(lane_in_group == which * samples + s, packed, 0.0) for which in range(2))
            scales = affine(one, two, norm[:, lanes], first_group)

            def row_source(begin, end):
                return act[s, begin:end, :, lanes].astype(jnp.float32).reshape(end - begin, 2, 8, LANES)

            def place(off, tile, pair_at, value):
                pad_first[off, pair_at:pair_at + value.shape[0], :, :, lanes] = value

            edges(tile, scales, [col_first[s, box, :, lanes].astype(jnp.float32) for box in range(2)])
            halo_rows = [row_first[box, s, :, lanes].astype(jnp.float32) for box in (1, 4)]
            corners = []
            for box in (0, 2, 3, 5):
                row = row_first[box, s, :, lanes].astype(jnp.float32)
                corners.append(pltpu.roll(row[8:16], 1, 0) if box % 3 == 0 else pltpu.roll(row[0:8], 7, 0))
            return lambda block: activate(block, tile, scales, halo_rows, corners, row_source, place)

        tiles = [one_tile(tile) for tile in range(2)]
        return lambda block: [tile(block) for tile in tiles]

    zero = jnp.zeros((LANES, LANES), jnp.bfloat16)
    wide_zero = jnp.zeros((2 * LANES, LANES), jnp.bfloat16)

    def square_of(a, b, c, d):
        return jnp.concatenate([jnp.concatenate([a, b], axis=1), jnp.concatenate([c, d], axis=1)], axis=0)

    def conv_rest(weight, pair_from, pair_n):
        total = None
        for off in range(3):
            w0, w1, w2 = (weight(row_off, off) for row_off in range(3))
            for shift, tap in ((0, square_of(w0, zero, w1, w0)), (1, square_of(w2, w1, zero, w2))):
                lhs = pad_rest[off, pair_from + shift:pair_from + shift + pair_n].reshape(pair_n * cols, 2 * LANES)
                part = jnp.dot(lhs, tap, preferred_element_type=jnp.float32)
                total = part if total is None else total + part
        return total

    def conv_first(pair_from, pair_n):
        total = None
        for off in range(3):
            w0, w1, w2 = (wf[row_off, off] for row_off in range(3))
            for at, (a, b) in enumerate(((w0, wide_zero), (w1, w0), (w2, w1), (wide_zero, w2))):
                begin = pair_from + at // 2
                lhs = pad_first[off, begin:begin + pair_n, at % 2].reshape(pair_n * cols, 2 * LANES)
                part = jnp.dot(lhs, jnp.concatenate([a, b], axis=1), preferred_element_type=jnp.float32)
                total = part if total is None else total + part
        return total

    def in_chunks(block, conv, use):
        block(-1)
        done, per_chunk = 0, pairs // CHUNKS
        for chunk in range(CHUNKS):
            while 4 * done < (chunk + 1) * per_chunk:
                block(done)
                done += 1
            total = conv(chunk * per_chunk, per_chunk)
            halves = [total[:, half * LANES:(half + 1) * LANES].reshape(per_chunk, 1, cols, LANES) for half in range(2)]
            use(2 * chunk * per_chunk, jnp.concatenate(halves, axis=1).reshape(2 * per_chunk * cols, LANES))

    def finish(at, s, block, conv, bias, target, residual):
        acc = []

        def use(row, value):
            rows_in = value.shape[0] // cols
            value = value + bias
            if residual is not None:
                value = value + residual[s, row * cols:row * cols + value.shape[0], :]
            value = value.astype(jnp.bfloat16).astype(jnp.float32)
            target[s, row * cols:row * cols + value.shape[0], :] = value
            for edge, edge_row in enumerate((0, rows - 1)):
                if row <= edge_row < row + rows_in:
                    line = value[(edge_row - row) * cols:(edge_row - row + 1) * cols]
                    row_out[at, s, edge, 8:8 + cols, :] = line
                    corner_out[at, s, 2 * edge, 2:3, :] = line[0:1]
                    corner_out[at, s, 2 * edge + 1, 2:3, :] = line[cols - 1:cols]
            split = value.reshape(value.shape[0] // 16, 2, 8, LANES)
            acc.append([jnp.sum(split, axis=0), jnp.sum(split * split, axis=0)])

        in_chunks(block, conv, use)
        sums = []
        for which in range(2):
            part = acc[0][which]
            for more in acc[1:]:
                part = part + more[which]
            sums.append(jnp.sum(part[0] + part[1], axis=0, keepdims=True))
        sums = jnp.concatenate(sums, axis=0)
        st_rest[at, s, 0] = sums
        for box in range(4):
            corner_out[at, s, box, 0:2, :] = sums
        for box in range(2):
            col_out[at, s, box, 8:8 + rows, :] = target[s, pl.ds(box * (cols - 1), rows, stride=cols), :]
            row_out[at, s, box, 0:2, :] = sums
            col_out[at, s, box, 0:2, :] = sums
        send_rest(at, s)

    def first_sums(s, carry):
        wait_for(act.at[s], load_sem.at[s])

        def body(step, sums):
            sums = list(sums)
            for at in range(ROW_BLOCK):
                r = step * ROW_BLOCK + at
                for tile in range(2):
                    row = act[s, r, :, tile * LANES:(tile + 1) * LANES].astype(jnp.float32)
                    v0, v1 = row[0:8], row[8:16]
                    slab[0, tile, pl.ds(pl.multiple_of(r * 8, 8), 8), :] = v0
                    slab[1, tile, pl.ds(pl.multiple_of(r * 8, 8), 8), :] = v1
                    sums[2 * tile] = sums[2 * tile] + (v0 + v1)
                    sums[2 * tile + 1] = sums[2 * tile + 1] + (v0 * v0 + v1 * v1)
            return tuple(sums)

        sums = lax.fori_loop(0, rows // ROW_BLOCK, body, (jnp.zeros((8, LANES), jnp.float32),) * 4)
        for side in range(2):
            for tile in range(2):
                column = slab[side, tile, pl.ds(7 * side, rows, stride=8), :]
                cs_first[s, side, :, tile * LANES:(tile + 1) * LANES] = column.astype(jnp.bfloat16)
        for tile in range(2):
            for which in range(2):
                sums_first[tile, pl.ds(which * samples + s, 1), :] = jnp.sum(sums[2 * tile + which], axis=0, keepdims=True)
        return carry

    lax.fori_loop(0, samples, first_sums, 0)
    for load in loads[samples:]:
        load.start()
    row_at = lax.broadcasted_iota(jnp.int32, (8, LANES), 0)
    for tile in range(2):
        grouped = jnp.where(row_at == lane_in_group, group_total(sums_first[tile], first_group), 0.0)
        st_first[0, tile:tile + 1, :] = jnp.sum(grouped, axis=0, keepdims=True)
    pl.semaphore_wait(barrier, peers_n - 1)
    for slot, off in enumerate(order):
        remote(st_first.at[0], st_first.at[slot + 1], first_send.at[0], first_recv.at[0], off)
    for row, y_off, base in ((0, -1, 3), (rows - 1, 1, 0)):
        for x_off, at in ((-1, 2), (0, 1), (1, 0)):
            remote(act.at[:, row], row_first.at[base + at], first_send.at[1], first_recv.at[1], (x_off, y_off))

    def first_columns(s, carry):
        for off, box in col_to.items():
            remote(cs_first.at[s, box], col_first.at[s, 1 - box], first_send.at[2], col_recv.at[s], off)
        return carry

    lax.fori_loop(0, samples, first_columns, 0)

    for load in loads[samples:samples + 3]:
        load.wait()
    bias = bias_rest[...].astype(jnp.float32)

    def shortcut(s, carry):
        flat = act[s].reshape(rows * cols, 2 * LANES)
        hid[s] = jnp.dot(flat, ws[...], preferred_element_type=jnp.float32) + bias[6:7]
        return carry

    lax.fori_loop(0, samples, shortcut, 0)
    for tap in range(9):
        three = wo_ref[tap // 3, tap % 3].astype(jnp.float32)
        eight = jnp.concatenate([three, jnp.zeros((8 - three.shape[0], LANES), jnp.float32)], axis=0)
        wo[tap] = jnp.concatenate([eight] * 16, axis=0).T.astype(jnp.bfloat16)
    for load in loads[samples + 3:]:
        load.wait()
    wait_for(st_first.at[pl.ds(1, peers_n - 1)], first_recv.at[0])
    total_first[0:2, :] = jnp.sum(st_first[...], axis=0)
    wait_for(row_first, first_recv.at[1])

    def layer_first(s, carry):
        finish(0, s, prepare_first(s), conv_first, bias[0:1], mid, None)
        return carry

    lax.fori_loop(0, samples, layer_first, 0)

    def layer_rest(layer, source, target, residual):
        def one_sample(s, carry):
            block = prepare_rest(layer - 1, s, source)
            conv = functools.partial(conv_rest, lambda row_off, off: wr[layer - 1, row_off, off])
            finish(layer, s, block, conv, bias_rows[pl.ds(layer, 1), :], target, residual)
            return carry

        lax.fori_loop(0, samples, one_sample, 0)

    def layer_pair(step, carry):
        layer_rest(2 * step + 1, mid, hid, hid)
        layer_rest(2 * step + 2, hid, mid, None)
        return carry

    bias_rows[0:bias.shape[0], :] = bias
    lax.fori_loop(0, (LAYERS - 2) // 2, layer_pair, 0)
    layer_rest(LAYERS - 2, mid, hid, hid)

    lane = lax.broadcasted_iota(jnp.int32, (rows, LANES), 1)
    out_bias = bias_out[...].astype(jnp.float32)

    def layer_last(s, carry):
        def use(row, value):
            mid[s, row * cols:row * cols + value.shape[0], :] = value

        in_chunks(prepare_rest(LAYERS - 2, s, hid), functools.partial(conv_rest, lambda row_off, off: wo[3 * row_off + off]), use)
        merged = mid[s, pl.ds(0, rows, stride=cols), :]
        for col in range(1, cols):
            merged = jnp.where(lane // 8 == col, mid[s, pl.ds(col, rows, stride=cols), :], merged)
        turn[...] = jnp.concatenate([merged] * (LANES // rows), axis=0).T
        for chan in range(y_ref.shape[1]):
            plane = turn[pl.ds(chan, cols, stride=8), :]
            y_ref[s, chan] = plane[:, 0:rows] + out_bias[0:1, chan:chan + 1]
        return carry

    lax.fori_loop(0, samples, layer_last, 0)

    wait_for(st_first.at[pl.ds(1, peers_n - 1)], first_send.at[0])
    wait_for(row_first, first_send.at[1])
    wait_for(cs_first, first_send.at[2])
    wait_for(st_rest.at[:, :, pl.ds(1, len(plain))], send.at[0])
    wait_for(corner_out, send.at[1])
    wait_for(row_out, send.at[2])
    wait_for(col_out, send.at[3])


def solution(mesh):
    rows_n, cols_n = mesh.shape["sy"], mesh.shape["sx"]
    peers_n = rows_n * cols_n
    tile_spec = P("dp", "sy", "sx", None)
    replicated = P()

    def local_decode(act_in, norm_first, w_first, w_short, norm_rest, w_rest, bias_rest, w_out, bias_out):
        samples, rows, cols, wide = act_in.shape
        chans = w_short.shape[1]
        out_chans = w_out.shape[3]
        f32, bf16 = jnp.float32, jnp.bfloat16
        rest, plain_n = LAYERS - 1, peers_n - 9
        whole = pl.BlockSpec(memory_space=pltpu.VMEM)
        there = pl.BlockSpec(memory_space=pltpu.HBM)
        image = pl.pallas_call(
            functools.partial(decode_kernel, rows_n, cols_n),
            name="decode",
            out_shape=jax.ShapeDtypeStruct((samples, out_chans, cols, rows), f32),
            in_specs=[there] * 9,
            out_specs=whole,
            scratch_shapes=[
                pltpu.VMEM(act_in.shape, bf16),
                pltpu.VMEM(norm_first.shape, bf16),
                pltpu.VMEM(w_first.shape, bf16),
                pltpu.VMEM(w_short.shape, bf16),
                pltpu.VMEM(norm_rest.shape, bf16),
                pltpu.VMEM(w_rest.shape, bf16),
                pltpu.VMEM(bias_rest.shape, bf16),
                pltpu.VMEM((3, 3, out_chans, chans), bf16),
                pltpu.VMEM((1, out_chans), bf16),
                pltpu.VMEM((2, 8, LANES), f32),
                pltpu.VMEM((8, LANES), f32),
                pltpu.VMEM((9, chans, LANES), bf16),
                pltpu.VMEM((samples, rows * cols, chans), f32),
                pltpu.VMEM((samples, rows * cols, chans), f32),
                pltpu.VMEM((8, chans), f32),
                pltpu.VMEM((3, rows // 2 + 1, 2, cols, wide), bf16),
                pltpu.VMEM((3, rows // 2 + 1, cols, 2 * chans), bf16),
                pltpu.VMEM((2, 2, rows * 8, LANES), f32),
                pltpu.VMEM((2, rows, LANES), f32),
                pltpu.VMEM((2, rows, LANES), f32),
                pltpu.VMEM((LANES, LANES), f32),
                pltpu.VMEM((peers_n, 2, LANES), f32),
                pltpu.VMEM((6, samples, cols, wide), bf16),
                pltpu.VMEM((samples, 2, rows, wide), bf16),
                pltpu.VMEM((samples, 2, rows, wide), bf16),
                pltpu.VMEM((rest, samples, plain_n + 1, 2, chans), f32),
                pltpu.VMEM((rest, samples, 4, 4, chans), f32),
                pltpu.VMEM((rest, samples, 2, 8 + cols, chans), f32),
                pltpu.VMEM((rest, samples, 2, 8 + rows, chans), f32),
                pltpu.VMEM((rest, samples, 4, 4, chans), f32),
                pltpu.VMEM((rest, samples, 2, 8 + cols, chans), f32),
                pltpu.VMEM((rest, samples, 2, 8 + rows, chans), f32),
                pltpu.VMEM((plain_n + 8 + 16 + cols + rows, 2, chans), f32),
                pltpu.SemaphoreType.DMA((samples + 8,)),
                pltpu.SemaphoreType.DMA((2,)),
                pltpu.SemaphoreType.DMA((samples,)),
                pltpu.SemaphoreType.DMA((3,)),
                pltpu.SemaphoreType.DMA((rest, samples)),
                pltpu.SemaphoreType.DMA((4,)),
            ],
            compiler_params=pltpu.CompilerParams(collective_id=0, has_side_effects=True, vmem_limit_bytes=48 * 1024 * 1024),
        )(*[pltpu.with_memory_space_constraint(x, pltpu.HBM) for x in (act_in, norm_first, w_first, w_short, norm_rest, w_rest, bias_rest, jnp.transpose(w_out, (0, 1, 3, 2)), bias_out.reshape(1, out_chans))])
        return jnp.transpose(image, (0, 3, 2, 1))

    return jax.shard_map(local_decode, mesh=mesh, in_specs=(tile_spec,) + (replicated,) * 8, out_specs=tile_spec, check_vma=False)
```

```python
import functools

import jax
import jax.numpy as jnp
from jax import lax
from jax.experimental import pallas as pl
from jax.experimental.pallas import tpu as pltpu
from jax.sharding import PartitionSpec as P

GROUPS = 32
GN_EPS = 1e-6
MESH = pl.DeviceIdType.MESH
LANES = 128
ROW_BLOCK = 2
LAYERS = 7
CHUNKS = 4
BLOCK = 2


def group_total(vec, per_group):
    lane = lax.broadcasted_iota(jnp.int32, vec.shape, 1) & (per_group - 1)
    parts = [vec]
    for dist in range(1, per_group):
        parts.append(jnp.where(lane >= dist, pltpu.roll(vec, dist, 1), pltpu.roll(vec, LANES - per_group + dist, 1)))
    while len(parts) > 1:
        parts = [parts[at] + parts[at + 1] if at + 1 < len(parts) else parts[at] for at in range(0, len(parts), 2)]
    return parts[0]


def far_first(rows_n, cols_n):
    every = [(a, b) for a in range(cols_n) for b in range(rows_n) if a or b]
    return sorted(every, key=lambda off: -(min(off[0], cols_n - off[0]) + min(off[1], rows_n - off[1]) / 2))


def decode_kernel(rows_n, cols_n, act_hbm, nf_hbm, wf_hbm, ws_hbm, nr_hbm, wr_hbm, br_hbm, wo_hbm, bo_hbm, y_ref,
                  act, norm_first, wf, ws, norm_rest, wr, bias_rest, wo_ref, bias_out, sums_first, total_first, wo, mid, hid, bias_rows, pad_first, pad_rest, slab, edge_l, edge_r, turn,
                  st_first, row_first, col_first, cs_first,
                  st_rest, corner_in, row_in, col_in, corner_out, row_out, col_out, whole_inbox,
                  load_sem, first_recv, col_recv, first_send, recv, send):
    samples, rows, cols, _ = act.shape
    pairs = rows // 2
    peers_n = rows_n * cols_n
    sx, sy = lax.axis_index("sx"), lax.axis_index("sy")
    at_x = [sx] + [lax.rem(sx + off, cols_n) for off in range(1, cols_n)]
    at_y = [sy] + [lax.rem(sy + off, rows_n) for off in range(1, rows_n)]
    order = far_first(rows_n, cols_n)
    has_l, has_r, has_t, has_b = sx > 0, sx < cols_n - 1, sy > 0, sy < rows_n - 1

    def device(off):
        return {"sx": at_x[off[0] % cols_n], "sy": at_y[off[1] % rows_n]}

    def wrap(off):
        return (off[0] % cols_n, off[1] % rows_n)

    corner_to = {wrap(off): at for at, off in enumerate(((-1, -1), (1, -1), (-1, 1), (1, 1)))}
    row_to = {wrap(off): at for at, off in enumerate(((0, -1), (0, 1)))}
    col_to = {wrap(off): at for at, off in enumerate(((-1, 0), (1, 0)))}
    plain = [off for off in order if off not in corner_to and off not in row_to and off not in col_to]

    loads = [pltpu.make_async_copy(act_hbm.at[s], act.at[s], load_sem.at[s]) for s in range(samples)]
    others = ((ws_hbm, ws), (br_hbm, bias_rest), (wo_hbm, wo_ref), (nf_hbm, norm_first), (wf_hbm, wf), (wr_hbm, wr), (nr_hbm, norm_rest), (bo_hbm, bias_out))
    for at, (src, dst) in enumerate(others):
        loads.append(pltpu.make_async_copy(src, dst, load_sem.at[samples + at]))
    for load in loads[:samples]:
        load.start()
    barrier = pltpu.get_barrier_semaphore()
    for off in order:
        pl.semaphore_signal(barrier, inc=1, device_id=device(off), device_id_type=MESH)

    def remote(src, dst, send_to, recv_at, off):
        pltpu.make_async_remote_copy(src_ref=src, dst_ref=dst, send_sem=send_to, recv_sem=recv_at, device_id=device(off), device_id_type=MESH).start()

    def wait_for(ref, sem):
        pltpu.make_async_copy(ref, ref, sem).wait()

    def send_rest(at, s):
        sem = recv.at[at, s]
        for off in order:
            if off in corner_to:
                box = corner_to[off]
                remote(corner_out.at[at, s, box], corner_in.at[at, s, 3 - box], send.at[1], sem, off)
            elif off in row_to:
                box = row_to[off]
                remote(row_out.at[at, s, box], row_in.at[at, s, 1 - box], send.at[2], sem, off)
            elif off in col_to:
                box = col_to[off]
                remote(col_out.at[at, s, box], col_in.at[at, s, 1 - box], send.at[3], sem, off)
            else:
                remote(st_rest.at[at, s, 0], st_rest.at[at, s, 1 + plain.index(off)], send.at[0], sem, off)

    sub = lax.broadcasted_iota(jnp.int32, (1, 8, LANES), 1)
    first_sub, last_sub = sub == 0, sub == 7

    def tree_sum(stack):
        while stack.shape[0] > 1:
            half = stack.shape[0] // 2
            folded = stack[:half] + stack[half:2 * half]
            stack = folded if stack.shape[0] == 2 * half else jnp.concatenate([folded[:1] + stack[2 * half:], folded[1:]], axis=0) if half > 1 else folded + stack[2 * half:]
        return stack[0]

    def affine(one, two, norm, per_group):
        count = rows * rows_n * cols * cols_n * per_group
        mean = group_total(one, per_group) / count
        square = group_total(two, per_group) / count
        scale = lax.rsqrt(square - mean * mean + GN_EPS) * jnp.broadcast_to(norm[0:1], (8, LANES))
        shift = jnp.broadcast_to(norm[1:2], (8, LANES)) - mean * scale
        return 0.5 * scale, 0.5 * shift

    first_group = 2 * LANES // GROUPS
    lane_in_group = lax.broadcasted_iota(jnp.int32, (8, LANES), 1) & (first_group - 1)

    def silu(x, scales):
        u = x * scales[0] + scales[1]
        return u + u * jnp.tanh(u)

    def spread(rows_of_cols, from_left, from_right):
        v0, v1 = rows_of_cols[:, 0], rows_of_cols[:, 1]
        r0, r1 = pltpu.roll(v0, 1, 1), pltpu.roll(v1, 1, 1)
        q0, q1 = pltpu.roll(v0, 7, 1), pltpu.roll(v1, 7, 1)
        shifted = (
            (jnp.where(first_sub, from_left, r0), jnp.where(first_sub, r0, r1)),
            (v0, v1),
            (jnp.where(last_sub, q1, q0), jnp.where(last_sub, from_right, q1)),
        )
        return [jnp.concatenate(pair, axis=1) for pair in shifted]

    def edges(tile, scales, halo_cols):
        one_row = (scales[0][0:1], scales[1][0:1])
        edge_l[tile] = jnp.where(has_l, silu(halo_cols[0], one_row), 0.0)
        edge_r[tile] = jnp.where(has_r, silu(halo_cols[1], one_row), 0.0)

    def activate(block, tile, scales, halo_rows, corners, row_source, place):
        begin, end = max(0, BLOCK * block + 1), min(rows, BLOCK * (block + 1) + 1)
        value = row_source(begin, end)
        lefts = [jnp.broadcast_to(edge_l[tile, r:r + 1, :], (8, LANES)) for r in range(begin, end)]
        rights = [jnp.broadcast_to(edge_r[tile, r:r + 1, :], (8, LANES)) for r in range(begin, end)]
        value = silu(value, scales)
        for at, has in enumerate((has_t, has_b)):
            if block == (-1, rows // BLOCK - 1)[at]:
                halo = jnp.where(has, silu(halo_rows[at].reshape(1, 2, 8, LANES), scales), 0.0)
                corner_l = jnp.where(jnp.logical_and(has, has_l), silu(corners[2 * at], scales), 0.0)
                corner_r = jnp.where(jnp.logical_and(has, has_r), silu(corners[2 * at + 1], scales), 0.0)
                where_at = 0 if at == 0 else len(lefts)
                value = jnp.concatenate([halo, value] if at == 0 else [value, halo], axis=0)
                lefts.insert(where_at, corner_l)
                rights.insert(where_at, corner_r)
        for off, part in enumerate(spread(value, jnp.stack(lefts), jnp.stack(rights))):
            place(off, tile, BLOCK // 2 * block + 1 if block >= 0 else 0, part.reshape(part.shape[0] // 2, 2, cols, LANES))

    def prepare_rest(at, s, source):
        wait_for(whole_inbox, recv.at[at, s])
        slots = [st_rest[at, s], corner_in[at, s, :, 0:2], row_in[at, s, :, 0:2], col_in[at, s, :, 0:2]]
        total = tree_sum(jnp.concatenate(slots, axis=0))
        one, two = (jnp.broadcast_to(total[which:which + 1], (8, LANES)) for which in range(2))
        scales = affine(one, two, norm_rest[at].astype(jnp.float32), LANES // GROUPS)

        def row_source(begin, end):
            return source[s, begin * cols:end * cols, :].reshape(end - begin, 2, 8, LANES)

        def place(off, tile, pair_at, value):
            for half in range(2):
                pad_rest[off, pair_at:pair_at + value.shape[0], :, half * LANES:(half + 1) * LANES] = value[:, half]

        edges(0, scales, [col_in[at, s, box, 8:8 + rows, :] for box in range(2)])
        halo_rows = [row_in[at, s, box, 8:8 + cols, :] for box in range(2)]
        corners = [jnp.broadcast_to(corner_in[at, s, box, 2:3, :], (8, LANES)) for box in range(4)]
        return lambda block: activate(block, 0, scales, halo_rows, corners, row_source, place)

    def prepare_first(s):
        wait_for(col_first.at[s], col_recv.at[s])
        norm = norm_first[...].astype(jnp.float32)

        def one_tile(tile):
            lanes = slice(tile * LANES, (tile + 1) * LANES)
            packed = jnp.broadcast_to(total_first[tile:tile + 1], (8, LANES))
            one, two = (jnp.where(lane_in_group == which * samples + s, packed, 0.0) for which in range(2))
            scales = affine(one, two, norm[:, lanes], first_group)

            def row_source(begin, end):
                return act[s, begin:end, :, lanes].astype(jnp.float32).reshape(end - begin, 2, 8, LANES)

            def place(off, tile, pair_at, value):
                pad_first[off, pair_at:pair_at + value.shape[0], :, :, lanes] = value

            edges(tile, scales, [col_first[s, box, :, lanes].astype(jnp.float32) for box in range(2)])
            halo_rows = [row_first[box, s, :, lanes].astype(jnp.float32) for box in (1, 4)]
            corners = []
            for box in (0, 2, 3, 5):
                row = row_first[box, s, :, lanes].astype(jnp.float32)
                corners.append(pltpu.roll(row[8:16], 1, 0) if box % 3 == 0 else pltpu.roll(row[0:8], 7, 0))
            return lambda block: activate(block, tile, scales, halo_rows, corners, row_source, place)

        tiles = [one_tile(tile) for tile in range(2)]
        return lambda block: [tile(block) for tile in tiles]

    zero = jnp.zeros((LANES, LANES), jnp.bfloat16)
    wide_zero = jnp.zeros((2 * LANES, LANES), jnp.bfloat16)

    def square_of(a, b, c, d):
        return jnp.concatenate([jnp.concatenate([a, b], axis=1), jnp.concatenate([c, d], axis=1)], axis=0)

    def conv_rest(weight, pair_from, pair_n):
        total = None
        for off in range(3):
            w0, w1, w2 = (weight(row_off, off) for row_off in range(3))
            for shift, tap in ((0, square_of(w0, zero, w1, w0)), (1, square_of(w2, w1, zero, w2))):
                lhs = pad_rest[off, pair_from + shift:pair_from + shift + pair_n].reshape(pair_n * cols, 2 * LANES)
                part = jnp.dot(lhs, tap.astype(jnp.float32), preferred_element_type=jnp.float32)
                total = part if total is None else total + part
        return total

    def conv_first(pair_from, pair_n):
        total = None
        for off in range(3):
            w0, w1, w2 = (wf[row_off, off] for row_off in range(3))
            for at, (a, b) in enumerate(((w0, wide_zero), (w1, w0), (w2, w1), (wide_zero, w2))):
                begin = pair_from + at // 2
                lhs = pad_first[off, begin:begin + pair_n, at % 2].reshape(pair_n * cols, 2 * LANES)
                part = jnp.dot(lhs, jnp.concatenate([a, b], axis=1).astype(jnp.float32), preferred_element_type=jnp.float32)
                total = part if total is None else total + part
        return total

    def in_chunks(block, conv, use):
        block(-1)
        done, per_chunk = 0, pairs // CHUNKS
        for chunk in range(CHUNKS):
            while BLOCK // 2 * done < (chunk + 1) * per_chunk:
                block(done)
                done += 1
            total = conv(chunk * per_chunk, per_chunk)
            halves = [total[:, half * LANES:(half + 1) * LANES].reshape(per_chunk, 1, cols, LANES) for half in range(2)]
            use(2 * chunk * per_chunk, jnp.concatenate(halves, axis=1).reshape(2 * per_chunk * cols, LANES))

    def finish(at, s, block, conv, bias, target, residual):
        acc = []

        def use(row, value):
            rows_in = value.shape[0] // cols
            value = value + bias
            if residual is not None:
                value = value + residual[s, row * cols:row * cols + value.shape[0], :]
            value = value.astype(jnp.bfloat16).astype(jnp.float32)
            target[s, row * cols:row * cols + value.shape[0], :] = value
            for edge, edge_row in enumerate((0, rows - 1)):
                if row <= edge_row < row + rows_in:
                    line = value[(edge_row - row) * cols:(edge_row - row + 1) * cols]
                    row_out[at, s, edge, 8:8 + cols, :] = line
                    corner_out[at, s, 2 * edge, 2:3, :] = line[0:1]
                    corner_out[at, s, 2 * edge + 1, 2:3, :] = line[cols - 1:cols]
            split = value.reshape(value.shape[0] // 16, 2, 8, LANES)
            acc.append([jnp.sum(split, axis=0), jnp.sum(split * split, axis=0)])

        in_chunks(block, conv, use)
        sums = []
        for which in range(2):
            part = acc[0][which]
            for more in acc[1:]:
                part = part + more[which]
            sums.append(jnp.sum(part[0] + part[1], axis=0, keepdims=True))
        sums = jnp.concatenate(sums, axis=0)
        st_rest[at, s, 0] = sums
        for box in range(4):
            corner_out[at, s, box, 0:2, :] = sums
        for box in range(2):
            col_out[at, s, box, 8:8 + rows, :] = target[s, pl.ds(box * (cols - 1), rows, stride=cols), :]
            row_out[at, s, box, 0:2, :] = sums
            col_out[at, s, box, 0:2, :] = sums
        send_rest(at, s)

    def first_sums(s, carry):
        wait_for(act.at[s], load_sem.at[s])

        def body(step, sums):
            sums = list(sums)
            for at in range(ROW_BLOCK):
                r = step * ROW_BLOCK + at
                for tile in range(2):
                    row = act[s, r, :, tile * LANES:(tile + 1) * LANES].astype(jnp.float32)
                    v0, v1 = row[0:8], row[8:16]
                    slab[0, tile, pl.ds(pl.multiple_of(r * 8, 8), 8), :] = v0
                    slab[1, tile, pl.ds(pl.multiple_of(r * 8, 8), 8), :] = v1
                    sums[2 * tile] = sums[2 * tile] + (v0 + v1)
                    sums[2 * tile + 1] = sums[2 * tile + 1] + (v0 * v0 + v1 * v1)
            return tuple(sums)

        sums = lax.fori_loop(0, rows // ROW_BLOCK, body, (jnp.zeros((8, LANES), jnp.float32),) * 4)
        for side in range(2):
            for tile in range(2):
                column = slab[side, tile, pl.ds(7 * side, rows, stride=8), :]
                cs_first[s, side, :, tile * LANES:(tile + 1) * LANES] = column.astype(jnp.bfloat16)
        for tile in range(2):
            for which in range(2):
                sums_first[tile, pl.ds(which * samples + s, 1), :] = jnp.sum(sums[2 * tile + which], axis=0, keepdims=True)
        return carry

    lax.fori_loop(0, samples, first_sums, 0)
    for load in loads[samples:]:
        load.start()
    row_at = lax.broadcasted_iota(jnp.int32, (8, LANES), 0)
    for tile in range(2):
        grouped = jnp.where(row_at == lane_in_group, group_total(sums_first[tile], first_group), 0.0)
        st_first[0, tile:tile + 1, :] = jnp.sum(grouped, axis=0, keepdims=True)
    pl.semaphore_wait(barrier, peers_n - 1)
    for slot, off in enumerate(order):
        remote(st_first.at[0], st_first.at[slot + 1], first_send.at[0], first_recv.at[0], off)
    for row, y_off, base in ((0, -1, 3), (rows - 1, 1, 0)):
        for x_off, at in ((-1, 2), (0, 1), (1, 0)):
            remote(act.at[:, row], row_first.at[base + at], first_send.at[1], first_recv.at[1], (x_off, y_off))

    def first_columns(s, carry):
        for off, box in col_to.items():
            remote(cs_first.at[s, box], col_first.at[s, 1 - box], first_send.at[2], col_recv.at[s], off)
        return carry

    lax.fori_loop(0, samples, first_columns, 0)

    for load in loads[samples:samples + 3]:
        load.wait()
    bias = bias_rest[...].astype(jnp.float32)

    def shortcut(s, carry):
        flat = act[s].reshape(rows * cols, 2 * LANES)
        hid[s] = jnp.dot(flat, ws[...], preferred_element_type=jnp.float32) + bias[6:7]
        return carry

    lax.fori_loop(0, samples, shortcut, 0)
    for tap in range(9):
        three = wo_ref[tap // 3, tap % 3].astype(jnp.float32)
        eight = jnp.concatenate([three, jnp.zeros((8 - three.shape[0], LANES), jnp.float32)], axis=0)
        wo[tap] = jnp.concatenate([eight] * 16, axis=0).T.astype(jnp.bfloat16)
    for load in loads[samples + 3:]:
        load.wait()
    wait_for(st_first.at[pl.ds(1, peers_n - 1)], first_recv.at[0])
    total_first[0:2, :] = jnp.sum(st_first[...], axis=0)
    wait_for(row_first, first_recv.at[1])

    def layer_first(s, carry):
        finish(0, s, prepare_first(s), conv_first, bias[0:1], mid, None)
        return carry

    lax.fori_loop(0, samples, layer_first, 0)

    def layer_rest(layer, source, target, residual):
        def one_sample(s, carry):
            block = prepare_rest(layer - 1, s, source)
            conv = functools.partial(conv_rest, lambda row_off, off: wr[layer - 1, row_off, off])
            finish(layer, s, block, conv, bias_rows[pl.ds(layer, 1), :], target, residual)
            return carry

        lax.fori_loop(0, samples, one_sample, 0)

    def layer_pair(step, carry):
        layer_rest(2 * step + 1, mid, hid, hid)
        layer_rest(2 * step + 2, hid, mid, None)
        return carry

    bias_rows[0:bias.shape[0], :] = bias
    lax.fori_loop(0, (LAYERS - 2) // 2, layer_pair, 0)
    layer_rest(LAYERS - 2, mid, hid, hid)

    lane = lax.broadcasted_iota(jnp.int32, (rows, LANES), 1)
    out_bias = bias_out[...].astype(jnp.float32)

    def layer_last(s, carry):
        def use(row, value):
            mid[s, row * cols:row * cols + value.shape[0], :] = value

        in_chunks(prepare_rest(LAYERS - 2, s, hid), functools.partial(conv_rest, lambda row_off, off: wo[3 * row_off + off]), use)
        merged = mid[s, pl.ds(0, rows, stride=cols), :]
        for col in range(1, cols):
            merged = jnp.where(lane // 8 == col, mid[s, pl.ds(col, rows, stride=cols), :], merged)
        turn[...] = jnp.concatenate([merged] * (LANES // rows), axis=0).T
        for chan in range(y_ref.shape[1]):
            plane = turn[pl.ds(chan, cols, stride=8), :]
            y_ref[s, chan] = plane[:, 0:rows] + out_bias[0:1, chan:chan + 1]
        return carry

    lax.fori_loop(0, samples, layer_last, 0)

    wait_for(st_first.at[pl.ds(1, peers_n - 1)], first_send.at[0])
    wait_for(row_first, first_send.at[1])
    wait_for(cs_first, first_send.at[2])
    wait_for(st_rest.at[:, :, pl.ds(1, len(plain))], send.at[0])
    wait_for(corner_out, send.at[1])
    wait_for(row_out, send.at[2])
    wait_for(col_out, send.at[3])


def solution(mesh):
    rows_n, cols_n = mesh.shape["sy"], mesh.shape["sx"]
    peers_n = rows_n * cols_n
    tile_spec = P("dp", "sy", "sx", None)
    replicated = P()

    def local_decode(act_in, norm_first, w_first, w_short, norm_rest, w_rest, bias_rest, w_out, bias_out):
        samples, rows, cols, wide = act_in.shape
        chans = w_short.shape[1]
        out_chans = w_out.shape[3]
        f32, bf16 = jnp.float32, jnp.bfloat16
        rest, plain_n = LAYERS - 1, peers_n - 9
        whole = pl.BlockSpec(memory_space=pltpu.VMEM)
        there = pl.BlockSpec(memory_space=pltpu.HBM)
        image = pl.pallas_call(
            functools.partial(decode_kernel, rows_n, cols_n),
            name="decode",
            out_shape=jax.ShapeDtypeStruct((samples, out_chans, cols, rows), f32),
            in_specs=[there] * 9,
            out_specs=whole,
            scratch_shapes=[
                pltpu.VMEM(act_in.shape, bf16),
                pltpu.VMEM(norm_first.shape, bf16),
                pltpu.VMEM(w_first.shape, bf16),
                pltpu.VMEM(w_short.shape, bf16),
                pltpu.VMEM(norm_rest.shape, bf16),
                pltpu.VMEM(w_rest.shape, bf16),
                pltpu.VMEM(bias_rest.shape, bf16),
                pltpu.VMEM((3, 3, out_chans, chans), bf16),
                pltpu.VMEM((1, out_chans), bf16),
                pltpu.VMEM((2, 8, LANES), f32),
                pltpu.VMEM((8, LANES), f32),
                pltpu.VMEM((9, chans, LANES), bf16),
                pltpu.VMEM((samples, rows * cols, chans), f32),
                pltpu.VMEM((samples, rows * cols, chans), f32),
                pltpu.VMEM((8, chans), f32),
                pltpu.VMEM((3, rows // 2 + 1, 2, cols, wide), f32),
                pltpu.VMEM((3, rows // 2 + 1, cols, 2 * chans), f32),
                pltpu.VMEM((2, 2, rows * 8, LANES), f32),
                pltpu.VMEM((2, rows, LANES), f32),
                pltpu.VMEM((2, rows, LANES), f32),
                pltpu.VMEM((LANES, LANES), f32),
                pltpu.VMEM((peers_n, 2, LANES), f32),
                pltpu.VMEM((6, samples, cols, wide), bf16),
                pltpu.VMEM((samples, 2, rows, wide), bf16),
                pltpu.VMEM((samples, 2, rows, wide), bf16),
                pltpu.VMEM((rest, samples, plain_n + 1, 2, chans), f32),
                pltpu.VMEM((rest, samples, 4, 4, chans), f32),
                pltpu.VMEM((rest, samples, 2, 8 + cols, chans), f32),
                pltpu.VMEM((rest, samples, 2, 8 + rows, chans), f32),
                pltpu.VMEM((rest, samples, 4, 4, chans), f32),
                pltpu.VMEM((rest, samples, 2, 8 + cols, chans), f32),
                pltpu.VMEM((rest, samples, 2, 8 + rows, chans), f32),
                pltpu.VMEM((plain_n + 8 + 16 + cols + rows, 2, chans), f32),
                pltpu.SemaphoreType.DMA((samples + 8,)),
                pltpu.SemaphoreType.DMA((2,)),
                pltpu.SemaphoreType.DMA((samples,)),
                pltpu.SemaphoreType.DMA((3,)),
                pltpu.SemaphoreType.DMA((rest, samples)),
                pltpu.SemaphoreType.DMA((4,)),
            ],
            compiler_params=pltpu.CompilerParams(collective_id=0, has_side_effects=True, vmem_limit_bytes=48 * 1024 * 1024),
        )(*[pltpu.with_memory_space_constraint(x, pltpu.HBM) for x in (act_in, norm_first, w_first, w_short, norm_rest, w_rest, bias_rest, jnp.transpose(w_out, (0, 1, 3, 2)), bias_out.reshape(1, out_chans))])
        return jnp.transpose(image, (0, 3, 2, 1))

    return jax.shard_map(local_decode, mesh=mesh, in_specs=(tile_spec,) + (replicated,) * 8, out_specs=tile_spec, check_vma=False)
```

```python
import functools

import jax
import jax.numpy as jnp
from jax import lax
from jax.experimental import pallas as pl
from jax.experimental.pallas import tpu as pltpu
from jax.sharding import PartitionSpec as P

GROUPS = 32
GN_EPS = 1e-6
MESH = pl.DeviceIdType.MESH
LANES = 128
ROW_BLOCK = 2
LAYERS = 7
CHUNKS = 4
BLOCK = 2


def group_total(vec, per_group):
    lane = lax.broadcasted_iota(jnp.int32, vec.shape, 1) & (per_group - 1)
    parts = [vec]
    for dist in range(1, per_group):
        parts.append(jnp.where(lane >= dist, pltpu.roll(vec, dist, 1), pltpu.roll(vec, LANES - per_group + dist, 1)))
    while len(parts) > 1:
        parts = [parts[at] + parts[at + 1] if at + 1 < len(parts) else parts[at] for at in range(0, len(parts), 2)]
    return parts[0]


def far_first(rows_n, cols_n):
    every = [(a, b) for a in range(cols_n) for b in range(rows_n) if a or b]
    return sorted(every, key=lambda off: -(min(off[0], cols_n - off[0]) + min(off[1], rows_n - off[1]) / 2))


def decode_kernel(rows_n, cols_n, act_hbm, nf_hbm, wf_hbm, ws_hbm, nr_hbm, wr_hbm, br_hbm, wo_hbm, bo_hbm, y_ref,
                  act, norm_first, wf, ws, norm_rest, wr, bias_rest, wo_ref, bias_out, sums_first, total_first, wo, mid, hid, bias_rows, pad_first, pad_rest, slab, edge_l, edge_r, turn,
                  st_first, row_first, col_first, cs_first,
                  st_rest, corner_in, row_in, col_in, corner_out, row_out, col_out, whole_inbox,
                  load_sem, first_recv, col_recv, first_send, recv, send):
    samples, rows, cols, _ = act.shape
    pairs = rows // 2
    peers_n = rows_n * cols_n
    sx, sy = lax.axis_index("sx"), lax.axis_index("sy")
    at_x = [sx] + [lax.rem(sx + off, cols_n) for off in range(1, cols_n)]
    at_y = [sy] + [lax.rem(sy + off, rows_n) for off in range(1, rows_n)]
    order = far_first(rows_n, cols_n)
    has_l, has_r, has_t, has_b = sx > 0, sx < cols_n - 1, sy > 0, sy < rows_n - 1

    def device(off):
        return {"sx": at_x[off[0] % cols_n], "sy": at_y[off[1] % rows_n]}

    def wrap(off):
        return (off[0] % cols_n, off[1] % rows_n)

    corner_to = {wrap(off): at for at, off in enumerate(((-1, -1), (1, -1), (-1, 1), (1, 1)))}
    row_to = {wrap(off): at for at, off in enumerate(((0, -1), (0, 1)))}
    col_to = {wrap(off): at for at, off in enumerate(((-1, 0), (1, 0)))}
    plain = [off for off in order if off not in corner_to and off not in row_to and off not in col_to]

    half_rows = rows // 2
    loads = []
    for s in range(samples):
        for half in range(2):
            part = pl.ds(half * half_rows, half_rows)
            loads.append(pltpu.make_async_copy(act_hbm.at[s, part], act.at[s, part], load_sem.at[2 * s + half]))
    act_loads = 2 * samples
    others = ((ws_hbm, ws), (br_hbm, bias_rest), (wo_hbm, wo_ref), (nf_hbm, norm_first), (wf_hbm, wf), (wr_hbm, wr), (nr_hbm, norm_rest), (bo_hbm, bias_out))
    for at, (src, dst) in enumerate(others):
        loads.append(pltpu.make_async_copy(src, dst, load_sem.at[act_loads + at]))
    for load in loads[:act_loads]:
        load.start()
    barrier = pltpu.get_barrier_semaphore()
    for off in order:
        pl.semaphore_signal(barrier, inc=1, device_id=device(off), device_id_type=MESH)

    def remote(src, dst, send_to, recv_at, off):
        pltpu.make_async_remote_copy(src_ref=src, dst_ref=dst, send_sem=send_to, recv_sem=recv_at, device_id=device(off), device_id_type=MESH).start()

    def wait_for(ref, sem):
        pltpu.make_async_copy(ref, ref, sem).wait()

    def send_plain(at, s):
        for slot, off in enumerate(plain):
            remote(st_rest.at[at, s, 0], st_rest.at[at, s, 1 + slot], send.at[0], recv.at[at, s], off)

    def send_edges(at, s):
        for off, box in corner_to.items():
            remote(corner_out.at[at, s, box], corner_in.at[at, s, 3 - box], send.at[1], recv.at[at, s], off)
        for off, box in col_to.items():
            remote(col_out.at[at, s, box], col_in.at[at, s, 1 - box], send.at[3], recv.at[at, s], off)
        for off, box in row_to.items():
            remote(row_out.at[at, s, box], row_in.at[at, s, 1 - box], send.at[2], recv.at[at, s], off)

    sub = lax.broadcasted_iota(jnp.int32, (1, 8, LANES), 1)
    first_sub, last_sub = sub == 0, sub == 7

    def tree_sum(stack):
        while stack.shape[0] > 1:
            half = stack.shape[0] // 2
            folded = stack[:half] + stack[half:2 * half]
            stack = folded if stack.shape[0] == 2 * half else jnp.concatenate([folded[:1] + stack[2 * half:], folded[1:]], axis=0) if half > 1 else folded + stack[2 * half:]
        return stack[0]

    def affine(one, two, norm, per_group):
        count = rows * rows_n * cols * cols_n * per_group
        mean = group_total(one, per_group) / count
        square = group_total(two, per_group) / count
        scale = lax.rsqrt(square - mean * mean + GN_EPS) * jnp.broadcast_to(norm[0:1], (8, LANES))
        shift = jnp.broadcast_to(norm[1:2], (8, LANES)) - mean * scale
        return 0.5 * scale, 0.5 * shift

    first_group = 2 * LANES // GROUPS
    lane_in_group = lax.broadcasted_iota(jnp.int32, (8, LANES), 1) & (first_group - 1)

    def silu(x, scales):
        u = x * scales[0] + scales[1]
        return u + u * jnp.tanh(u)

    def spread(rows_of_cols, from_left, from_right):
        v0, v1 = rows_of_cols[:, 0], rows_of_cols[:, 1]
        r0, r1 = pltpu.roll(v0, 1, 1), pltpu.roll(v1, 1, 1)
        q0, q1 = pltpu.roll(v0, 7, 1), pltpu.roll(v1, 7, 1)
        shifted = (
            (jnp.where(first_sub, from_left, r0), jnp.where(first_sub, r0, r1)),
            (v0, v1),
            (jnp.where(last_sub, q1, q0), jnp.where(last_sub, from_right, q1)),
        )
        return [jnp.concatenate(pair, axis=1) for pair in shifted]

    def edges(tile, scales, halo_cols):
        one_row = (scales[0][0:1], scales[1][0:1])
        edge_l[tile] = jnp.where(has_l, silu(halo_cols[0], one_row), 0.0)
        edge_r[tile] = jnp.where(has_r, silu(halo_cols[1], one_row), 0.0)

    def activate(block, tile, scales, halo_rows, corners, row_source, place):
        begin, end = max(0, BLOCK * block + 1), min(rows, BLOCK * (block + 1) + 1)
        value = row_source(begin, end)
        lefts = [jnp.broadcast_to(edge_l[tile, r:r + 1, :], (8, LANES)) for r in range(begin, end)]
        rights = [jnp.broadcast_to(edge_r[tile, r:r + 1, :], (8, LANES)) for r in range(begin, end)]
        value = silu(value, scales)
        for at, has in enumerate((has_t, has_b)):
            if block == (-1, rows // BLOCK - 1)[at]:
                halo = jnp.where(has, silu(halo_rows[at].reshape(1, 2, 8, LANES), scales), 0.0)
                corner_l = jnp.where(jnp.logical_and(has, has_l), silu(corners[2 * at], scales), 0.0)
                corner_r = jnp.where(jnp.logical_and(has, has_r), silu(corners[2 * at + 1], scales), 0.0)
                where_at = 0 if at == 0 else len(lefts)
                value = jnp.concatenate([halo, value] if at == 0 else [value, halo], axis=0)
                lefts.insert(where_at, corner_l)
                rights.insert(where_at, corner_r)
        for off, part in enumerate(spread(value, jnp.stack(lefts), jnp.stack(rights))):
            place(off, tile, BLOCK // 2 * block + 1 if block >= 0 else 0, part.reshape(part.shape[0] // 2, 2, cols, LANES))

    def prepare_rest(at, s, source):
        wait_for(whole_inbox, recv.at[at, s])
        slots = [st_rest[at, s], corner_in[at, s, :, 0:2], row_in[at, s, :, 0:2], col_in[at, s, :, 0:2]]
        total = tree_sum(jnp.concatenate(slots, axis=0))
        one, two = (jnp.broadcast_to(total[which:which + 1], (8, LANES)) for which in range(2))
        scales = affine(one, two, norm_rest[at].astype(jnp.float32), LANES // GROUPS)

        def row_source(begin, end):
            return source[s, begin * cols:end * cols, :].reshape(end - begin, 2, 8, LANES)

        def place(off, tile, pair_at, value):
            for half in range(2):
                pad_rest[off, pair_at:pair_at + value.shape[0], :, half * LANES:(half + 1) * LANES] = value[:, half]

        edges(0, scales, [col_in[at, s, box, 8:8 + rows, :] for box in range(2)])
        halo_rows = [row_in[at, s, box, 8:8 + cols, :] for box in range(2)]
        corners = [jnp.broadcast_to(corner_in[at, s, box, 2:3, :], (8, LANES)) for box in range(4)]
        return lambda block: activate(block, 0, scales, halo_rows, corners, row_source, place)

    def prepare_first(s):
        wait_for(col_first.at[s], col_recv.at[s])
        norm = norm_first[...].astype(jnp.float32)

        def one_tile(tile):
            lanes = slice(tile * LANES, (tile + 1) * LANES)
            packed = jnp.broadcast_to(total_first[tile:tile + 1], (8, LANES))
            one, two = (jnp.where(lane_in_group == which * samples + s, packed, 0.0) for which in range(2))
            scales = affine(one, two, norm[:, lanes], first_group)

            def row_source(begin, end):
                return act[s, begin:end, :, lanes].astype(jnp.float32).reshape(end - begin, 2, 8, LANES)

            def place(off, tile, pair_at, value):
                pad_first[off, pair_at:pair_at + value.shape[0], :, :, lanes] = value

            edges(tile, scales, [col_first[s, box, :, lanes].astype(jnp.float32) for box in range(2)])
            halo_rows = [row_first[box, s, :, lanes].astype(jnp.float32) for box in (1, 4)]
            corners = []
            for box in (0, 2, 3, 5):
                row = row_first[box, s, :, lanes].astype(jnp.float32)
                corners.append(pltpu.roll(row[8:16], 1, 0) if box % 3 == 0 else pltpu.roll(row[0:8], 7, 0))
            return lambda block: activate(block, tile, scales, halo_rows, corners, row_source, place)

        tiles = [one_tile(tile) for tile in range(2)]
        return lambda block: [tile(block) for tile in tiles]

    zero = jnp.zeros((LANES, LANES), jnp.bfloat16)
    wide_zero = jnp.zeros((2 * LANES, LANES), jnp.bfloat16)

    def square_of(a, b, c, d):
        return jnp.concatenate([jnp.concatenate([a, b], axis=1), jnp.concatenate([c, d], axis=1)], axis=0)

    def conv_rest(weight, pair_from, pair_n):
        total = None
        for off in range(3):
            w0, w1, w2 = (weight(row_off, off) for row_off in range(3))
            for shift, tap in ((0, square_of(w0, zero, w1, w0)), (1, square_of(w2, w1, zero, w2))):
                lhs = pad_rest[off, pair_from + shift:pair_from + shift + pair_n].reshape(pair_n * cols, 2 * LANES)
                part = jnp.dot(lhs, tap.astype(jnp.float32), preferred_element_type=jnp.float32)
                total = part if total is None else total + part
        return total

    def conv_first(pair_from, pair_n):
        total = None
        for off in range(3):
            w0, w1, w2 = (wf[row_off, off] for row_off in range(3))
            for at, (a, b) in enumerate(((w0, wide_zero), (w1, w0), (w2, w1), (wide_zero, w2))):
                begin = pair_from + at // 2
                lhs = pad_first[off, begin:begin + pair_n, at % 2].reshape(pair_n * cols, 2 * LANES)
                part = jnp.dot(lhs, jnp.concatenate([a, b], axis=1).astype(jnp.float32), preferred_element_type=jnp.float32)
                total = part if total is None else total + part
        return total

    def in_chunks(block, conv, use):
        block(-1)
        done, per_chunk = 0, pairs // CHUNKS
        for chunk in range(CHUNKS):
            while BLOCK // 2 * done < (chunk + 1) * per_chunk:
                block(done)
                done += 1
            total = conv(chunk * per_chunk, per_chunk)
            halves = [total[:, half * LANES:(half + 1) * LANES].reshape(per_chunk, 1, cols, LANES) for half in range(2)]
            use(2 * chunk * per_chunk, jnp.concatenate(halves, axis=1).reshape(2 * per_chunk * cols, LANES))

    def finish(at, s, block, conv, bias, target, residual):
        acc = []

        def use(row, value):
            rows_in = value.shape[0] // cols
            value = value + bias
            if residual is not None:
                value = value + residual[s, row * cols:row * cols + value.shape[0], :]
            value = value.astype(jnp.bfloat16).astype(jnp.float32)
            target[s, row * cols:row * cols + value.shape[0], :] = value
            for edge, edge_row in enumerate((0, rows - 1)):
                if row <= edge_row < row + rows_in:
                    line = value[(edge_row - row) * cols:(edge_row - row + 1) * cols]
                    row_out[at, s, edge, 8:8 + cols, :] = line
                    corner_out[at, s, 2 * edge, 2:3, :] = line[0:1]
                    corner_out[at, s, 2 * edge + 1, 2:3, :] = line[cols - 1:cols]
            for box in range(2):
                column = target[s, pl.ds(row * cols + box * (cols - 1), rows_in, stride=cols), :]
                col_out[at, s, box, 8 + row:8 + row + rows_in, :] = column
            split = value.reshape(value.shape[0] // 16, 2, 8, LANES)
            acc.append([jnp.sum(split, axis=0), jnp.sum(split * split, axis=0)])

        in_chunks(block, conv, use)
        sums = []
        for which in range(2):
            part = acc[0][which]
            for more in acc[1:]:
                part = part + more[which]
            sums.append(jnp.sum(part[0] + part[1], axis=0, keepdims=True))
        sums = jnp.concatenate(sums, axis=0)
        st_rest[at, s, 0] = sums
        send_plain(at, s)
        for box in range(4):
            corner_out[at, s, box, 0:2, :] = sums
        for box in range(2):
            row_out[at, s, box, 0:2, :] = sums
            col_out[at, s, box, 0:2, :] = sums
        send_edges(at, s)

    def first_sums(s, carry):

        def body(step, sums):
            sums = list(sums)
            for at in range(ROW_BLOCK):
                r = step * ROW_BLOCK + at
                for tile in range(2):
                    row = act[s, r, :, tile * LANES:(tile + 1) * LANES].astype(jnp.float32)
                    v0, v1 = row[0:8], row[8:16]
                    slab[0, tile, pl.ds(pl.multiple_of(r * 8, 8), 8), :] = v0
                    slab[1, tile, pl.ds(pl.multiple_of(r * 8, 8), 8), :] = v1
                    sums[2 * tile] = sums[2 * tile] + (v0 + v1)
                    sums[2 * tile + 1] = sums[2 * tile + 1] + (v0 * v0 + v1 * v1)
            return tuple(sums)

        sums = (jnp.zeros((8, LANES), jnp.float32),) * 4
        for half in range(2):
            wait_for(act.at[s, pl.ds(half * half_rows, half_rows)], load_sem.at[2 * s + half])
            sums = lax.fori_loop(half * half_rows // ROW_BLOCK, (half + 1) * half_rows // ROW_BLOCK, body, sums)
        for side in range(2):
            for tile in range(2):
                column = slab[side, tile, pl.ds(7 * side, rows, stride=8), :]
                cs_first[s, side, :, tile * LANES:(tile + 1) * LANES] = column.astype(jnp.bfloat16)
        for tile in range(2):
            for which in range(2):
                sums_first[tile, pl.ds(which * samples + s, 1), :] = jnp.sum(sums[2 * tile + which], axis=0, keepdims=True)
        return carry

    lax.fori_loop(0, samples, first_sums, 0)
    for load in loads[act_loads:]:
        load.start()
    row_at = lax.broadcasted_iota(jnp.int32, (8, LANES), 0)
    for tile in range(2):
        grouped = jnp.where(row_at == lane_in_group, group_total(sums_first[tile], first_group), 0.0)
        st_first[0, tile:tile + 1, :] = jnp.sum(grouped, axis=0, keepdims=True)
    pl.semaphore_wait(barrier, peers_n - 1)
    for slot, off in enumerate(order):
        remote(st_first.at[0], st_first.at[slot + 1], first_send.at[0], first_recv.at[0], off)
    for row, y_off, base in ((0, -1, 3), (rows - 1, 1, 0)):
        for x_off, at in ((-1, 2), (0, 1), (1, 0)):
            remote(act.at[:, row], row_first.at[base + at], first_send.at[1], first_recv.at[1], (x_off, y_off))

    def first_columns(s, carry):
        for off, box in col_to.items():
            remote(cs_first.at[s, box], col_first.at[s, 1 - box], first_send.at[2], col_recv.at[s], off)
        return carry

    lax.fori_loop(0, samples, first_columns, 0)

    for load in loads[act_loads:act_loads + 3]:
        load.wait()
    bias = bias_rest[...].astype(jnp.float32)

    def shortcut(s, carry):
        flat = act[s].reshape(rows * cols, 2 * LANES)
        hid[s] = jnp.dot(flat, ws[...], preferred_element_type=jnp.float32) + bias[6:7]
        return carry

    lax.fori_loop(0, samples, shortcut, 0)
    for tap in range(9):
        three = wo_ref[tap // 3, tap % 3].astype(jnp.float32)
        eight = jnp.concatenate([three, jnp.zeros((8 - three.shape[0], LANES), jnp.float32)], axis=0)
        wo[tap] = jnp.concatenate([eight] * 16, axis=0).T.astype(jnp.bfloat16)
    for load in loads[act_loads + 3:]:
        load.wait()
    wait_for(st_first.at[pl.ds(1, peers_n - 1)], first_recv.at[0])
    total_first[0:2, :] = jnp.sum(st_first[...], axis=0)
    wait_for(row_first, first_recv.at[1])

    def layer_first(s, carry):
        finish(0, s, prepare_first(s), conv_first, bias[0:1], mid, None)
        return carry

    lax.fori_loop(0, samples, layer_first, 0)

    def layer_rest(layer, source, target, residual):
        def one_sample(s, carry):
            block = prepare_rest(layer - 1, s, source)
            conv = functools.partial(conv_rest, lambda row_off, off: wr[layer - 1, row_off, off])
            finish(layer, s, block, conv, bias_rows[pl.ds(layer, 1), :], target, residual)
            return carry

        lax.fori_loop(0, samples, one_sample, 0)

    def layer_pair(step, carry):
        layer_rest(2 * step + 1, mid, hid, hid)
        layer_rest(2 * step + 2, hid, mid, None)
        return carry

    bias_rows[0:bias.shape[0], :] = bias
    lax.fori_loop(0, (LAYERS - 2) // 2, layer_pair, 0)
    layer_rest(LAYERS - 2, mid, hid, hid)

    lane = lax.broadcasted_iota(jnp.int32, (rows, LANES), 1)
    out_bias = bias_out[...].astype(jnp.float32)

    def layer_last(s, carry):
        def use(row, value):
            mid[s, row * cols:row * cols + value.shape[0], :] = value

        in_chunks(prepare_rest(LAYERS - 2, s, hid), functools.partial(conv_rest, lambda row_off, off: wo[3 * row_off + off]), use)
        merged = mid[s, pl.ds(0, rows, stride=cols), :]
        for col in range(1, cols):
            merged = jnp.where(lane // 8 == col, mid[s, pl.ds(col, rows, stride=cols), :], merged)
        turn[...] = jnp.concatenate([merged] * (LANES // rows), axis=0).T
        for chan in range(y_ref.shape[1]):
            plane = turn[pl.ds(chan, cols, stride=8), :]
            y_ref[s, chan] = plane[:, 0:rows] + out_bias[0:1, chan:chan + 1]
        return carry

    lax.fori_loop(0, samples, layer_last, 0)

    wait_for(st_first.at[pl.ds(1, peers_n - 1)], first_send.at[0])
    wait_for(row_first, first_send.at[1])
    wait_for(cs_first, first_send.at[2])
    wait_for(st_rest.at[:, :, pl.ds(1, len(plain))], send.at[0])
    wait_for(corner_out, send.at[1])
    wait_for(row_out, send.at[2])
    wait_for(col_out, send.at[3])


def solution(mesh):
    rows_n, cols_n = mesh.shape["sy"], mesh.shape["sx"]
    peers_n = rows_n * cols_n
    tile_spec = P("dp", "sy", "sx", None)
    replicated = P()

    def local_decode(act_in, norm_first, w_first, w_short, norm_rest, w_rest, bias_rest, w_out, bias_out):
        samples, rows, cols, wide = act_in.shape
        chans = w_short.shape[1]
        out_chans = w_out.shape[3]
        f32, bf16 = jnp.float32, jnp.bfloat16
        rest, plain_n = LAYERS - 1, peers_n - 9
        whole = pl.BlockSpec(memory_space=pltpu.VMEM)
        there = pl.BlockSpec(memory_space=pltpu.HBM)
        image = pl.pallas_call(
            functools.partial(decode_kernel, rows_n, cols_n),
            name="decode",
            out_shape=jax.ShapeDtypeStruct((samples, out_chans, cols, rows), f32),
            in_specs=[there] * 9,
            out_specs=whole,
            scratch_shapes=[
                pltpu.VMEM(act_in.shape, bf16),
                pltpu.VMEM(norm_first.shape, bf16),
                pltpu.VMEM(w_first.shape, bf16),
                pltpu.VMEM(w_short.shape, bf16),
                pltpu.VMEM(norm_rest.shape, bf16),
                pltpu.VMEM(w_rest.shape, bf16),
                pltpu.VMEM(bias_rest.shape, bf16),
                pltpu.VMEM((3, 3, out_chans, chans), bf16),
                pltpu.VMEM((1, out_chans), bf16),
                pltpu.VMEM((2, 8, LANES), f32),
                pltpu.VMEM((8, LANES), f32),
                pltpu.VMEM((9, chans, LANES), bf16),
                pltpu.VMEM((samples, rows * cols, chans), f32),
                pltpu.VMEM((samples, rows * cols, chans), f32),
                pltpu.VMEM((8, chans), f32),
                pltpu.VMEM((3, rows // 2 + 1, 2, cols, wide), f32),
                pltpu.VMEM((3, rows // 2 + 1, cols, 2 * chans), f32),
                pltpu.VMEM((2, 2, rows * 8, LANES), f32),
                pltpu.VMEM((2, rows, LANES), f32),
                pltpu.VMEM((2, rows, LANES), f32),
                pltpu.VMEM((LANES, LANES), f32),
                pltpu.VMEM((peers_n, 2, LANES), f32),
                pltpu.VMEM((6, samples, cols, wide), bf16),
                pltpu.VMEM((samples, 2, rows, wide), bf16),
                pltpu.VMEM((samples, 2, rows, wide), bf16),
                pltpu.VMEM((rest, samples, plain_n + 1, 2, chans), f32),
                pltpu.VMEM((rest, samples, 4, 4, chans), f32),
                pltpu.VMEM((rest, samples, 2, 8 + cols, chans), f32),
                pltpu.VMEM((rest, samples, 2, 8 + rows, chans), f32),
                pltpu.VMEM((rest, samples, 4, 4, chans), f32),
                pltpu.VMEM((rest, samples, 2, 8 + cols, chans), f32),
                pltpu.VMEM((rest, samples, 2, 8 + rows, chans), f32),
                pltpu.VMEM((plain_n + 8 + 16 + cols + rows, 2, chans), f32),
                pltpu.SemaphoreType.DMA((2 * samples + 8,)),
                pltpu.SemaphoreType.DMA((2,)),
                pltpu.SemaphoreType.DMA((samples,)),
                pltpu.SemaphoreType.DMA((3,)),
                pltpu.SemaphoreType.DMA((rest, samples)),
                pltpu.SemaphoreType.DMA((4,)),
            ],
            compiler_params=pltpu.CompilerParams(collective_id=0, has_side_effects=True, vmem_limit_bytes=48 * 1024 * 1024),
        )(*[pltpu.with_memory_space_constraint(x, pltpu.HBM) for x in (act_in, norm_first, w_first, w_short, norm_rest, w_rest, bias_rest, jnp.transpose(w_out, (0, 1, 3, 2)), bias_out.reshape(1, out_chans))])
        return jnp.transpose(image, (0, 3, 2, 1))

    return jax.shard_map(local_decode, mesh=mesh, in_specs=(tile_spec,) + (replicated,) * 8, out_specs=tile_spec, check_vma=False)
```

```python
import functools

import jax
import jax.numpy as jnp
from jax import lax
from jax.experimental import pallas as pl
from jax.experimental.pallas import tpu as pltpu
from jax.sharding import PartitionSpec as P

GROUPS = 32
GN_EPS = 1e-6
MESH = pl.DeviceIdType.MESH
LANES = 128
ROW_BLOCK = 2
LAYERS = 7
CHUNKS = 4
BLOCK = 2


def group_total(vec, per_group):
    lane = lax.broadcasted_iota(jnp.int32, vec.shape, 1) & (per_group - 1)
    parts = [vec]
    for dist in range(1, per_group):
        parts.append(jnp.where(lane >= dist, pltpu.roll(vec, dist, 1), pltpu.roll(vec, LANES - per_group + dist, 1)))
    while len(parts) > 1:
        parts = [parts[at] + parts[at + 1] if at + 1 < len(parts) else parts[at] for at in range(0, len(parts), 2)]
    return parts[0]


def far_first(rows_n, cols_n):
    every = [(a, b) for a in range(cols_n) for b in range(rows_n) if a or b]
    return sorted(every, key=lambda off: -(min(off[0], cols_n - off[0]) + min(off[1], rows_n - off[1]) / 2))


def decode_kernel(rows_n, cols_n, act_hbm, nf_hbm, wf_hbm, ws_hbm, nr_hbm, wr_hbm, br_hbm, wo_hbm, bo_hbm, y_ref,
                  act, norm_first, wf, ws, norm_rest, wr, bias_rest, wo_ref, bias_out, sums_first, total_first, wo, mid, hid, bias_rows, pad_first, pad_rest, slab, edge_l, edge_r, turn,
                  st_first, row_first, col_first, cs_first,
                  st_rest, corner_in, row_in, col_in, corner_out, row_out, col_out, whole_inbox,
                  load_sem, first_recv, col_recv, first_send, recv, send):
    samples, rows, cols, _ = act.shape
    pairs = rows // 2
    peers_n = rows_n * cols_n
    sx, sy = lax.axis_index("sx"), lax.axis_index("sy")
    at_x = [sx] + [lax.rem(sx + off, cols_n) for off in range(1, cols_n)]
    at_y = [sy] + [lax.rem(sy + off, rows_n) for off in range(1, rows_n)]
    order = far_first(rows_n, cols_n)
    has_l, has_r, has_t, has_b = sx > 0, sx < cols_n - 1, sy > 0, sy < rows_n - 1

    def device(off):
        return {"sx": at_x[off[0] % cols_n], "sy": at_y[off[1] % rows_n]}

    def wrap(off):
        return (off[0] % cols_n, off[1] % rows_n)

    corner_to = {wrap(off): at for at, off in enumerate(((-1, -1), (1, -1), (-1, 1), (1, 1)))}
    row_to = {wrap(off): at for at, off in enumerate(((0, -1), (0, 1)))}
    col_to = {wrap(off): at for at, off in enumerate(((-1, 0), (1, 0)))}
    plain = [off for off in order if off not in corner_to and off not in row_to]

    half_rows = rows // 2
    loads = []
    for s in range(samples):
        for half in range(2):
            part = pl.ds(half * half_rows, half_rows)
            loads.append(pltpu.make_async_copy(act_hbm.at[s, part], act.at[s, part], load_sem.at[2 * s + half]))
    act_loads = 2 * samples
    others = ((ws_hbm, ws), (br_hbm, bias_rest), (wo_hbm, wo_ref), (nf_hbm, norm_first), (wf_hbm, wf), (wr_hbm, wr), (nr_hbm, norm_rest), (bo_hbm, bias_out))
    for at, (src, dst) in enumerate(others):
        loads.append(pltpu.make_async_copy(src, dst, load_sem.at[act_loads + at]))
    for load in loads[:act_loads]:
        load.start()
    barrier = pltpu.get_barrier_semaphore()
    for off in order:
        pl.semaphore_signal(barrier, inc=1, device_id=device(off), device_id_type=MESH)

    def remote(src, dst, send_to, recv_at, off):
        pltpu.make_async_remote_copy(src_ref=src, dst_ref=dst, send_sem=send_to, recv_sem=recv_at, device_id=device(off), device_id_type=MESH).start()

    def wait_for(ref, sem):
        pltpu.make_async_copy(ref, ref, sem).wait()

    def send_plain(at, s):
        for slot, off in enumerate(plain):
            remote(st_rest.at[at, s, 0], st_rest.at[at, s, 1 + slot], send.at[0], recv.at[at, s], off)

    def send_edges(at, s):
        for off, box in corner_to.items():
            remote(corner_out.at[at, s, box], corner_in.at[at, s, 3 - box], send.at[1], recv.at[at, s], off)
        for off, box in col_to.items():
            remote(col_out.at[at, s, box], col_in.at[at, s, 1 - box], send.at[3], recv.at[at, s], off)
        for off, box in row_to.items():
            remote(row_out.at[at, s, box], row_in.at[at, s, 1 - box], send.at[2], recv.at[at, s], off)

    sub = lax.broadcasted_iota(jnp.int32, (1, 8, LANES), 1)
    first_sub, last_sub = sub == 0, sub == 7

    def tree_sum(stack):
        while stack.shape[0] > 1:
            half = stack.shape[0] // 2
            folded = stack[:half] + stack[half:2 * half]
            stack = folded if stack.shape[0] == 2 * half else jnp.concatenate([folded[:1] + stack[2 * half:], folded[1:]], axis=0) if half > 1 else folded + stack[2 * half:]
        return stack[0]

    def affine(one, two, norm, per_group):
        count = rows * rows_n * cols * cols_n * per_group
        mean = group_total(one, per_group) / count
        square = group_total(two, per_group) / count
        scale = lax.rsqrt(square - mean * mean + GN_EPS) * jnp.broadcast_to(norm[0:1], (8, LANES))
        shift = jnp.broadcast_to(norm[1:2], (8, LANES)) - mean * scale
        return 0.5 * scale, 0.5 * shift

    first_group = 2 * LANES // GROUPS
    lane_in_group = lax.broadcasted_iota(jnp.int32, (8, LANES), 1) & (first_group - 1)

    def silu(x, scales):
        u = x * scales[0] + scales[1]
        return u + u * jnp.tanh(u)

    def spread(rows_of_cols, from_left, from_right):
        v0, v1 = rows_of_cols[:, 0], rows_of_cols[:, 1]
        r0, r1 = pltpu.roll(v0, 1, 1), pltpu.roll(v1, 1, 1)
        q0, q1 = pltpu.roll(v0, 7, 1), pltpu.roll(v1, 7, 1)
        shifted = (
            (jnp.where(first_sub, from_left, r0), jnp.where(first_sub, r0, r1)),
            (v0, v1),
            (jnp.where(last_sub, q1, q0), jnp.where(last_sub, from_right, q1)),
        )
        return [jnp.concatenate(pair, axis=1) for pair in shifted]

    def edges(tile, scales, halo_cols):
        one_row = (scales[0][0:1], scales[1][0:1])
        edge_l[tile] = jnp.where(has_l, silu(halo_cols[0], one_row), 0.0)
        edge_r[tile] = jnp.where(has_r, silu(halo_cols[1], one_row), 0.0)

    def activate(block, tile, scales, halo_rows, corners, row_source, place):
        begin, end = max(0, BLOCK * block + 1), min(rows, BLOCK * (block + 1) + 1)
        value = row_source(begin, end)
        lefts = [jnp.broadcast_to(edge_l[tile, r:r + 1, :], (8, LANES)) for r in range(begin, end)]
        rights = [jnp.broadcast_to(edge_r[tile, r:r + 1, :], (8, LANES)) for r in range(begin, end)]
        value = silu(value, scales)
        for at, has in enumerate((has_t, has_b)):
            if block == (-1, rows // BLOCK - 1)[at]:
                halo = jnp.where(has, silu(halo_rows[at].reshape(1, 2, 8, LANES), scales), 0.0)
                corner_l = jnp.where(jnp.logical_and(has, has_l), silu(corners[2 * at], scales), 0.0)
                corner_r = jnp.where(jnp.logical_and(has, has_r), silu(corners[2 * at + 1], scales), 0.0)
                where_at = 0 if at == 0 else len(lefts)
                value = jnp.concatenate([halo, value] if at == 0 else [value, halo], axis=0)
                lefts.insert(where_at, corner_l)
                rights.insert(where_at, corner_r)
        for off, part in enumerate(spread(value, jnp.stack(lefts), jnp.stack(rights))):
            place(off, tile, BLOCK // 2 * block + 1 if block >= 0 else 0, part.reshape(part.shape[0] // 2, 2, cols, LANES))

    def prepare_rest(at, s, source):
        wait_for(whole_inbox, recv.at[at, s])
        slots = [st_rest[at, s], corner_in[at, s, :, 0:2], row_in[at, s, :, 0:2]]
        total = tree_sum(jnp.concatenate(slots, axis=0))
        one, two = (jnp.broadcast_to(total[which:which + 1], (8, LANES)) for which in range(2))
        scales = affine(one, two, norm_rest[at].astype(jnp.float32), LANES // GROUPS)

        def row_source(begin, end):
            return source[s, begin * cols:end * cols, :].reshape(end - begin, 2, 8, LANES)

        def place(off, tile, pair_at, value):
            for half in range(2):
                pad_rest[off, pair_at:pair_at + value.shape[0], :, half * LANES:(half + 1) * LANES] = value[:, half]

        edges(0, scales, [col_in[at, s, box].astype(jnp.float32) for box in range(2)])
        halo_rows = [row_in[at, s, box, 8:8 + cols, :] for box in range(2)]
        corners = [jnp.broadcast_to(corner_in[at, s, box, 2:3, :], (8, LANES)) for box in range(4)]
        return lambda block: activate(block, 0, scales, halo_rows, corners, row_source, place)

    def prepare_first(s):
        wait_for(col_first.at[s], col_recv.at[s])
        norm = norm_first[...].astype(jnp.float32)

        def one_tile(tile):
            lanes = slice(tile * LANES, (tile + 1) * LANES)
            packed = jnp.broadcast_to(total_first[tile:tile + 1], (8, LANES))
            one, two = (jnp.where(lane_in_group == which * samples + s, packed, 0.0) for which in range(2))
            scales = affine(one, two, norm[:, lanes], first_group)

            def row_source(begin, end):
                return act[s, begin:end, :, lanes].astype(jnp.float32).reshape(end - begin, 2, 8, LANES)

            def place(off, tile, pair_at, value):
                pad_first[off, pair_at:pair_at + value.shape[0], :, :, lanes] = value

            edges(tile, scales, [col_first[s, box, :, lanes].astype(jnp.float32) for box in range(2)])
            halo_rows = [row_first[box, s, :, lanes].astype(jnp.float32) for box in (1, 4)]
            corners = []
            for box in (0, 2, 3, 5):
                row = row_first[box, s, :, lanes].astype(jnp.float32)
                corners.append(pltpu.roll(row[8:16], 1, 0) if box % 3 == 0 else pltpu.roll(row[0:8], 7, 0))
            return lambda block: activate(block, tile, scales, halo_rows, corners, row_source, place)

        tiles = [one_tile(tile) for tile in range(2)]
        return lambda block: [tile(block) for tile in tiles]

    zero = jnp.zeros((LANES, LANES), jnp.bfloat16)
    wide_zero = jnp.zeros((2 * LANES, LANES), jnp.bfloat16)

    def square_of(a, b, c, d):
        return jnp.concatenate([jnp.concatenate([a, b], axis=1), jnp.concatenate([c, d], axis=1)], axis=0)

    def conv_rest(weight, pair_from, pair_n):
        total = None
        for off in range(3):
            w0, w1, w2 = (weight(row_off, off) for row_off in range(3))
            for shift, tap in ((0, square_of(w0, zero, w1, w0)), (1, square_of(w2, w1, zero, w2))):
                lhs = pad_rest[off, pair_from + shift:pair_from + shift + pair_n].reshape(pair_n * cols, 2 * LANES)
                part = jnp.dot(lhs, tap.astype(jnp.float32), preferred_element_type=jnp.float32)
                total = part if total is None else total + part
        return total

    def conv_first(pair_from, pair_n):
        total = None
        for off in range(3):
            w0, w1, w2 = (wf[row_off, off] for row_off in range(3))
            for at, (a, b) in enumerate(((w0, wide_zero), (w1, w0), (w2, w1), (wide_zero, w2))):
                begin = pair_from + at // 2
                lhs = pad_first[off, begin:begin + pair_n, at % 2].reshape(pair_n * cols, 2 * LANES)
                part = jnp.dot(lhs, jnp.concatenate([a, b], axis=1).astype(jnp.float32), preferred_element_type=jnp.float32)
                total = part if total is None else total + part
        return total

    def in_chunks(block, conv, use):
        block(-1)
        done, per_chunk = 0, pairs // CHUNKS
        for chunk in range(CHUNKS):
            while BLOCK // 2 * done < (chunk + 1) * per_chunk:
                block(done)
                done += 1
            total = conv(chunk * per_chunk, per_chunk)
            halves = [total[:, half * LANES:(half + 1) * LANES].reshape(per_chunk, 1, cols, LANES) for half in range(2)]
            use(2 * chunk * per_chunk, jnp.concatenate(halves, axis=1).reshape(2 * per_chunk * cols, LANES))

    def finish(at, s, block, conv, bias, target, residual):
        acc = []

        def use(row, value):
            rows_in = value.shape[0] // cols
            value = value + bias
            if residual is not None:
                value = value + residual[s, row * cols:row * cols + value.shape[0], :]
            value = value.astype(jnp.bfloat16).astype(jnp.float32)
            target[s, row * cols:row * cols + value.shape[0], :] = value
            for edge, edge_row in enumerate((0, rows - 1)):
                if row <= edge_row < row + rows_in:
                    line = value[(edge_row - row) * cols:(edge_row - row + 1) * cols]
                    row_out[at, s, edge, 8:8 + cols, :] = line
                    corner_out[at, s, 2 * edge, 2:3, :] = line[0:1]
                    corner_out[at, s, 2 * edge + 1, 2:3, :] = line[cols - 1:cols]
            for box in range(2):
                column = target[s, pl.ds(row * cols + box * (cols - 1), rows_in, stride=cols), :]
                col_out[at, s, box, row:row + rows_in, :] = column.astype(jnp.bfloat16)
            split = value.reshape(value.shape[0] // 16, 2, 8, LANES)
            acc.append([jnp.sum(split, axis=0), jnp.sum(split * split, axis=0)])

        in_chunks(block, conv, use)
        sums = []
        for which in range(2):
            part = acc[0][which]
            for more in acc[1:]:
                part = part + more[which]
            sums.append(jnp.sum(part[0] + part[1], axis=0, keepdims=True))
        sums = jnp.concatenate(sums, axis=0)
        st_rest[at, s, 0] = sums
        send_plain(at, s)
        for box in range(4):
            corner_out[at, s, box, 0:2, :] = sums
        for box in range(2):
            row_out[at, s, box, 0:2, :] = sums
        send_edges(at, s)

    def first_sums(s, carry):

        def body(step, sums):
            sums = list(sums)
            for at in range(ROW_BLOCK):
                r = step * ROW_BLOCK + at
                for tile in range(2):
                    row = act[s, r, :, tile * LANES:(tile + 1) * LANES].astype(jnp.float32)
                    v0, v1 = row[0:8], row[8:16]
                    slab[0, tile, pl.ds(pl.multiple_of(r * 8, 8), 8), :] = v0
                    slab[1, tile, pl.ds(pl.multiple_of(r * 8, 8), 8), :] = v1
                    sums[2 * tile] = sums[2 * tile] + (v0 + v1)
                    sums[2 * tile + 1] = sums[2 * tile + 1] + (v0 * v0 + v1 * v1)
            return tuple(sums)

        sums = (jnp.zeros((8, LANES), jnp.float32),) * 4
        for half in range(2):
            wait_for(act.at[s, pl.ds(half * half_rows, half_rows)], load_sem.at[2 * s + half])
            sums = lax.fori_loop(half * half_rows // ROW_BLOCK, (half + 1) * half_rows // ROW_BLOCK, body, sums)
        for side in range(2):
            for tile in range(2):
                column = slab[side, tile, pl.ds(7 * side, rows, stride=8), :]
                cs_first[s, side, :, tile * LANES:(tile + 1) * LANES] = column.astype(jnp.bfloat16)
        for tile in range(2):
            for which in range(2):
                sums_first[tile, pl.ds(which * samples + s, 1), :] = jnp.sum(sums[2 * tile + which], axis=0, keepdims=True)
        return carry

    lax.fori_loop(0, samples, first_sums, 0)
    for load in loads[act_loads:]:
        load.start()
    row_at = lax.broadcasted_iota(jnp.int32, (8, LANES), 0)
    for tile in range(2):
        grouped = jnp.where(row_at == lane_in_group, group_total(sums_first[tile], first_group), 0.0)
        st_first[0, tile:tile + 1, :] = jnp.sum(grouped, axis=0, keepdims=True)
    pl.semaphore_wait(barrier, peers_n - 1)
    for slot, off in enumerate(order):
        remote(st_first.at[0], st_first.at[slot + 1], first_send.at[0], first_recv.at[0], off)
    for row, y_off, base in ((0, -1, 3), (rows - 1, 1, 0)):
        for x_off, at in ((-1, 2), (0, 1), (1, 0)):
            remote(act.at[:, row], row_first.at[base + at], first_send.at[1], first_recv.at[1], (x_off, y_off))

    def first_columns(s, carry):
        for off, box in col_to.items():
            remote(cs_first.at[s, box], col_first.at[s, 1 - box], first_send.at[2], col_recv.at[s], off)
        return carry

    lax.fori_loop(0, samples, first_columns, 0)

    for load in loads[act_loads:act_loads + 3]:
        load.wait()
    bias = bias_rest[...].astype(jnp.float32)

    def shortcut(s, carry):
        flat = act[s].reshape(rows * cols, 2 * LANES)
        hid[s] = jnp.dot(flat, ws[...], preferred_element_type=jnp.float32) + bias[6:7]
        return carry

    lax.fori_loop(0, samples, shortcut, 0)
    for tap in range(9):
        three = wo_ref[tap // 3, tap % 3].astype(jnp.float32)
        eight = jnp.concatenate([three, jnp.zeros((8 - three.shape[0], LANES), jnp.float32)], axis=0)
        wo[tap] = jnp.concatenate([eight] * 16, axis=0).T.astype(jnp.bfloat16)
    for load in loads[act_loads + 3:]:
        load.wait()
    wait_for(st_first.at[pl.ds(1, peers_n - 1)], first_recv.at[0])
    total_first[0:2, :] = jnp.sum(st_first[...], axis=0)
    wait_for(row_first, first_recv.at[1])

    def layer_first(s, carry):
        finish(0, s, prepare_first(s), conv_first, bias[0:1], mid, None)
        return carry

    lax.fori_loop(0, samples, layer_first, 0)

    def layer_rest(layer, source, target, residual):
        def one_sample(s, carry):
            block = prepare_rest(layer - 1, s, source)
            conv = functools.partial(conv_rest, lambda row_off, off: wr[layer - 1, row_off, off])
            finish(layer, s, block, conv, bias_rows[pl.ds(layer, 1), :], target, residual)
            return carry

        lax.fori_loop(0, samples, one_sample, 0)

    def layer_pair(step, carry):
        layer_rest(2 * step + 1, mid, hid, hid)
        layer_rest(2 * step + 2, hid, mid, None)
        return carry

    bias_rows[0:bias.shape[0], :] = bias
    lax.fori_loop(0, (LAYERS - 2) // 2, layer_pair, 0)
    layer_rest(LAYERS - 2, mid, hid, hid)

    lane = lax.broadcasted_iota(jnp.int32, (rows, LANES), 1)
    out_bias = bias_out[...].astype(jnp.float32)

    def layer_last(s, carry):
        def use(row, value):
            mid[s, row * cols:row * cols + value.shape[0], :] = value

        in_chunks(prepare_rest(LAYERS - 2, s, hid), functools.partial(conv_rest, lambda row_off, off: wo[3 * row_off + off]), use)
        merged = mid[s, pl.ds(0, rows, stride=cols), :]
        for col in range(1, cols):
            merged = jnp.where(lane // 8 == col, mid[s, pl.ds(col, rows, stride=cols), :], merged)
        turn[...] = jnp.concatenate([merged] * (LANES // rows), axis=0).T
        for chan in range(y_ref.shape[1]):
            plane = turn[pl.ds(chan, cols, stride=8), :]
            y_ref[s, chan] = plane[:, 0:rows] + out_bias[0:1, chan:chan + 1]
        return carry

    lax.fori_loop(0, samples, layer_last, 0)

    wait_for(st_first.at[pl.ds(1, peers_n - 1)], first_send.at[0])
    wait_for(row_first, first_send.at[1])
    wait_for(cs_first, first_send.at[2])
    wait_for(st_rest.at[:, :, pl.ds(1, len(plain))], send.at[0])
    wait_for(corner_out, send.at[1])
    wait_for(row_out, send.at[2])
    wait_for(col_out, send.at[3])


def solution(mesh):
    rows_n, cols_n = mesh.shape["sy"], mesh.shape["sx"]
    peers_n = rows_n * cols_n
    tile_spec = P("dp", "sy", "sx", None)
    replicated = P()

    def local_decode(act_in, norm_first, w_first, w_short, norm_rest, w_rest, bias_rest, w_out, bias_out):
        samples, rows, cols, wide = act_in.shape
        chans = w_short.shape[1]
        out_chans = w_out.shape[3]
        f32, bf16 = jnp.float32, jnp.bfloat16
        rest, plain_n = LAYERS - 1, peers_n - 7
        whole = pl.BlockSpec(memory_space=pltpu.VMEM)
        there = pl.BlockSpec(memory_space=pltpu.HBM)
        image = pl.pallas_call(
            functools.partial(decode_kernel, rows_n, cols_n),
            name="decode",
            out_shape=jax.ShapeDtypeStruct((samples, out_chans, cols, rows), f32),
            in_specs=[there] * 9,
            out_specs=whole,
            scratch_shapes=[
                pltpu.VMEM(act_in.shape, bf16),
                pltpu.VMEM(norm_first.shape, bf16),
                pltpu.VMEM(w_first.shape, bf16),
                pltpu.VMEM(w_short.shape, bf16),
                pltpu.VMEM(norm_rest.shape, bf16),
                pltpu.VMEM(w_rest.shape, bf16),
                pltpu.VMEM(bias_rest.shape, bf16),
                pltpu.VMEM((3, 3, out_chans, chans), bf16),
                pltpu.VMEM((1, out_chans), bf16),
                pltpu.VMEM((2, 8, LANES), f32),
                pltpu.VMEM((8, LANES), f32),
                pltpu.VMEM((9, chans, LANES), bf16),
                pltpu.VMEM((samples, rows * cols, chans), f32),
                pltpu.VMEM((samples, rows * cols, chans), f32),
                pltpu.VMEM((8, chans), f32),
                pltpu.VMEM((3, rows // 2 + 1, 2, cols, wide), f32),
                pltpu.VMEM((3, rows // 2 + 1, cols, 2 * chans), f32),
                pltpu.VMEM((2, 2, rows * 8, LANES), f32),
                pltpu.VMEM((2, rows, LANES), f32),
                pltpu.VMEM((2, rows, LANES), f32),
                pltpu.VMEM((LANES, LANES), f32),
                pltpu.VMEM((peers_n, 2, LANES), f32),
                pltpu.VMEM((6, samples, cols, wide), bf16),
                pltpu.VMEM((samples, 2, rows, wide), bf16),
                pltpu.VMEM((samples, 2, rows, wide), bf16),
                pltpu.VMEM((rest, samples, plain_n + 1, 2, chans), f32),
                pltpu.VMEM((rest, samples, 4, 4, chans), f32),
                pltpu.VMEM((rest, samples, 2, 8 + cols, chans), f32),
                pltpu.VMEM((rest, samples, 2, rows, chans), bf16),
                pltpu.VMEM((rest, samples, 4, 4, chans), f32),
                pltpu.VMEM((rest, samples, 2, 8 + cols, chans), f32),
                pltpu.VMEM((rest, samples, 2, rows, chans), bf16),
                pltpu.VMEM((plain_n + 8 + 8 + cols + rows // 2, 2, chans), f32),
                pltpu.SemaphoreType.DMA((2 * samples + 8,)),
                pltpu.SemaphoreType.DMA((2,)),
                pltpu.SemaphoreType.DMA((samples,)),
                pltpu.SemaphoreType.DMA((3,)),
                pltpu.SemaphoreType.DMA((rest, samples)),
                pltpu.SemaphoreType.DMA((4,)),
            ],
            compiler_params=pltpu.CompilerParams(collective_id=0, has_side_effects=True, vmem_limit_bytes=48 * 1024 * 1024),
        )(*[pltpu.with_memory_space_constraint(x, pltpu.HBM) for x in (act_in, norm_first, w_first, w_short, norm_rest, w_rest, bias_rest, jnp.transpose(w_out, (0, 1, 3, 2)), bias_out.reshape(1, out_chans))])
        return jnp.transpose(image, (0, 3, 2, 1))

    return jax.shard_map(local_decode, mesh=mesh, in_specs=(tile_spec,) + (replicated,) * 8, out_specs=tile_spec, check_vma=False)
```

```python
import functools

import jax
import jax.numpy as jnp
from jax import lax
from jax.experimental import pallas as pl
from jax.experimental.pallas import tpu as pltpu
from jax.sharding import PartitionSpec as P

GROUPS = 32
GN_EPS = 1e-6
MESH = pl.DeviceIdType.MESH
LANES = 128
ROW_BLOCK = 8
LAYERS = 7
CHUNKS = 4
BLOCK = 8


def group_total(vec, per_group):
    lane = lax.broadcasted_iota(jnp.int32, vec.shape, 1) & (per_group - 1)
    parts = [vec]
    for dist in range(1, per_group):
        parts.append(jnp.where(lane >= dist, pltpu.roll(vec, dist, 1), pltpu.roll(vec, LANES - per_group + dist, 1)))
    while len(parts) > 1:
        parts = [parts[at] + parts[at + 1] if at + 1 < len(parts) else parts[at] for at in range(0, len(parts), 2)]
    return parts[0]


def far_first(rows_n, cols_n):
    every = [(a, b) for a in range(cols_n) for b in range(rows_n) if a or b]
    return sorted(every, key=lambda off: -(min(off[0], cols_n - off[0]) + min(off[1], rows_n - off[1]) / 2))


def is_far(off, rows_n, cols_n):
    return min(off[0], cols_n - off[0]) + (min(off[1], rows_n - off[1]) + 1) // 2 > 2


def decode_kernel(rows_n, cols_n, act_hbm, nf_hbm, wf_hbm, ws_hbm, nr_hbm, wr_hbm, br_hbm, wo_hbm, bo_hbm, y_ref,
                  act, norm_first, wf, ws, norm_rest, wr, bias_rest, wo_ref, bias_out, sums_first, total_first, wo, mid, hid, bias_rows, pad_first, pad_rest, slab, edge_l, edge_r, turn,
                  st_first, row_first, col_first, cs_first,
                  st_rest, corner_in, row_in, col_in, corner_out, row_out, col_out, near_inbox,
                  load_sem, first_recv, col_recv, first_send, recv, near_recv, send):
    samples, rows, cols, _ = act.shape
    pairs = rows // 2
    peers_n = rows_n * cols_n
    sx, sy = lax.axis_index("sx"), lax.axis_index("sy")
    at_x = [sx] + [lax.rem(sx + off, cols_n) for off in range(1, cols_n)]
    at_y = [sy] + [lax.rem(sy + off, rows_n) for off in range(1, rows_n)]
    order = far_first(rows_n, cols_n)
    has_l, has_r, has_t, has_b = sx > 0, sx < cols_n - 1, sy > 0, sy < rows_n - 1

    def device(off):
        return {"sx": at_x[off[0] % cols_n], "sy": at_y[off[1] % rows_n]}

    def wrap(off):
        return (off[0] % cols_n, off[1] % rows_n)

    corner_to = {wrap(off): at for at, off in enumerate(((-1, -1), (1, -1), (-1, 1), (1, 1)))}
    row_to = {wrap(off): at for at, off in enumerate(((0, -1), (0, 1)))}
    col_to = {wrap(off): at for at, off in enumerate(((-1, 0), (1, 0)))}
    plain = [off for off in order if off not in corner_to and off not in row_to]
    plain.sort(key=lambda off: not is_far(off, rows_n, cols_n))
    far_n = sum(is_far(off, rows_n, cols_n) for off in plain)

    half_rows = rows // 2
    loads = []
    for s in range(samples):
        for half in range(2):
            part = pl.ds(half * half_rows, half_rows)
            loads.append(pltpu.make_async_copy(act_hbm.at[s, part], act.at[s, part], load_sem.at[2 * s + half]))
    act_loads = 2 * samples
    others = ((ws_hbm, ws), (br_hbm, bias_rest), (wo_hbm, wo_ref), (nf_hbm, norm_first), (wf_hbm, wf), (wr_hbm, wr), (nr_hbm, norm_rest), (bo_hbm, bias_out))
    for at, (src, dst) in enumerate(others):
        loads.append(pltpu.make_async_copy(src, dst, load_sem.at[act_loads + at]))
    for load in loads[:act_loads]:
        load.start()
    barrier = pltpu.get_barrier_semaphore()
    for off in order:
        pl.semaphore_signal(barrier, inc=1, device_id=device(off), device_id_type=MESH)

    def remote(src, dst, send_to, recv_at, off):
        pltpu.make_async_remote_copy(src_ref=src, dst_ref=dst, send_sem=send_to, recv_sem=recv_at, device_id=device(off), device_id_type=MESH).start()

    def wait_for(ref, sem):
        pltpu.make_async_copy(ref, ref, sem).wait()

    def send_far(at, s):
        for slot, off in enumerate(plain[:far_n]):
            remote(st_rest.at[at, 0, s], st_rest.at[at, 1 + slot, s], send.at[0], recv.at[at, s], off)

    def send_near(at, s):
        both, sem = pl.ds(s - 1, 2), near_recv.at[at, s // 2]
        for off, box in col_to.items():
            remote(col_out.at[at, box, both], col_in.at[at, 1 - box, both], send.at[3], sem, off)
        for slot, off in enumerate(plain):
            if slot >= far_n:
                remote(st_rest.at[at, 0, both], st_rest.at[at, 1 + slot, both], send.at[0], sem, off)
        for off, box in corner_to.items():
            remote(corner_out.at[at, box, both], corner_in.at[at, 3 - box, both], send.at[1], sem, off)
        for off, box in row_to.items():
            remote(row_out.at[at, box, both], row_in.at[at, 1 - box, both], send.at[2], sem, off)

    sub = lax.broadcasted_iota(jnp.int32, (1, 8, LANES), 1)
    first_sub, last_sub = sub == 0, sub == 7

    def tree_sum(stack):
        while stack.shape[0] > 1:
            half = stack.shape[0] // 2
            folded = stack[:half] + stack[half:2 * half]
            stack = folded if stack.shape[0] == 2 * half else jnp.concatenate([folded[:1] + stack[2 * half:], folded[1:]], axis=0) if half > 1 else folded + stack[2 * half:]
        return stack[0]

    def affine(one, two, norm, per_group):
        count = rows * rows_n * cols * cols_n * per_group
        mean = group_total(one, per_group) / count
        square = group_total(two, per_group) / count
        scale = lax.rsqrt(square - mean * mean + GN_EPS) * jnp.broadcast_to(norm[0:1], (8, LANES))
        shift = jnp.broadcast_to(norm[1:2], (8, LANES)) - mean * scale
        return 0.5 * scale, 0.5 * shift

    first_group = 2 * LANES // GROUPS
    lane_in_group = lax.broadcasted_iota(jnp.int32, (8, LANES), 1) & (first_group - 1)

    def silu(x, scales):
        u = x * scales[0] + scales[1]
        return u + u * jnp.tanh(u)

    def spread(rows_of_cols, from_left, from_right):
        v0, v1 = rows_of_cols[:, 0], rows_of_cols[:, 1]
        r0, r1 = pltpu.roll(v0, 1, 1), pltpu.roll(v1, 1, 1)
        q0, q1 = pltpu.roll(v0, 7, 1), pltpu.roll(v1, 7, 1)
        shifted = (
            (jnp.where(first_sub, from_left, r0), jnp.where(first_sub, r0, r1)),
            (v0, v1),
            (jnp.where(last_sub, q1, q0), jnp.where(last_sub, from_right, q1)),
        )
        return [jnp.concatenate(pair, axis=1) for pair in shifted]

    def edges(tile, scales, halo_cols):
        one_row = (scales[0][0:1], scales[1][0:1])
        edge_l[tile] = jnp.where(has_l, silu(halo_cols[0], one_row), 0.0)
        edge_r[tile] = jnp.where(has_r, silu(halo_cols[1], one_row), 0.0)

    def activate(block, tile, scales, halo_rows, corners, row_source, place):
        begin, end = max(0, BLOCK * block + 1), min(rows, BLOCK * (block + 1) + 1)
        value = row_source(begin, end)
        lefts = [jnp.broadcast_to(edge_l[tile, r:r + 1, :], (8, LANES)) for r in range(begin, end)]
        rights = [jnp.broadcast_to(edge_r[tile, r:r + 1, :], (8, LANES)) for r in range(begin, end)]
        value = silu(value, scales)
        for at, has in enumerate((has_t, has_b)):
            if block == (-1, rows // BLOCK - 1)[at]:
                halo = jnp.where(has, silu(halo_rows[at].reshape(1, 2, 8, LANES), scales), 0.0)
                corner_l = jnp.where(jnp.logical_and(has, has_l), silu(corners[2 * at], scales), 0.0)
                corner_r = jnp.where(jnp.logical_and(has, has_r), silu(corners[2 * at + 1], scales), 0.0)
                where_at = 0 if at == 0 else len(lefts)
                value = jnp.concatenate([halo, value] if at == 0 else [value, halo], axis=0)
                lefts.insert(where_at, corner_l)
                rights.insert(where_at, corner_r)
        for off, part in enumerate(spread(value, jnp.stack(lefts), jnp.stack(rights))):
            place(off, tile, BLOCK // 2 * block + 1 if block >= 0 else 0, part.reshape(part.shape[0] // 2, 2, cols, LANES))

    def prepare_rest(at, s, source):
        wait_for(st_rest.at[at, pl.ds(1, far_n), s], recv.at[at, s])

        @pl.when(lax.rem(s, 2) == 0)
        def _():
            wait_for(near_inbox, near_recv.at[at, s // 2])

        slots = [st_rest[at, :, s], corner_in[at, :, s, 0:2], row_in[at, :, s, 0:2]]
        total = tree_sum(jnp.concatenate(slots, axis=0))
        one, two = (jnp.broadcast_to(total[which:which + 1], (8, LANES)) for which in range(2))
        scales = affine(one, two, norm_rest[at].astype(jnp.float32), LANES // GROUPS)

        def row_source(begin, end):
            return source[s, begin * cols:end * cols, :].reshape(end - begin, 2, 8, LANES)

        def place(off, tile, pair_at, value):
            for half in range(2):
                pad_rest[off, pair_at:pair_at + value.shape[0], :, half * LANES:(half + 1) * LANES] = value[:, half]

        edges(0, scales, [col_in[at, box, s].astype(jnp.float32) for box in range(2)])
        halo_rows = [row_in[at, box, s, 8:8 + cols, :] for box in range(2)]
        corners = [jnp.broadcast_to(corner_in[at, box, s, 2:3, :], (8, LANES)) for box in range(4)]
        return lambda block: activate(block, 0, scales, halo_rows, corners, row_source, place)

    def prepare_first(s):
        wait_for(col_first.at[s], col_recv.at[s])
        norm = norm_first[...].astype(jnp.float32)

        def one_tile(tile):
            lanes = slice(tile * LANES, (tile + 1) * LANES)
            packed = jnp.broadcast_to(total_first[tile:tile + 1], (8, LANES))
            one, two = (jnp.where(lane_in_group == which * samples + s, packed, 0.0) for which in range(2))
            scales = affine(one, two, norm[:, lanes], first_group)

            def row_source(begin, end):
                return act[s, begin:end, :, lanes].astype(jnp.float32).reshape(end - begin, 2, 8, LANES)

            def place(off, tile, pair_at, value):
                pad_first[off, pair_at:pair_at + value.shape[0], :, :, lanes] = value

            edges(tile, scales, [col_first[s, box, :, lanes].astype(jnp.float32) for box in range(2)])
            halo_rows = [row_first[box, s, :, lanes].astype(jnp.float32) for box in (1, 4)]
            corners = []
            for box in (0, 2, 3, 5):
                row = row_first[box, s, :, lanes].astype(jnp.float32)
                corners.append(pltpu.roll(row[8:16], 1, 0) if box % 3 == 0 else pltpu.roll(row[0:8], 7, 0))
            return lambda block: activate(block, tile, scales, halo_rows, corners, row_source, place)

        tiles = [one_tile(tile) for tile in range(2)]
        return lambda block: [tile(block) for tile in tiles]

    zero = jnp.zeros((LANES, LANES), jnp.bfloat16)
    wide_zero = jnp.zeros((2 * LANES, LANES), jnp.bfloat16)

    def square_of(a, b, c, d):
        return jnp.concatenate([jnp.concatenate([a, b], axis=1), jnp.concatenate([c, d], axis=1)], axis=0)

    def conv_rest(weight, pair_from, pair_n):
        total = None
        for off in range(3):
            w0, w1, w2 = (weight(row_off, off) for row_off in range(3))
            for shift, tap in ((0, square_of(w0, zero, w1, w0)), (1, square_of(w2, w1, zero, w2))):
                lhs = pad_rest[off, pair_from + shift:pair_from + shift + pair_n].reshape(pair_n * cols, 2 * LANES)
                part = jnp.dot(lhs, tap.astype(jnp.float32), preferred_element_type=jnp.float32)
                total = part if total is None else total + part
        return total

    def conv_first(pair_from, pair_n):
        total = None
        for off in range(3):
            w0, w1, w2 = (wf[row_off, off] for row_off in range(3))
            for at, (a, b) in enumerate(((w0, wide_zero), (w1, w0), (w2, w1), (wide_zero, w2))):
                begin = pair_from + at // 2
                lhs = pad_first[off, begin:begin + pair_n, at % 2].reshape(pair_n * cols, 2 * LANES)
                part = jnp.dot(lhs, jnp.concatenate([a, b], axis=1).astype(jnp.float32), preferred_element_type=jnp.float32)
                total = part if total is None else total + part
        return total

    def in_chunks(block, conv, use):
        block(-1)
        done, per_chunk = 0, pairs // CHUNKS
        for chunk in range(CHUNKS):
            while BLOCK // 2 * done < (chunk + 1) * per_chunk:
                block(done)
                done += 1
            total = conv(chunk * per_chunk, per_chunk)
            halves = [total[:, half * LANES:(half + 1) * LANES].reshape(per_chunk, 1, cols, LANES) for half in range(2)]
            use(2 * chunk * per_chunk, jnp.concatenate(halves, axis=1).reshape(2 * per_chunk * cols, LANES))

    def finish(at, s, block, conv, bias, target, residual):
        acc = []

        def use(row, value):
            rows_in = value.shape[0] // cols
            value = value + bias
            if residual is not None:
                value = value + residual[s, row * cols:row * cols + value.shape[0], :]
            value = value.astype(jnp.bfloat16).astype(jnp.float32)
            target[s, row * cols:row * cols + value.shape[0], :] = value
            for edge, edge_row in enumerate((0, rows - 1)):
                if row <= edge_row < row + rows_in:
                    line = value[(edge_row - row) * cols:(edge_row - row + 1) * cols]
                    row_out[at, edge, s, 8:8 + cols, :] = line
                    corner_out[at, 2 * edge, s, 2:3, :] = line[0:1]
                    corner_out[at, 2 * edge + 1, s, 2:3, :] = line[cols - 1:cols]
            for box in range(2):
                column = target[s, pl.ds(row * cols + box * (cols - 1), rows_in, stride=cols), :]
                col_out[at, box, s, row:row + rows_in, :] = column.astype(jnp.bfloat16)
            split = value.reshape(value.shape[0] // 16, 2, 8, LANES)
            acc.append([jnp.sum(split, axis=0), jnp.sum(split * split, axis=0)])

        in_chunks(block, conv, use)
        sums = []
        for which in range(2):
            part = acc[0][which]
            for more in acc[1:]:
                part = part + more[which]
            sums.append(jnp.sum(part[0] + part[1], axis=0, keepdims=True))
        sums = jnp.concatenate(sums, axis=0)
        st_rest[at, 0, s] = sums
        send_far(at, s)
        for box in range(4):
            corner_out[at, box, s, 0:2, :] = sums
        for box in range(2):
            row_out[at, box, s, 0:2, :] = sums
        pl.when(lax.rem(s, 2) == 1)(lambda: send_near(at, s))

    def first_sums(s, carry):

        def body(step, sums):
            sums = list(sums)
            for at in range(ROW_BLOCK):
                r = step * ROW_BLOCK + at
                for tile in range(2):
                    row = act[s, r, :, tile * LANES:(tile + 1) * LANES].astype(jnp.float32)
                    v0, v1 = row[0:8], row[8:16]
                    slab[0, tile, pl.ds(pl.multiple_of(r * 8, 8), 8), :] = v0
                    slab[1, tile, pl.ds(pl.multiple_of(r * 8, 8), 8), :] = v1
                    sums[2 * tile] = sums[2 * tile] + (v0 + v1)
                    sums[2 * tile + 1] = sums[2 * tile + 1] + (v0 * v0 + v1 * v1)
            return tuple(sums)

        sums = (jnp.zeros((8, LANES), jnp.float32),) * 4
        for half in range(2):
            wait_for(act.at[s, pl.ds(half * half_rows, half_rows)], load_sem.at[2 * s + half])
            sums = lax.fori_loop(half * half_rows // ROW_BLOCK, (half + 1) * half_rows // ROW_BLOCK, body, sums)
        for side in range(2):
            for tile in range(2):
                column = slab[side, tile, pl.ds(7 * side, rows, stride=8), :]
                cs_first[s, side, :, tile * LANES:(tile + 1) * LANES] = column.astype(jnp.bfloat16)
        for tile in range(2):
            for which in range(2):
                sums_first[tile, pl.ds(which * samples + s, 1), :] = jnp.sum(sums[2 * tile + which], axis=0, keepdims=True)
        return carry

    lax.fori_loop(0, samples, first_sums, 0)
    for load in loads[act_loads:]:
        load.start()
    row_at = lax.broadcasted_iota(jnp.int32, (8, LANES), 0)
    for tile in range(2):
        grouped = jnp.where(row_at == lane_in_group, group_total(sums_first[tile], first_group), 0.0)
        st_first[0, tile:tile + 1, :] = jnp.sum(grouped, axis=0, keepdims=True)
    pl.semaphore_wait(barrier, peers_n - 1)
    for slot, off in enumerate(order):
        remote(st_first.at[0], st_first.at[slot + 1], first_send.at[0], first_recv.at[0], off)
    for row, y_off, base in ((0, -1, 3), (rows - 1, 1, 0)):
        for x_off, at in ((-1, 2), (0, 1), (1, 0)):
            remote(act.at[:, row], row_first.at[base + at], first_send.at[1], first_recv.at[1], (x_off, y_off))

    def first_columns(s, carry):
        for off, box in col_to.items():
            remote(cs_first.at[s, box], col_first.at[s, 1 - box], first_send.at[2], col_recv.at[s], off)
        return carry

    lax.fori_loop(0, samples, first_columns, 0)

    for load in loads[act_loads:act_loads + 3]:
        load.wait()
    bias = bias_rest[...].astype(jnp.float32)

    def shortcut(s, carry):
        flat = act[s].reshape(rows * cols, 2 * LANES)
        hid[s] = jnp.dot(flat, ws[...], preferred_element_type=jnp.float32) + bias[6:7]
        return carry

    lax.fori_loop(0, samples, shortcut, 0)
    for tap in range(9):
        three = wo_ref[tap // 3, tap % 3].astype(jnp.float32)
        eight = jnp.concatenate([three, jnp.zeros((8 - three.shape[0], LANES), jnp.float32)], axis=0)
        wo[tap] = jnp.concatenate([eight] * 16, axis=0).T.astype(jnp.bfloat16)
    for load in loads[act_loads + 3:]:
        load.wait()
    wait_for(st_first.at[pl.ds(1, peers_n - 1)], first_recv.at[0])
    total_first[0:2, :] = jnp.sum(st_first[...], axis=0)
    wait_for(row_first, first_recv.at[1])

    def layer_first(s, carry):
        finish(0, s, prepare_first(s), conv_first, bias[0:1], mid, None)
        return carry

    lax.fori_loop(0, samples, layer_first, 0)

    def layer_rest(layer, source, target, residual):
        def one_sample(s, carry):
            block = prepare_rest(layer - 1, s, source)
            conv = functools.partial(conv_rest, lambda row_off, off: wr[layer - 1, row_off, off])
            finish(layer, s, block, conv, bias_rows[pl.ds(layer, 1), :], target, residual)
            return carry

        lax.fori_loop(0, samples, one_sample, 0)

    def layer_pair(step, carry):
        layer_rest(2 * step + 1, mid, hid, hid)
        layer_rest(2 * step + 2, hid, mid, None)
        return carry

    bias_rows[0:bias.shape[0], :] = bias
    lax.fori_loop(0, (LAYERS - 2) // 2, layer_pair, 0)
    layer_rest(LAYERS - 2, mid, hid, hid)

    lane = lax.broadcasted_iota(jnp.int32, (rows, LANES), 1)
    out_bias = bias_out[...].astype(jnp.float32)

    def layer_last(s, carry):
        def use(row, value):
            mid[s, row * cols:row * cols + value.shape[0], :] = value

        in_chunks(prepare_rest(LAYERS - 2, s, hid), functools.partial(conv_rest, lambda row_off, off: wo[3 * row_off + off]), use)
        merged = mid[s, pl.ds(0, rows, stride=cols), :]
        for col in range(1, cols):
            merged = jnp.where(lane // 8 == col, mid[s, pl.ds(col, rows, stride=cols), :], merged)
        turn[...] = jnp.concatenate([merged] * (LANES // rows), axis=0).T
        for chan in range(y_ref.shape[1]):
            plane = turn[pl.ds(chan, cols, stride=8), :]
            y_ref[s, chan] = plane[:, 0:rows] + out_bias[0:1, chan:chan + 1]
        return carry

    lax.fori_loop(0, samples, layer_last, 0)

    wait_for(st_first.at[pl.ds(1, peers_n - 1)], first_send.at[0])
    wait_for(row_first, first_send.at[1])
    wait_for(cs_first, first_send.at[2])
    wait_for(st_rest.at[:, pl.ds(1, len(plain))], send.at[0])
    wait_for(corner_out, send.at[1])
    wait_for(row_out, send.at[2])
    wait_for(col_out, send.at[3])


def solution(mesh):
    rows_n, cols_n = mesh.shape["sy"], mesh.shape["sx"]
    peers_n = rows_n * cols_n
    tile_spec = P("dp", "sy", "sx", None)
    replicated = P()

    def local_decode(act_in, norm_first, w_first, w_short, norm_rest, w_rest, bias_rest, w_out, bias_out):
        samples, rows, cols, wide = act_in.shape
        chans = w_short.shape[1]
        out_chans = w_out.shape[3]
        f32, bf16 = jnp.float32, jnp.bfloat16
        rest, plain_n = LAYERS - 1, peers_n - 7
        far_n = sum(is_far(off, rows_n, cols_n) for off in far_first(rows_n, cols_n))
        whole = pl.BlockSpec(memory_space=pltpu.VMEM)
        there = pl.BlockSpec(memory_space=pltpu.HBM)
        image = pl.pallas_call(
            functools.partial(decode_kernel, rows_n, cols_n),
            name="decode",
            out_shape=jax.ShapeDtypeStruct((samples, out_chans, cols, rows), f32),
            in_specs=[there] * 9,
            out_specs=whole,
            scratch_shapes=[
                pltpu.VMEM(act_in.shape, bf16),
                pltpu.VMEM(norm_first.shape, bf16),
                pltpu.VMEM(w_first.shape, bf16),
                pltpu.VMEM(w_short.shape, bf16),
                pltpu.VMEM(norm_rest.shape, bf16),
                pltpu.VMEM(w_rest.shape, bf16),
                pltpu.VMEM(bias_rest.shape, bf16),
                pltpu.VMEM((3, 3, out_chans, chans), bf16),
                pltpu.VMEM((1, out_chans), bf16),
                pltpu.VMEM((2, 8, LANES), f32),
                pltpu.VMEM((8, LANES), f32),
                pltpu.VMEM((9, chans, LANES), bf16),
                pltpu.VMEM((samples, rows * cols, chans), f32),
                pltpu.VMEM((samples, rows * cols, chans), f32),
                pltpu.VMEM((8, chans), f32),
                pltpu.VMEM((3, rows // 2 + 1, 2, cols, wide), f32),
                pltpu.VMEM((3, rows // 2 + 1, cols, 2 * chans), f32),
                pltpu.VMEM((2, 2, rows * 8, LANES), f32),
                pltpu.VMEM((2, rows, LANES), f32),
                pltpu.VMEM((2, rows, LANES), f32),
                pltpu.VMEM((LANES, LANES), f32),
                pltpu.VMEM((peers_n, 2, LANES), f32),
                pltpu.VMEM((6, samples, cols, wide), bf16),
                pltpu.VMEM((samples, 2, rows, wide), bf16),
                pltpu.VMEM((samples, 2, rows, wide), bf16),
                pltpu.VMEM((rest, plain_n + 1, samples, 2, chans), f32),
                pltpu.VMEM((rest, 4, samples, 4, chans), f32),
                pltpu.VMEM((rest, 2, samples, 8 + cols, chans), f32),
                pltpu.VMEM((rest, 2, samples, rows, chans), bf16),
                pltpu.VMEM((rest, 4, samples, 4, chans), f32),
                pltpu.VMEM((rest, 2, samples, 8 + cols, chans), f32),
                pltpu.VMEM((rest, 2, samples, rows, chans), bf16),
                pltpu.VMEM((2, plain_n - far_n + 8 + 8 + cols + rows // 2, 2, chans), f32),
                pltpu.SemaphoreType.DMA((2 * samples + 8,)),
                pltpu.SemaphoreType.DMA((2,)),
                pltpu.SemaphoreType.DMA((samples,)),
                pltpu.SemaphoreType.DMA((3,)),
                pltpu.SemaphoreType.DMA((rest, samples)),
                pltpu.SemaphoreType.DMA((rest, samples // 2)),
                pltpu.SemaphoreType.DMA((4,)),
            ],
            compiler_params=pltpu.CompilerParams(collective_id=0, has_side_effects=True, vmem_limit_bytes=48 * 1024 * 1024),
        )(*[pltpu.with_memory_space_constraint(x, pltpu.HBM) for x in (act_in, norm_first, w_first, w_short, norm_rest, w_rest, bias_rest, jnp.transpose(w_out, (0, 1, 3, 2)), bias_out.reshape(1, out_chans))])
        return jnp.transpose(image, (0, 3, 2, 1))

    return jax.shard_map(local_decode, mesh=mesh, in_specs=(tile_spec,) + (replicated,) * 8, out_specs=tile_spec, check_vma=False)
```

```python
import functools

import jax
import jax.numpy as jnp
from jax import lax
from jax.experimental import pallas as pl
from jax.experimental.pallas import tpu as pltpu
from jax.sharding import PartitionSpec as P

GROUPS = 32
GN_EPS = 1e-6
MESH = pl.DeviceIdType.MESH
LANES = 128
ROW_BLOCK = 2
LAYERS = 7
CHUNKS = (10, 12, 10)
BLOCK = 2


def group_total(vec, per_group):
    lane = lax.broadcasted_iota(jnp.int32, vec.shape, 1) & (per_group - 1)
    parts = [vec]
    for dist in range(1, per_group):
        parts.append(jnp.where(lane >= dist, pltpu.roll(vec, dist, 1), pltpu.roll(vec, LANES - per_group + dist, 1)))
    while len(parts) > 1:
        parts = [parts[at] + parts[at + 1] if at + 1 < len(parts) else parts[at] for at in range(0, len(parts), 2)]
    return parts[0]


def far_first(rows_n, cols_n):
    every = [(a, b) for a in range(cols_n) for b in range(rows_n) if a or b]
    return sorted(every, key=lambda off: -(min(off[0], cols_n - off[0]) + min(off[1], rows_n - off[1]) / 2))


def decode_kernel(rows_n, cols_n, act_hbm, nf_hbm, wf_hbm, ws_hbm, nr_hbm, wr_hbm, br_hbm, wo_hbm, bo_hbm, y_ref,
                  act, norm_first, wf, ws, norm_rest, wr, bias_rest, wo_ref, bias_out, sums_first, total_first, wo, mid, hid, bias_rows, pad_first, pad_rest, slab, edge_l, edge_r, turn,
                  st_first, row_first, col_first, cs_first,
                  st_rest, corner_in, row_in, col_in, corner_out, row_out, col_out, whole_inbox,
                  load_sem, first_recv, col_recv, first_send, recv, send):
    samples, rows, cols, _ = act.shape
    pairs = rows // 2
    peers_n = rows_n * cols_n
    sx, sy = lax.axis_index("sx"), lax.axis_index("sy")
    at_x = [sx] + [lax.rem(sx + off, cols_n) for off in range(1, cols_n)]
    at_y = [sy] + [lax.rem(sy + off, rows_n) for off in range(1, rows_n)]
    order = far_first(rows_n, cols_n)
    has_l, has_r, has_t, has_b = sx > 0, sx < cols_n - 1, sy > 0, sy < rows_n - 1

    def device(off):
        return {"sx": at_x[off[0] % cols_n], "sy": at_y[off[1] % rows_n]}

    def wrap(off):
        return (off[0] % cols_n, off[1] % rows_n)

    corner_to = {wrap(off): at for at, off in enumerate(((-1, -1), (1, -1), (-1, 1), (1, 1)))}
    row_to = {wrap(off): at for at, off in enumerate(((0, -1), (0, 1)))}
    col_to = {wrap(off): at for at, off in enumerate(((-1, 0), (1, 0)))}
    plain = [off for off in order if off not in corner_to and off not in row_to and off not in col_to]

    half_rows = rows // 2
    loads = []
    for s in range(samples):
        for half in range(2):
            part = pl.ds(half * half_rows, half_rows)
            loads.append(pltpu.make_async_copy(act_hbm.at[s, part], act.at[s, part], load_sem.at[2 * s + half]))
    act_loads = 2 * samples
    others = ((ws_hbm, ws), (br_hbm, bias_rest), (wo_hbm, wo_ref), (nf_hbm, norm_first), (wf_hbm, wf), (wr_hbm, wr), (nr_hbm, norm_rest), (bo_hbm, bias_out))
    for at, (src, dst) in enumerate(others):
        loads.append(pltpu.make_async_copy(src, dst, load_sem.at[act_loads + at]))
    for load in loads[:act_loads]:
        load.start()
    barrier = pltpu.get_barrier_semaphore()
    for off in order:
        pl.semaphore_signal(barrier, inc=1, device_id=device(off), device_id_type=MESH)

    def remote(src, dst, send_to, recv_at, off):
        pltpu.make_async_remote_copy(src_ref=src, dst_ref=dst, send_sem=send_to, recv_sem=recv_at, device_id=device(off), device_id_type=MESH).start()

    def wait_for(ref, sem):
        pltpu.make_async_copy(ref, ref, sem).wait()

    def send_plain(at, s):
        for slot, off in enumerate(plain):
            remote(st_rest.at[at, s, 0], st_rest.at[at, s, 1 + slot], send.at[0], recv.at[at, s], off)

    def send_edges(at, s):
        for off, box in corner_to.items():
            remote(corner_out.at[at, s, box], corner_in.at[at, s, 3 - box], send.at[1], recv.at[at, s], off)
        for off, box in col_to.items():
            remote(col_out.at[at, s, box], col_in.at[at, s, 1 - box], send.at[3], recv.at[at, s], off)
        for off, box in row_to.items():
            remote(row_out.at[at, s, box], row_in.at[at, s, 1 - box], send.at[2], recv.at[at, s], off)

    sub = lax.broadcasted_iota(jnp.int32, (1, 8, LANES), 1)
    first_sub, last_sub = sub == 0, sub == 7

    def tree_sum(stack):
        while stack.shape[0] > 1:
            half = stack.shape[0] // 2
            folded = stack[:half] + stack[half:2 * half]
            stack = folded if stack.shape[0] == 2 * half else jnp.concatenate([folded[:1] + stack[2 * half:], folded[1:]], axis=0) if half > 1 else folded + stack[2 * half:]
        return stack[0]

    def affine(one, two, norm, per_group):
        count = rows * rows_n * cols * cols_n * per_group
        mean = group_total(one, per_group) / count
        square = group_total(two, per_group) / count
        scale = lax.rsqrt(square - mean * mean + GN_EPS) * jnp.broadcast_to(norm[0:1], (8, LANES))
        shift = jnp.broadcast_to(norm[1:2], (8, LANES)) - mean * scale
        return 0.5 * scale, 0.5 * shift

    first_group = 2 * LANES // GROUPS
    lane_in_group = lax.broadcasted_iota(jnp.int32, (8, LANES), 1) & (first_group - 1)

    def silu(x, scales):
        u = x * scales[0] + scales[1]
        return u + u * jnp.tanh(u)

    def spread(rows_of_cols, from_left, from_right):
        v0, v1 = rows_of_cols[:, 0], rows_of_cols[:, 1]
        r0, r1 = pltpu.roll(v0, 1, 1), pltpu.roll(v1, 1, 1)
        q0, q1 = pltpu.roll(v0, 7, 1), pltpu.roll(v1, 7, 1)
        shifted = (
            (jnp.where(first_sub, from_left, r0), jnp.where(first_sub, r0, r1)),
            (v0, v1),
            (jnp.where(last_sub, q1, q0), jnp.where(last_sub, from_right, q1)),
        )
        return [jnp.concatenate(pair, axis=1) for pair in shifted]

    def edges(tile, scales, halo_cols):
        one_row = (scales[0][0:1], scales[1][0:1])
        edge_l[tile] = jnp.where(has_l, silu(halo_cols[0], one_row), 0.0)
        edge_r[tile] = jnp.where(has_r, silu(halo_cols[1], one_row), 0.0)

    def activate(block, tile, scales, halo_rows, corners, row_source, place):
        begin, end = max(0, BLOCK * block + 1), min(rows, BLOCK * (block + 1) + 1)
        value = row_source(begin, end)
        lefts = [jnp.broadcast_to(edge_l[tile, r:r + 1, :], (8, LANES)) for r in range(begin, end)]
        rights = [jnp.broadcast_to(edge_r[tile, r:r + 1, :], (8, LANES)) for r in range(begin, end)]
        value = silu(value, scales)
        for at, has in enumerate((has_t, has_b)):
            if block == (-1, rows // BLOCK - 1)[at]:
                halo = jnp.where(has, silu(halo_rows[at].reshape(1, 2, 8, LANES), scales), 0.0)
                corner_l = jnp.where(jnp.logical_and(has, has_l), silu(corners[2 * at], scales), 0.0)
                corner_r = jnp.where(jnp.logical_and(has, has_r), silu(corners[2 * at + 1], scales), 0.0)
                where_at = 0 if at == 0 else len(lefts)
                value = jnp.concatenate([halo, value] if at == 0 else [value, halo], axis=0)
                lefts.insert(where_at, corner_l)
                rights.insert(where_at, corner_r)
        for off, part in enumerate(spread(value, jnp.stack(lefts), jnp.stack(rights))):
            place(off, tile, BLOCK // 2 * block + 1 if block >= 0 else 0, part.reshape(part.shape[0] // 2, 2, cols, LANES))

    def prepare_rest(at, s, source):
        wait_for(whole_inbox, recv.at[at, s])
        slots = [st_rest[at, s], corner_in[at, s, :, 0:2], row_in[at, s, :, 0:2], col_in[at, s, :, 0:2]]
        total = tree_sum(jnp.concatenate(slots, axis=0))
        one, two = (jnp.broadcast_to(total[which:which + 1], (8, LANES)) for which in range(2))
        scales = affine(one, two, norm_rest[at].astype(jnp.float32), LANES // GROUPS)

        def row_source(begin, end):
            return source[s, begin * cols:end * cols, :].reshape(end - begin, 2, 8, LANES)

        def place(off, tile, pair_at, value):
            for half in range(2):
                pad_rest[off, pair_at:pair_at + value.shape[0], :, half * LANES:(half + 1) * LANES] = value[:, half]

        edges(0, scales, [col_in[at, s, box, 8:8 + rows, :] for box in range(2)])
        halo_rows = [row_in[at, s, box, 8:8 + cols, :] for box in range(2)]
        corners = [jnp.broadcast_to(corner_in[at, s, box, 2:3, :], (8, LANES)) for box in range(4)]
        return lambda block: activate(block, 0, scales, halo_rows, corners, row_source, place)

    def prepare_first(s):
        wait_for(col_first.at[s], col_recv.at[s])
        norm = norm_first[...].astype(jnp.float32)

        def one_tile(tile):
            lanes = slice(tile * LANES, (tile + 1) * LANES)
            packed = jnp.broadcast_to(total_first[tile:tile + 1], (8, LANES))
            one, two = (jnp.where(lane_in_group == which * samples + s, packed, 0.0) for which in range(2))
            scales = affine(one, two, norm[:, lanes], first_group)

            def row_source(begin, end):
                return act[s, begin:end, :, lanes].astype(jnp.float32).reshape(end - begin, 2, 8, LANES)

            def place(off, tile, pair_at, value):
                pad_first[off, pair_at:pair_at + value.shape[0], :, :, lanes] = value

            edges(tile, scales, [col_first[s, box, :, lanes].astype(jnp.float32) for box in range(2)])
            halo_rows = [row_first[box, s, :, lanes].astype(jnp.float32) for box in (1, 4)]
            corners = []
            for box in (0, 2, 3, 5):
                row = row_first[box, s, :, lanes].astype(jnp.float32)
                corners.append(pltpu.roll(row[8:16], 1, 0) if box % 3 == 0 else pltpu.roll(row[0:8], 7, 0))
            return lambda block: activate(block, tile, scales, halo_rows, corners, row_source, place)

        tiles = [one_tile(tile) for tile in range(2)]
        return lambda block: [tile(block) for tile in tiles]

    zero = jnp.zeros((LANES, LANES), jnp.bfloat16)
    wide_zero = jnp.zeros((2 * LANES, LANES), jnp.bfloat16)

    def square_of(a, b, c, d):
        return jnp.concatenate([jnp.concatenate([a, b], axis=1), jnp.concatenate([c, d], axis=1)], axis=0)

    def conv_rest(weight, pair_from, pair_n):
        total = None
        for off in range(3):
            w0, w1, w2 = (weight(row_off, off) for row_off in range(3))
            for shift, tap in ((0, square_of(w0, zero, w1, w0)), (1, square_of(w2, w1, zero, w2))):
                lhs = pad_rest[off, pair_from + shift:pair_from + shift + pair_n].reshape(pair_n * cols, 2 * LANES)
                part = jnp.dot(lhs, tap.astype(jnp.float32), preferred_element_type=jnp.float32)
                total = part if total is None else total + part
        return total

    def conv_first(pair_from, pair_n):
        total = None
        for off in range(3):
            w0, w1, w2 = (wf[row_off, off] for row_off in range(3))
            for at, (a, b) in enumerate(((w0, wide_zero), (w1, w0), (w2, w1), (wide_zero, w2))):
                begin = pair_from + at // 2
                lhs = pad_first[off, begin:begin + pair_n, at % 2].reshape(pair_n * cols, 2 * LANES)
                part = jnp.dot(lhs, jnp.concatenate([a, b], axis=1).astype(jnp.float32), preferred_element_type=jnp.float32)
                total = part if total is None else total + part
        return total

    def in_chunks(block, conv, use):
        block(-1)
        done, begin = 0, 0
        for chunk in CHUNKS:
            per_chunk = chunk * pairs // sum(CHUNKS)
            while BLOCK // 2 * done < begin + per_chunk:
                block(done)
                done += 1
            total = conv(begin, per_chunk)
            halves = [total[:, half * LANES:(half + 1) * LANES].reshape(per_chunk, 1, cols, LANES) for half in range(2)]
            use(2 * begin, jnp.concatenate(halves, axis=1).reshape(2 * per_chunk * cols, LANES))
            begin += per_chunk

    def finish(at, s, block, conv, bias, target, residual):
        acc = []

        def use(row, value):
            rows_in = value.shape[0] // cols
            value = value + bias
            if residual is not None:
                value = value + residual[s, row * cols:row * cols + value.shape[0], :]
            value = value.astype(jnp.bfloat16).astype(jnp.float32)
            target[s, row * cols:row * cols + value.shape[0], :] = value
            for edge, edge_row in enumerate((0, rows - 1)):
                if row <= edge_row < row + rows_in:
                    line = value[(edge_row - row) * cols:(edge_row - row + 1) * cols]
                    row_out[at, s, edge, 8:8 + cols, :] = line
                    corner_out[at, s, 2 * edge, 2:3, :] = line[0:1]
                    corner_out[at, s, 2 * edge + 1, 2:3, :] = line[cols - 1:cols]
            for box in range(2):
                column = target[s, pl.ds(row * cols + box * (cols - 1), rows_in, stride=cols), :]
                col_out[at, s, box, 8 + row:8 + row + rows_in, :] = column
            split = value.reshape(value.shape[0] // 16, 2, 8, LANES)
            acc.append([jnp.sum(split, axis=0), jnp.sum(split * split, axis=0)])

        in_chunks(block, conv, use)
        sums = []
        for which in range(2):
            part = acc[0][which]
            for more in acc[1:]:
                part = part + more[which]
            sums.append(jnp.sum(part[0] + part[1], axis=0, keepdims=True))
        sums = jnp.concatenate(sums, axis=0)
        st_rest[at, s, 0] = sums
        send_plain(at, s)
        for box in range(4):
            corner_out[at, s, box, 0:2, :] = sums
        for box in range(2):
            row_out[at, s, box, 0:2, :] = sums
            col_out[at, s, box, 0:2, :] = sums
        send_edges(at, s)

    def first_sums(s, carry):

        def body(step, sums):
            sums = list(sums)
            for at in range(ROW_BLOCK):
                r = step * ROW_BLOCK + at
                for tile in range(2):
                    row = act[s, r, :, tile * LANES:(tile + 1) * LANES].astype(jnp.float32)
                    v0, v1 = row[0:8], row[8:16]
                    slab[0, tile, pl.ds(pl.multiple_of(r * 8, 8), 8), :] = v0
                    slab[1, tile, pl.ds(pl.multiple_of(r * 8, 8), 8), :] = v1
                    sums[2 * tile] = sums[2 * tile] + (v0 + v1)
                    sums[2 * tile + 1] = sums[2 * tile + 1] + (v0 * v0 + v1 * v1)
            return tuple(sums)

        sums = (jnp.zeros((8, LANES), jnp.float32),) * 4
        for half in range(2):
            wait_for(act.at[s, pl.ds(half * half_rows, half_rows)], load_sem.at[2 * s + half])
            sums = lax.fori_loop(half * half_rows // ROW_BLOCK, (half + 1) * half_rows // ROW_BLOCK, body, sums)
        for side in range(2):
            for tile in range(2):
                column = slab[side, tile, pl.ds(7 * side, rows, stride=8), :]
                cs_first[s, side, :, tile * LANES:(tile + 1) * LANES] = column.astype(jnp.bfloat16)
        for tile in range(2):
            for which in range(2):
                sums_first[tile, pl.ds(which * samples + s, 1), :] = jnp.sum(sums[2 * tile + which], axis=0, keepdims=True)
        return carry

    lax.fori_loop(0, samples, first_sums, 0)
    for load in loads[act_loads:]:
        load.start()
    row_at = lax.broadcasted_iota(jnp.int32, (8, LANES), 0)
    for tile in range(2):
        grouped = jnp.where(row_at == lane_in_group, group_total(sums_first[tile], first_group), 0.0)
        st_first[0, tile:tile + 1, :] = jnp.sum(grouped, axis=0, keepdims=True)
    pl.semaphore_wait(barrier, peers_n - 1)
    for slot, off in enumerate(order):
        remote(st_first.at[0], st_first.at[slot + 1], first_send.at[0], first_recv.at[0], off)
    for row, y_off, base in ((0, -1, 3), (rows - 1, 1, 0)):
        for x_off, at in ((-1, 2), (0, 1), (1, 0)):
            remote(act.at[:, row], row_first.at[base + at], first_send.at[1], first_recv.at[1], (x_off, y_off))

    def first_columns(s, carry):
        for off, box in col_to.items():
            remote(cs_first.at[s, box], col_first.at[s, 1 - box], first_send.at[2], col_recv.at[s], off)
        return carry

    lax.fori_loop(0, samples, first_columns, 0)

    for load in loads[act_loads:act_loads + 3]:
        load.wait()
    bias = bias_rest[...].astype(jnp.float32)

    def shortcut(s, carry):
        flat = act[s].reshape(rows * cols, 2 * LANES)
        hid[s] = jnp.dot(flat, ws[...], preferred_element_type=jnp.float32) + bias[6:7]
        return carry

    lax.fori_loop(0, samples, shortcut, 0)
    for tap in range(9):
        three = wo_ref[tap // 3, tap % 3].astype(jnp.float32)
        eight = jnp.concatenate([three, jnp.zeros((8 - three.shape[0], LANES), jnp.float32)], axis=0)
        wo[tap] = jnp.concatenate([eight] * 16, axis=0).T.astype(jnp.bfloat16)
    for load in loads[act_loads + 3:]:
        load.wait()
    wait_for(st_first.at[pl.ds(1, peers_n - 1)], first_recv.at[0])
    total_first[0:2, :] = jnp.sum(st_first[...], axis=0)
    wait_for(row_first, first_recv.at[1])

    def layer_first(s, carry):
        finish(0, s, prepare_first(s), conv_first, bias[0:1], mid, None)
        return carry

    lax.fori_loop(0, samples, layer_first, 0)

    def layer_rest(layer, source, target, residual):
        def one_sample(s, carry):
            block = prepare_rest(layer - 1, s, source)
            conv = functools.partial(conv_rest, lambda row_off, off: wr[layer - 1, row_off, off])
            finish(layer, s, block, conv, bias_rows[pl.ds(layer, 1), :], target, residual)
            return carry

        lax.fori_loop(0, samples, one_sample, 0)

    def layer_pair(step, carry):
        layer_rest(2 * step + 1, mid, hid, hid)
        layer_rest(2 * step + 2, hid, mid, None)
        return carry

    bias_rows[0:bias.shape[0], :] = bias
    lax.fori_loop(0, (LAYERS - 2) // 2, layer_pair, 0)
    layer_rest(LAYERS - 2, mid, hid, hid)

    lane = lax.broadcasted_iota(jnp.int32, (rows, LANES), 1)
    out_bias = bias_out[...].astype(jnp.float32)

    def layer_last(s, carry):
        def use(row, value):
            mid[s, row * cols:row * cols + value.shape[0], :] = value

        in_chunks(prepare_rest(LAYERS - 2, s, hid), functools.partial(conv_rest, lambda row_off, off: wo[3 * row_off + off]), use)
        merged = mid[s, pl.ds(0, rows, stride=cols), :]
        for col in range(1, cols):
            merged = jnp.where(lane // 8 == col, mid[s, pl.ds(col, rows, stride=cols), :], merged)
        turn[...] = jnp.concatenate([merged] * (LANES // rows), axis=0).T
        for chan in range(y_ref.shape[1]):
            plane = turn[pl.ds(chan, cols, stride=8), :]
            y_ref[s, chan] = plane[:, 0:rows] + out_bias[0:1, chan:chan + 1]
        return carry

    lax.fori_loop(0, samples, layer_last, 0)

    wait_for(st_first.at[pl.ds(1, peers_n - 1)], first_send.at[0])
    wait_for(row_first, first_send.at[1])
    wait_for(cs_first, first_send.at[2])
    wait_for(st_rest.at[:, :, pl.ds(1, len(plain))], send.at[0])
    wait_for(corner_out, send.at[1])
    wait_for(row_out, send.at[2])
    wait_for(col_out, send.at[3])


def solution(mesh):
    rows_n, cols_n = mesh.shape["sy"], mesh.shape["sx"]
    peers_n = rows_n * cols_n
    tile_spec = P("dp", "sy", "sx", None)
    replicated = P()

    def local_decode(act_in, norm_first, w_first, w_short, norm_rest, w_rest, bias_rest, w_out, bias_out):
        samples, rows, cols, wide = act_in.shape
        chans = w_short.shape[1]
        out_chans = w_out.shape[3]
        f32, bf16 = jnp.float32, jnp.bfloat16
        rest, plain_n = LAYERS - 1, peers_n - 9
        whole = pl.BlockSpec(memory_space=pltpu.VMEM)
        there = pl.BlockSpec(memory_space=pltpu.HBM)
        image = pl.pallas_call(
            functools.partial(decode_kernel, rows_n, cols_n),
            name="decode",
            out_shape=jax.ShapeDtypeStruct((samples, out_chans, cols, rows), f32),
            in_specs=[there] * 9,
            out_specs=whole,
            scratch_shapes=[
                pltpu.VMEM(act_in.shape, bf16),
                pltpu.VMEM(norm_first.shape, bf16),
                pltpu.VMEM(w_first.shape, bf16),
                pltpu.VMEM(w_short.shape, bf16),
                pltpu.VMEM(norm_rest.shape, bf16),
                pltpu.VMEM(w_rest.shape, bf16),
                pltpu.VMEM(bias_rest.shape, bf16),
                pltpu.VMEM((3, 3, out_chans, chans), bf16),
                pltpu.VMEM((1, out_chans), bf16),
                pltpu.VMEM((2, 8, LANES), f32),
                pltpu.VMEM((8, LANES), f32),
                pltpu.VMEM((9, chans, LANES), bf16),
                pltpu.VMEM((samples, rows * cols, chans), f32),
                pltpu.VMEM((samples, rows * cols, chans), f32),
                pltpu.VMEM((8, chans), f32),
                pltpu.VMEM((3, rows // 2 + 1, 2, cols, wide), f32),
                pltpu.VMEM((3, rows // 2 + 1, cols, 2 * chans), f32),
                pltpu.VMEM((2, 2, rows * 8, LANES), f32),
                pltpu.VMEM((2, rows, LANES), f32),
                pltpu.VMEM((2, rows, LANES), f32),
                pltpu.VMEM((LANES, LANES), f32),
                pltpu.VMEM((peers_n, 2, LANES), f32),
                pltpu.VMEM((6, samples, cols, wide), bf16),
                pltpu.VMEM((samples, 2, rows, wide), bf16),
                pltpu.VMEM((samples, 2, rows, wide), bf16),
                pltpu.VMEM((rest, samples, plain_n + 1, 2, chans), f32),
                pltpu.VMEM((rest, samples, 4, 4, chans), f32),
                pltpu.VMEM((rest, samples, 2, 8 + cols, chans), f32),
                pltpu.VMEM((rest, samples, 2, 8 + rows, chans), f32),
                pltpu.VMEM((rest, samples, 4, 4, chans), f32),
                pltpu.VMEM((rest, samples, 2, 8 + cols, chans), f32),
                pltpu.VMEM((rest, samples, 2, 8 + rows, chans), f32),
                pltpu.VMEM((plain_n + 8 + 16 + cols + rows, 2, chans), f32),
                pltpu.SemaphoreType.DMA((2 * samples + 8,)),
                pltpu.SemaphoreType.DMA((2,)),
                pltpu.SemaphoreType.DMA((samples,)),
                pltpu.SemaphoreType.DMA((3,)),
                pltpu.SemaphoreType.DMA((rest, samples)),
                pltpu.SemaphoreType.DMA((4,)),
            ],
            compiler_params=pltpu.CompilerParams(collective_id=0, has_side_effects=True, vmem_limit_bytes=48 * 1024 * 1024),
        )(*[pltpu.with_memory_space_constraint(x, pltpu.HBM) for x in (act_in, norm_first, w_first, w_short, norm_rest, w_rest, bias_rest, jnp.transpose(w_out, (0, 1, 3, 2)), bias_out.reshape(1, out_chans))])
        return jnp.transpose(image, (0, 3, 2, 1))

    return jax.shard_map(local_decode, mesh=mesh, in_specs=(tile_spec,) + (replicated,) * 8, out_specs=tile_spec, check_vma=False)
```

```python
import functools

import jax
import jax.numpy as jnp
from jax import lax
from jax.experimental import pallas as pl
from jax.experimental.pallas import tpu as pltpu
from jax.sharding import PartitionSpec as P

GROUPS = 32
GN_EPS = 1e-6
MESH = pl.DeviceIdType.MESH
LANES = 128
ROW_BLOCK = 2
LAYERS = 7
CHUNKS = (11, 11, 10)
BLOCK = 2


def group_total(vec, per_group):
    lane = lax.broadcasted_iota(jnp.int32, vec.shape, 1) & (per_group - 1)
    parts = [vec]
    for dist in range(1, per_group):
        parts.append(jnp.where(lane >= dist, pltpu.roll(vec, dist, 1), pltpu.roll(vec, LANES - per_group + dist, 1)))
    while len(parts) > 1:
        parts = [parts[at] + parts[at + 1] if at + 1 < len(parts) else parts[at] for at in range(0, len(parts), 2)]
    return parts[0]


def far_first(rows_n, cols_n):
    every = [(a, b) for a in range(cols_n) for b in range(rows_n) if a or b]
    return sorted(every, key=lambda off: -(min(off[0], cols_n - off[0]) + min(off[1], rows_n - off[1]) / 2))


def decode_kernel(rows_n, cols_n, act_hbm, nf_hbm, wf_hbm, ws_hbm, nr_hbm, wr_hbm, br_hbm, wo_hbm, bo_hbm, y_ref,
                  act, norm_first, wf, ws, norm_rest, wr, bias_rest, wo_ref, bias_out, sums_first, total_first, wo, mid, hid, bias_rows, pad_first, pad_rest, slab, edge_l, edge_r, turn,
                  st_first, row_first, col_first, cs_first,
                  st_rest, corner_in, row_in, col_in, corner_out, row_out, col_out, whole_inbox,
                  load_sem, first_recv, col_recv, first_send, recv, send):
    samples, rows, cols, _ = act.shape
    pairs = rows // 2
    peers_n = rows_n * cols_n
    sx, sy = lax.axis_index("sx"), lax.axis_index("sy")
    at_x = [sx] + [lax.rem(sx + off, cols_n) for off in range(1, cols_n)]
    at_y = [sy] + [lax.rem(sy + off, rows_n) for off in range(1, rows_n)]
    order = far_first(rows_n, cols_n)
    has_l, has_r, has_t, has_b = sx > 0, sx < cols_n - 1, sy > 0, sy < rows_n - 1

    def device(off):
        return {"sx": at_x[off[0] % cols_n], "sy": at_y[off[1] % rows_n]}

    def wrap(off):
        return (off[0] % cols_n, off[1] % rows_n)

    corner_to = {wrap(off): at for at, off in enumerate(((-1, -1), (1, -1), (-1, 1), (1, 1)))}
    row_to = {wrap(off): at for at, off in enumerate(((0, -1), (0, 1)))}
    col_to = {wrap(off): at for at, off in enumerate(((-1, 0), (1, 0)))}
    plain = [off for off in order if off not in corner_to and off not in row_to and off not in col_to]

    half_rows = rows // 2
    loads = []
    for s in range(samples):
        for half in range(2):
            part = pl.ds(half * half_rows, half_rows)
            loads.append(pltpu.make_async_copy(act_hbm.at[s, part], act.at[s, part], load_sem.at[2 * s + half]))
    act_loads = 2 * samples
    others = ((ws_hbm, ws), (br_hbm, bias_rest), (wo_hbm, wo_ref), (nf_hbm, norm_first), (wf_hbm, wf), (wr_hbm, wr), (nr_hbm, norm_rest), (bo_hbm, bias_out))
    for at, (src, dst) in enumerate(others):
        loads.append(pltpu.make_async_copy(src, dst, load_sem.at[act_loads + at]))
    for load in loads[:act_loads]:
        load.start()
    barrier = pltpu.get_barrier_semaphore()
    for off in order:
        pl.semaphore_signal(barrier, inc=1, device_id=device(off), device_id_type=MESH)

    def remote(src, dst, send_to, recv_at, off):
        pltpu.make_async_remote_copy(src_ref=src, dst_ref=dst, send_sem=send_to, recv_sem=recv_at, device_id=device(off), device_id_type=MESH).start()

    def wait_for(ref, sem):
        pltpu.make_async_copy(ref, ref, sem).wait()

    def send_plain(at, s):
        for slot, off in enumerate(plain):
            remote(st_rest.at[at, s, 0], st_rest.at[at, s, 1 + slot], send.at[0], recv.at[at, s], off)

    def send_edges(at, s):
        for off, box in corner_to.items():
            remote(corner_out.at[at, s, box], corner_in.at[at, s, 3 - box], send.at[1], recv.at[at, s], off)
        for off, box in col_to.items():
            remote(col_out.at[at, s, box], col_in.at[at, s, 1 - box], send.at[3], recv.at[at, s], off)
        for off, box in row_to.items():
            remote(row_out.at[at, s, box], row_in.at[at, s, 1 - box], send.at[2], recv.at[at, s], off)

    sub = lax.broadcasted_iota(jnp.int32, (1, 8, LANES), 1)
    first_sub, last_sub = sub == 0, sub == 7

    def tree_sum(stack):
        while stack.shape[0] > 1:
            half = stack.shape[0] // 2
            folded = stack[:half] + stack[half:2 * half]
            stack = folded if stack.shape[0] == 2 * half else jnp.concatenate([folded[:1] + stack[2 * half:], folded[1:]], axis=0) if half > 1 else folded + stack[2 * half:]
        return stack[0]

    def affine(one, two, norm, per_group):
        count = rows * rows_n * cols * cols_n * per_group
        mean = group_total(one, per_group) / count
        square = group_total(two, per_group) / count
        scale = lax.rsqrt(square - mean * mean + GN_EPS) * jnp.broadcast_to(norm[0:1], (8, LANES))
        shift = jnp.broadcast_to(norm[1:2], (8, LANES)) - mean * scale
        return 0.5 * scale, 0.5 * shift

    first_group = 2 * LANES // GROUPS
    lane_in_group = lax.broadcasted_iota(jnp.int32, (8, LANES), 1) & (first_group - 1)

    def silu(x, scales):
        u = x * scales[0] + scales[1]
        return u + u * jnp.tanh(u)

    def spread(rows_of_cols, from_left, from_right):
        v0, v1 = rows_of_cols[:, 0], rows_of_cols[:, 1]
        r0, r1 = pltpu.roll(v0, 1, 1), pltpu.roll(v1, 1, 1)
        q0, q1 = pltpu.roll(v0, 7, 1), pltpu.roll(v1, 7, 1)
        shifted = (
            (jnp.where(first_sub, from_left, r0), jnp.where(first_sub, r0, r1)),
            (v0, v1),
            (jnp.where(last_sub, q1, q0), jnp.where(last_sub, from_right, q1)),
        )
        return [jnp.concatenate(pair, axis=1) for pair in shifted]

    def edges(tile, scales, halo_cols):
        one_row = (scales[0][0:1], scales[1][0:1])
        edge_l[tile] = jnp.where(has_l, silu(halo_cols[0], one_row), 0.0)
        edge_r[tile] = jnp.where(has_r, silu(halo_cols[1], one_row), 0.0)

    def activate(block, tile, scales, halo_rows, corners, row_source, place):
        begin, end = max(0, BLOCK * block + 1), min(rows, BLOCK * (block + 1) + 1)
        value = row_source(begin, end)
        lefts = [jnp.broadcast_to(edge_l[tile, r:r + 1, :], (8, LANES)) for r in range(begin, end)]
        rights = [jnp.broadcast_to(edge_r[tile, r:r + 1, :], (8, LANES)) for r in range(begin, end)]
        value = silu(value, scales)
        for at, has in enumerate((has_t, has_b)):
            if block == (-1, rows // BLOCK - 1)[at]:
                halo = jnp.where(has, silu(halo_rows[at].reshape(1, 2, 8, LANES), scales), 0.0)
                corner_l = jnp.where(jnp.logical_and(has, has_l), silu(corners[2 * at], scales), 0.0)
                corner_r = jnp.where(jnp.logical_and(has, has_r), silu(corners[2 * at + 1], scales), 0.0)
                where_at = 0 if at == 0 else len(lefts)
                value = jnp.concatenate([halo, value] if at == 0 else [value, halo], axis=0)
                lefts.insert(where_at, corner_l)
                rights.insert(where_at, corner_r)
        for off, part in enumerate(spread(value, jnp.stack(lefts), jnp.stack(rights))):
            place(off, tile, BLOCK // 2 * block + 1 if block >= 0 else 0, part.reshape(part.shape[0] // 2, 2, cols, LANES))

    def prepare_rest(at, s, source):
        wait_for(whole_inbox, recv.at[at, s])
        slots = [st_rest[at, s], corner_in[at, s, :, 0:2], row_in[at, s, :, 0:2], col_in[at, s, :, 0:2]]
        total = tree_sum(jnp.concatenate(slots, axis=0))
        one, two = (jnp.broadcast_to(total[which:which + 1], (8, LANES)) for which in range(2))
        scales = affine(one, two, norm_rest[at].astype(jnp.float32), LANES // GROUPS)

        def row_source(begin, end):
            return source[s, begin * cols:end * cols, :].reshape(end - begin, 2, 8, LANES)

        def place(off, tile, pair_at, value):
            for half in range(2):
                pad_rest[off, pair_at:pair_at + value.shape[0], :, half * LANES:(half + 1) * LANES] = value[:, half]

        edges(0, scales, [col_in[at, s, box, 8:8 + rows, :] for box in range(2)])
        halo_rows = [row_in[at, s, box, 8:8 + cols, :] for box in range(2)]
        corners = [jnp.broadcast_to(corner_in[at, s, box, 2:3, :], (8, LANES)) for box in range(4)]
        return lambda block: activate(block, 0, scales, halo_rows, corners, row_source, place)

    def prepare_first(s):
        wait_for(col_first.at[s], col_recv.at[s])
        norm = norm_first[...].astype(jnp.float32)

        def one_tile(tile):
            lanes = slice(tile * LANES, (tile + 1) * LANES)
            packed = jnp.broadcast_to(total_first[tile:tile + 1], (8, LANES))
            one, two = (jnp.where(lane_in_group == which * samples + s, packed, 0.0) for which in range(2))
            scales = affine(one, two, norm[:, lanes], first_group)

            def row_source(begin, end):
                return act[s, begin:end, :, lanes].astype(jnp.float32).reshape(end - begin, 2, 8, LANES)

            def place(off, tile, pair_at, value):
                pad_first[off, pair_at:pair_at + value.shape[0], :, :, lanes] = value

            edges(tile, scales, [col_first[s, box, :, lanes].astype(jnp.float32) for box in range(2)])
            halo_rows = [row_first[box, s, :, lanes].astype(jnp.float32) for box in (1, 4)]
            corners = []
            for box in (0, 2, 3, 5):
                row = row_first[box, s, :, lanes].astype(jnp.float32)
                corners.append(pltpu.roll(row[8:16], 1, 0) if box % 3 == 0 else pltpu.roll(row[0:8], 7, 0))
            return lambda block: activate(block, tile, scales, halo_rows, corners, row_source, place)

        tiles = [one_tile(tile) for tile in range(2)]
        return lambda block: [tile(block) for tile in tiles]

    zero = jnp.zeros((LANES, LANES), jnp.bfloat16)
    wide_zero = jnp.zeros((2 * LANES, LANES), jnp.bfloat16)

    def square_of(a, b, c, d):
        return jnp.concatenate([jnp.concatenate([a, b], axis=1), jnp.concatenate([c, d], axis=1)], axis=0)

    def conv_rest(weight, pair_from, pair_n):
        total = None
        for off in range(3):
            w0, w1, w2 = (weight(row_off, off) for row_off in range(3))
            for shift, tap in ((0, square_of(w0, zero, w1, w0)), (1, square_of(w2, w1, zero, w2))):
                lhs = pad_rest[off, pair_from + shift:pair_from + shift + pair_n].reshape(pair_n * cols, 2 * LANES)
                part = jnp.dot(lhs, tap.astype(jnp.float32), preferred_element_type=jnp.float32)
                total = part if total is None else total + part
        return total

    def conv_first(pair_from, pair_n):
        total = None
        for off in range(3):
            w0, w1, w2 = (wf[row_off, off] for row_off in range(3))
            for at, (a, b) in enumerate(((w0, wide_zero), (w1, w0), (w2, w1), (wide_zero, w2))):
                begin = pair_from + at // 2
                lhs = pad_first[off, begin:begin + pair_n, at % 2].reshape(pair_n * cols, 2 * LANES)
                part = jnp.dot(lhs, jnp.concatenate([a, b], axis=1).astype(jnp.float32), preferred_element_type=jnp.float32)
                total = part if total is None else total + part
        return total

    def in_chunks(block, conv, use):
        block(-1)
        done, begin = 0, 0
        for chunk in CHUNKS:
            per_chunk = chunk * pairs // sum(CHUNKS)
            while BLOCK // 2 * done < begin + per_chunk:
                block(done)
                done += 1
            total = conv(begin, per_chunk)
            halves = [total[:, half * LANES:(half + 1) * LANES].reshape(per_chunk, 1, cols, LANES) for half in range(2)]
            use(2 * begin, jnp.concatenate(halves, axis=1).reshape(2 * per_chunk * cols, LANES))
            begin += per_chunk

    def finish(at, s, block, conv, bias, target, residual):
        acc = []

        def use(row, value):
            rows_in = value.shape[0] // cols
            value = value + bias
            if residual is not None:
                value = value + residual[s, row * cols:row * cols + value.shape[0], :]
            value = value.astype(jnp.bfloat16).astype(jnp.float32)
            target[s, row * cols:row * cols + value.shape[0], :] = value
            for edge, edge_row in enumerate((0, rows - 1)):
                if row <= edge_row < row + rows_in:
                    line = value[(edge_row - row) * cols:(edge_row - row + 1) * cols]
                    row_out[at, s, edge, 8:8 + cols, :] = line
                    corner_out[at, s, 2 * edge, 2:3, :] = line[0:1]
                    corner_out[at, s, 2 * edge + 1, 2:3, :] = line[cols - 1:cols]
            for box in range(2):
                column = target[s, pl.ds(row * cols + box * (cols - 1), rows_in, stride=cols), :]
                col_out[at, s, box, 8 + row:8 + row + rows_in, :] = column
            split = value.reshape(value.shape[0] // 16, 2, 8, LANES)
            acc.append([jnp.sum(split, axis=0), jnp.sum(split * split, axis=0)])

        in_chunks(block, conv, use)
        sums = []
        for which in range(2):
            part = acc[0][which]
            for more in acc[1:]:
                part = part + more[which]
            sums.append(jnp.sum(part[0] + part[1], axis=0, keepdims=True))
        sums = jnp.concatenate(sums, axis=0)
        st_rest[at, s, 0] = sums
        send_plain(at, s)
        for box in range(4):
            corner_out[at, s, box, 0:2, :] = sums
        for box in range(2):
            row_out[at, s, box, 0:2, :] = sums
            col_out[at, s, box, 0:2, :] = sums
        send_edges(at, s)

    def first_sums(s, carry):

        def body(step, sums):
            sums = list(sums)
            for at in range(ROW_BLOCK):
                r = step * ROW_BLOCK + at
                for tile in range(2):
                    row = act[s, r, :, tile * LANES:(tile + 1) * LANES].astype(jnp.float32)
                    v0, v1 = row[0:8], row[8:16]
                    slab[0, tile, pl.ds(pl.multiple_of(r * 8, 8), 8), :] = v0
                    slab[1, tile, pl.ds(pl.multiple_of(r * 8, 8), 8), :] = v1
                    sums[2 * tile] = sums[2 * tile] + (v0 + v1)
                    sums[2 * tile + 1] = sums[2 * tile + 1] + (v0 * v0 + v1 * v1)
            return tuple(sums)

        sums = (jnp.zeros((8, LANES), jnp.float32),) * 4
        for half in range(2):
            wait_for(act.at[s, pl.ds(half * half_rows, half_rows)], load_sem.at[2 * s + half])
            sums = lax.fori_loop(half * half_rows // ROW_BLOCK, (half + 1) * half_rows // ROW_BLOCK, body, sums)
        for side in range(2):
            for tile in range(2):
                column = slab[side, tile, pl.ds(7 * side, rows, stride=8), :]
                cs_first[s, side, :, tile * LANES:(tile + 1) * LANES] = column.astype(jnp.bfloat16)
        for tile in range(2):
            for which in range(2):
                sums_first[tile, pl.ds(which * samples + s, 1), :] = jnp.sum(sums[2 * tile + which], axis=0, keepdims=True)
        return carry

    lax.fori_loop(0, samples, first_sums, 0)
    for load in loads[act_loads:]:
        load.start()
    row_at = lax.broadcasted_iota(jnp.int32, (8, LANES), 0)
    for tile in range(2):
        grouped = jnp.where(row_at == lane_in_group, group_total(sums_first[tile], first_group), 0.0)
        st_first[0, tile:tile + 1, :] = jnp.sum(grouped, axis=0, keepdims=True)
    pl.semaphore_wait(barrier, peers_n - 1)
    for slot, off in enumerate(order):
        remote(st_first.at[0], st_first.at[slot + 1], first_send.at[0], first_recv.at[0], off)
    for row, y_off, base in ((0, -1, 3), (rows - 1, 1, 0)):
        for x_off, at in ((-1, 2), (0, 1), (1, 0)):
            remote(act.at[:, row], row_first.at[base + at], first_send.at[1], first_recv.at[1], (x_off, y_off))

    def first_columns(s, carry):
        for off, box in col_to.items():
            remote(cs_first.at[s, box], col_first.at[s, 1 - box], first_send.at[2], col_recv.at[s], off)
        return carry

    lax.fori_loop(0, samples, first_columns, 0)

    for load in loads[act_loads:act_loads + 3]:
        load.wait()
    bias = bias_rest[...].astype(jnp.float32)

    def shortcut(s, carry):
        flat = act[s].reshape(rows * cols, 2 * LANES)
        hid[s] = jnp.dot(flat, ws[...], preferred_element_type=jnp.float32) + bias[6:7]
        return carry

    lax.fori_loop(0, samples, shortcut, 0)
    for tap in range(9):
        three = wo_ref[tap // 3, tap % 3].astype(jnp.float32)
        eight = jnp.concatenate([three, jnp.zeros((8 - three.shape[0], LANES), jnp.float32)], axis=0)
        wo[tap] = jnp.concatenate([eight] * 16, axis=0).T.astype(jnp.bfloat16)
    for load in loads[act_loads + 3:]:
        load.wait()
    wait_for(st_first.at[pl.ds(1, peers_n - 1)], first_recv.at[0])
    total_first[0:2, :] = jnp.sum(st_first[...], axis=0)
    wait_for(row_first, first_recv.at[1])

    def layer_first(s, carry):
        finish(0, s, prepare_first(s), conv_first, bias[0:1], mid, None)
        return carry

    lax.fori_loop(0, samples, layer_first, 0)

    def layer_rest(layer, source, target, residual):
        def one_sample(s, carry):
            block = prepare_rest(layer - 1, s, source)
            conv = functools.partial(conv_rest, lambda row_off, off: wr[layer - 1, row_off, off])
            finish(layer, s, block, conv, bias_rows[pl.ds(layer, 1), :], target, residual)
            return carry

        lax.fori_loop(0, samples, one_sample, 0)

    def layer_pair(step, carry):
        layer_rest(2 * step + 1, mid, hid, hid)
        layer_rest(2 * step + 2, hid, mid, None)
        return carry

    bias_rows[0:bias.shape[0], :] = bias
    lax.fori_loop(0, (LAYERS - 2) // 2, layer_pair, 0)
    layer_rest(LAYERS - 2, mid, hid, hid)

    lane = lax.broadcasted_iota(jnp.int32, (rows, LANES), 1)
    out_bias = bias_out[...].astype(jnp.float32)

    def layer_last(s, carry):
        def use(row, value):
            mid[s, row * cols:row * cols + value.shape[0], :] = value

        in_chunks(prepare_rest(LAYERS - 2, s, hid), functools.partial(conv_rest, lambda row_off, off: wo[3 * row_off + off]), use)
        merged = mid[s, pl.ds(0, rows, stride=cols), :]
        for col in range(1, cols):
            merged = jnp.where(lane // 8 == col, mid[s, pl.ds(col, rows, stride=cols), :], merged)
        turn[...] = jnp.concatenate([merged] * (LANES // rows), axis=0).T
        for chan in range(y_ref.shape[1]):
            plane = turn[pl.ds(chan, cols, stride=8), :]
            y_ref[s, chan] = plane[:, 0:rows] + out_bias[0:1, chan:chan + 1]
        return carry

    lax.fori_loop(0, samples, layer_last, 0)

    wait_for(st_first.at[pl.ds(1, peers_n - 1)], first_send.at[0])
    wait_for(row_first, first_send.at[1])
    wait_for(cs_first, first_send.at[2])
    wait_for(st_rest.at[:, :, pl.ds(1, len(plain))], send.at[0])
    wait_for(corner_out, send.at[1])
    wait_for(row_out, send.at[2])
    wait_for(col_out, send.at[3])


def solution(mesh):
    rows_n, cols_n = mesh.shape["sy"], mesh.shape["sx"]
    peers_n = rows_n * cols_n
    tile_spec = P("dp", "sy", "sx", None)
    replicated = P()

    def local_decode(act_in, norm_first, w_first, w_short, norm_rest, w_rest, bias_rest, w_out, bias_out):
        samples, rows, cols, wide = act_in.shape
        chans = w_short.shape[1]
        out_chans = w_out.shape[3]
        f32, bf16 = jnp.float32, jnp.bfloat16
        rest, plain_n = LAYERS - 1, peers_n - 9
        whole = pl.BlockSpec(memory_space=pltpu.VMEM)
        there = pl.BlockSpec(memory_space=pltpu.HBM)
        image = pl.pallas_call(
            functools.partial(decode_kernel, rows_n, cols_n),
            name="decode",
            out_shape=jax.ShapeDtypeStruct((samples, out_chans, cols, rows), f32),
            in_specs=[there] * 9,
            out_specs=whole,
            scratch_shapes=[
                pltpu.VMEM(act_in.shape, bf16),
                pltpu.VMEM(norm_first.shape, bf16),
                pltpu.VMEM(w_first.shape, bf16),
                pltpu.VMEM(w_short.shape, bf16),
                pltpu.VMEM(norm_rest.shape, bf16),
                pltpu.VMEM(w_rest.shape, bf16),
                pltpu.VMEM(bias_rest.shape, bf16),
                pltpu.VMEM((3, 3, out_chans, chans), bf16),
                pltpu.VMEM((1, out_chans), bf16),
                pltpu.VMEM((2, 8, LANES), f32),
                pltpu.VMEM((8, LANES), f32),
                pltpu.VMEM((9, chans, LANES), bf16),
                pltpu.VMEM((samples, rows * cols, chans), f32),
                pltpu.VMEM((samples, rows * cols, chans), f32),
                pltpu.VMEM((8, chans), f32),
                pltpu.VMEM((3, rows // 2 + 1, 2, cols, wide), f32),
                pltpu.VMEM((3, rows // 2 + 1, cols, 2 * chans), f32),
                pltpu.VMEM((2, 2, rows * 8, LANES), f32),
                pltpu.VMEM((2, rows, LANES), f32),
                pltpu.VMEM((2, rows, LANES), f32),
                pltpu.VMEM((LANES, LANES), f32),
                pltpu.VMEM((peers_n, 2, LANES), f32),
                pltpu.VMEM((6, samples, cols, wide), bf16),
                pltpu.VMEM((samples, 2, rows, wide), bf16),
                pltpu.VMEM((samples, 2, rows, wide), bf16),
                pltpu.VMEM((rest, samples, plain_n + 1, 2, chans), f32),
                pltpu.VMEM((rest, samples, 4, 4, chans), f32),
                pltpu.VMEM((rest, samples, 2, 8 + cols, chans), f32),
                pltpu.VMEM((rest, samples, 2, 8 + rows, chans), f32),
                pltpu.VMEM((rest, samples, 4, 4, chans), f32),
                pltpu.VMEM((rest, samples, 2, 8 + cols, chans), f32),
                pltpu.VMEM((rest, samples, 2, 8 + rows, chans), f32),
                pltpu.VMEM((plain_n + 8 + 16 + cols + rows, 2, chans), f32),
                pltpu.SemaphoreType.DMA((2 * samples + 8,)),
                pltpu.SemaphoreType.DMA((2,)),
                pltpu.SemaphoreType.DMA((samples,)),
                pltpu.SemaphoreType.DMA((3,)),
                pltpu.SemaphoreType.DMA((rest, samples)),
                pltpu.SemaphoreType.DMA((4,)),
            ],
            compiler_params=pltpu.CompilerParams(collective_id=0, has_side_effects=True, vmem_limit_bytes=48 * 1024 * 1024),
        )(*[pltpu.with_memory_space_constraint(x, pltpu.HBM) for x in (act_in, norm_first, w_first, w_short, norm_rest, w_rest, bias_rest, jnp.transpose(w_out, (0, 1, 3, 2)), bias_out.reshape(1, out_chans))])
        return jnp.transpose(image, (0, 3, 2, 1))

    return jax.shard_map(local_decode, mesh=mesh, in_specs=(tile_spec,) + (replicated,) * 8, out_specs=tile_spec, check_vma=False)
```
